32 devices in a mesh: tensor: 4 (over z), replica: 2 (over y), fsdp: 4 (over x, core).
Axes of the slice: x: 2, y: 2, z: 4, core: 2. Of those that a mesh axis runs over, the one named last changes fastest.
Arguments:
- x_tokens: bfloat16 [2048, 2048], P(('replica', 'fsdp'))
- dy_tokens: bfloat16 [2048, 2048], P(('replica', 'fsdp'))
- w_gate: bfloat16 [2, 2048, 8192], P(None, 'fsdp', 'tensor')
- w_up: bfloat16 [2, 2048, 8192], P(None, 'fsdp', 'tensor')
- w_down: bfloat16 [2, 8192, 2048], P(None, ('tensor', 'fsdp'))
- norm_gain: float32 [2, 2048], replicated
Outputs:
- output 1: bfloat16 [2048, 2048], P(('replica', 'fsdp'))
- output 2: float32 [2, 2048, 8192], P(None, 'fsdp', 'tensor')
- output 3: float32 [2, 2048, 8192], P(None, 'fsdp', 'tensor')
- output 4: float32 [2, 8192, 2048], P(None, ('tensor', 'fsdp'))
- output 5: float32 [2, 2048], replicated
All inputs are finite; a program needn't handle non-finite values.
Results may differ from the reference program's by a relative error of at most 0.00785844.
Values are sent between devices in bfloat16 or wider.
A program may use at most 1 GiB of HBM per device.

```python
import jax
import jax.numpy as jnp
from jax import lax

D_MODEL = 2048
D_FF = 8192
TOK_DEV = 256
LAYERS = 2
REPLICA_SIZE = 2
FSDP_SIZE = 4
TOKENS = TOK_DEV * REPLICA_SIZE * FSDP_SIZE
ROW_BLOCK = min(TOK_DEV, 256)
NUM_BLOCKS = TOKENS // ROW_BLOCK


def setup_inputs(seed: int = 0) -> dict:
    key_list = jax.random.split(jax.random.key(seed), 6)
    x_tokens = jax.random.normal(key_list[0], (TOKENS, D_MODEL), jnp.float32)
    dy_tokens = jax.random.normal(key_list[1], (TOKENS, D_MODEL), jnp.float32) * TOKENS ** -0.5
    w_gate = jax.random.normal(key_list[2], (LAYERS, D_MODEL, D_FF), jnp.float32) * D_MODEL ** -0.5
    w_up = jax.random.normal(key_list[3], (LAYERS, D_MODEL, D_FF), jnp.float32) * D_MODEL ** -0.5
    w_down = jax.random.normal(key_list[4], (LAYERS, D_FF, D_MODEL), jnp.float32) * D_FF ** -0.5
    norm_gain = jax.random.uniform(key_list[5], (LAYERS, D_MODEL), jnp.float32, 0.5, 1.5)
    return {"x_tokens": x_tokens.astype(jnp.bfloat16), "dy_tokens": dy_tokens.astype(jnp.bfloat16), "w_gate": w_gate.astype(jnp.bfloat16), "w_up": w_up.astype(jnp.bfloat16), "w_down": w_down.astype(jnp.bfloat16), "norm_gain": norm_gain}


def layer_forward(h_in, w_g, w_u, w_d, gain_vec):
    h_f = h_in.astype(jnp.float32)
    r_inv = lax.rsqrt(jnp.mean(h_f * h_f, axis=-1, keepdims=True) + 1e-6)
    normed = (h_f * r_inv * gain_vec).astype(jnp.bfloat16)
    gate_val = jnp.dot(normed, w_g, preferred_element_type=jnp.float32).astype(jnp.bfloat16)
    up_val = jnp.dot(normed, w_u, preferred_element_type=jnp.float32).astype(jnp.bfloat16)
    act_val = (jax.nn.silu(gate_val.astype(jnp.float32)) * up_val.astype(jnp.float32)).astype(jnp.bfloat16)
    mlp_out = jnp.dot(act_val, w_d, preferred_element_type=jnp.float32)
    h_out = (h_f + mlp_out).astype(jnp.bfloat16)
    return h_out, (h_in, normed, gate_val, up_val, act_val)


def layer_backward(d_resid, w_g, w_u, w_d, gain_vec, saved_acts):
    h_in, normed, gate_val, up_val, act_val = saved_acts
    d_out = d_resid.astype(jnp.bfloat16)
    d_act = jnp.dot(d_out, w_d.T, preferred_element_type=jnp.float32).astype(jnp.bfloat16)
    dw_d = jnp.dot(act_val.T, d_out, preferred_element_type=jnp.float32)
    gate_f = gate_val.astype(jnp.float32)
    sig_gate = jax.nn.sigmoid(gate_f)
    d_act_f = d_act.astype(jnp.float32)
    d_gate = (d_act_f * up_val.astype(jnp.float32) * sig_gate * (1.0 + gate_f * (1.0 - sig_gate))).astype(jnp.bfloat16)
    d_up = (d_act_f * gate_f * sig_gate).astype(jnp.bfloat16)
    dw_g = jnp.dot(normed.T, d_gate, preferred_element_type=jnp.float32)
    dw_u = jnp.dot(normed.T, d_up, preferred_element_type=jnp.float32)
    d_normed = jnp.dot(d_gate, w_g.T, preferred_element_type=jnp.float32) + jnp.dot(d_up, w_u.T, preferred_element_type=jnp.float32)
    h_f = h_in.astype(jnp.float32)
    r_inv = lax.rsqrt(jnp.mean(h_f * h_f, axis=-1, keepdims=True) + 1e-6)
    x_hat = h_f * r_inv
    d_gain = jnp.sum(d_normed * x_hat, axis=0)
    v_term = d_normed * gain_vec
    d_next = d_resid + r_inv * (v_term - x_hat * jnp.mean(v_term * x_hat, axis=-1, keepdims=True))
    return d_next, (dw_g, dw_u, dw_d, d_gain)


def block_pass(x_block, dy_block, w_gate, w_up, w_down, norm_gain):
    def fwd_step(h_cur, layer_w):
        w_g, w_u, w_d, gain_vec = layer_w
        return layer_forward(h_cur, w_g, w_u, w_d, gain_vec)

    y_block, saved_acts = lax.scan(fwd_step, x_block, (w_gate, w_up, w_down, norm_gain))

    def bwd_step(d_resid, layer_in):
        layer_w, saved_layer = layer_in
        w_g, w_u, w_d, gain_vec = layer_w
        return layer_backward(d_resid, w_g, w_u, w_d, gain_vec, saved_layer)

    _, layer_grads = lax.scan(bwd_step, dy_block.astype(jnp.float32), ((w_gate, w_up, w_down, norm_gain), saved_acts), reverse=True)
    return y_block, layer_grads


def reference(x_tokens, dy_tokens, w_gate, w_up, w_down, norm_gain):
    x_blocks = x_tokens.reshape(NUM_BLOCKS, ROW_BLOCK, D_MODEL)
    dy_blocks = dy_tokens.reshape(NUM_BLOCKS, ROW_BLOCK, D_MODEL)

    def outer_step(grad_sum, block_in):
        x_block, dy_block = block_in
        y_block, layer_grads = block_pass(x_block, dy_block, w_gate, w_up, w_down, norm_gain)
        return tuple(total + part for total, part in zip(grad_sum, layer_grads)), y_block

    zero_init = (jnp.zeros((LAYERS, D_MODEL, D_FF), jnp.float32), jnp.zeros((LAYERS, D_MODEL, D_FF), jnp.float32), jnp.zeros((LAYERS, D_FF, D_MODEL), jnp.float32), jnp.zeros((LAYERS, D_MODEL), jnp.float32))
    grad_sum, y_blocks = lax.scan(outer_step, zero_init, (x_blocks, dy_blocks))
    return (y_blocks.reshape(TOKENS, D_MODEL), grad_sum[0], grad_sum[1], grad_sum[2], grad_sum[3])
```

```python
import jax
import jax.numpy as jnp
from jax import lax
from jax.sharding import PartitionSpec as P

AXES = ("tensor", "replica", "fsdp")
F32 = jnp.float32
BF16 = jnp.bfloat16


def dev_index(z, y, x, c):
    return (z * 2 + y) * 4 + x * 2 + c


def make_pairs(fn):
    return [(dev_index(z, y, x, c), dev_index(*fn(z, y, x, c))) for z in range(4) for y in range(2) for x in range(2) for c in range(2)]


OVER_X = make_pairs(lambda z, y, x, c: (z, y, 1 - x, c))
OVER_XC = make_pairs(lambda z, y, x, c: (z, y, 1 - x, (c + y) % 2))
OVER_Y = make_pairs(lambda z, y, x, c: (z, 1 - y, x, c))
OVER_C = make_pairs(lambda z, y, x, c: (z, y, x, 1 - c))


def send(val, pairs):
    return lax.ppermute(val, AXES, pairs)


def mm(lhs, rhs, ldim, rdim):
    return lax.dot_general(lhs, rhs, (((ldim,), (rdim,)), ((), ())), preferred_element_type=F32)


def rms(h_bf, gain_vec):
    h_f = h_bf.astype(F32)
    r_inv = lax.rsqrt(jnp.mean(h_f * h_f, axis=-1, keepdims=True) + 1e-6)
    return h_f, r_inv, (h_f * r_inv * gain_vec).astype(BF16)


def solution(mesh):
    tok_spec = P(("replica", "fsdp"), None)
    wide_spec = P(None, "fsdp", "tensor")
    down_spec = P(None, ("tensor", "fsdp"), None)
    gain_spec = P(None, None)

    def device_fn(x_loc, dy_loc, w_gate, w_up, w_down, norm_gain):
        z = lax.axis_index("tensor")
        y = lax.axis_index("replica")
        f = lax.axis_index("fsdp")
        x, c = f // 2, f % 2
        xo = 1 - x
        cs = (c + y) % 2

        def core_half(arr, k):
            return lax.dynamic_index_in_dim(arr.reshape(2, 512, 2, 2, 512), k, axis=3, keepdims=False)

        def gather_weights(l):
            gu = jnp.stack([w_gate[l], w_up[l]])
            part = send(core_half(gu, 1 - c), OVER_C)
            via_x = send(core_half(gu, cs), OVER_XC)
            wd_x = send(lax.dynamic_slice_in_dim(w_down[l], y * 256, 256, 0), OVER_X)
            via_y = send(via_x, OVER_Y)
            wd_y = send(wd_x, OVER_Y)
            full = jnp.zeros((4, 2, 512, 2, 512), BF16)
            for idx, piece in ((f, core_half(gu, c)), (2 * x + 1 - c, part), (2 * xo + cs, via_x), (2 * xo + 1 - cs, via_y)):
                full = lax.dynamic_update_index_in_dim(full, piece, idx, 0)
            full = full.reshape(4, 2, 512, 1024)
            wg = full[:, 0].reshape(2048, 1024)
            wu = full[:, 1].reshape(2048, 1024)
            wd = jnp.zeros((4, 256, 2048), BF16)
            wd = lax.dynamic_update_slice_in_dim(wd, w_down[l].reshape(2, 256, 2048), 2 * x, 0)
            wd = lax.dynamic_update_index_in_dim(wd, wd_x, 2 * xo + y, 0)
            wd = lax.dynamic_update_index_in_dim(wd, wd_y, 2 * xo + 1 - y, 0)
            return wg, wu, wd.reshape(1024, 2048)

        def pair_up(v):
            return jnp.concatenate([v, send(v, OVER_C)], axis=-2)

        def plane_rest(v):
            rows = v.shape[-2]
            from_x = send(v, OVER_X)
            from_y = send(v, OVER_Y)
            d_x = send(from_y[..., : rows // 2, :], OVER_X)
            d_y = send(from_x[..., rows // 2 :, :], OVER_Y)
            mine = jnp.concatenate([from_x, from_y, d_x, d_y], axis=-2)
            return jnp.concatenate([mine, send(mine, OVER_C)], axis=-2)

        def fwd(n, wts):
            a = mm(n, wts[0], 1, 0).astype(BF16)
            b = mm(n, wts[1], 1, 0).astype(BF16)
            a_f = a.astype(F32)
            return a, b, (a_f * jax.nn.sigmoid(a_f) * b.astype(F32)).astype(BF16)

        def bwd(o, a, b, wts):
            q_f = mm(o, wts[2], 1, 1).astype(BF16).astype(F32)
            a_f = a.astype(F32)
            s = jax.nn.sigmoid(a_f)
            da = (q_f * b.astype(F32) * s * (1.0 + a_f * (1.0 - s))).astype(BF16)
            return da, (q_f * a_f * s).astype(BF16)

        def sum_scatter(p):
            own = p[:256] + send(p[256:], OVER_C)
            return lax.psum_scatter(own, "tensor", scatter_dimension=0, tiled=True)

        def over_z(v):
            return lax.all_gather(v, "tensor", axis=0, tiled=True)

        def chunk(v):
            return lax.dynamic_slice_in_dim(v, z * 64, 64, 0)

        def weight_grads(n2, nr, o2, orest, act2, actr, d2, dr):
            n_all = jnp.concatenate([n2, nr])
            n_rows = lax.dynamic_slice_in_dim(n_all, x * 1024, 1024, 1)
            da = jnp.concatenate([d2[0], dr[0]])
            db = jnp.concatenate([d2[1], dr[1]])
            g_col = lax.dynamic_slice_in_dim(jnp.concatenate([act2, actr]), x * 512, 512, 1)
            dwd = mm(g_col, jnp.concatenate([o2, orest]), 0, 0)
            outs = []
            for d in (da, db):
                quad = mm(n_rows, d, 0, 0)
                keep = lax.dynamic_slice_in_dim(quad, c * 512, 512, 0)
                got = send(lax.dynamic_slice_in_dim(quad, (1 - c) * 512, 512, 0), OVER_C)
                lo = jnp.where(c == 0, keep, got).reshape(512, 2, 1, 512)
                hi = jnp.where(c == 0, got, keep).reshape(512, 2, 1, 512)
                outs.append(jnp.concatenate([lo, hi], axis=2).reshape(512, 2048))
            return outs[0], outs[1], dwd

        wts0 = gather_weights(0)
        both = jnp.stack([x_loc, dy_loc])
        own2 = pair_up(both)
        x2, o2_1 = own2[0], own2[1]
        xf2, r2, n2_0 = rms(x2, norm_gain[0])
        rest = plane_rest(both)
        a2_0, b2_0, g2_0 = fwd(n2_0, wts0)
        s0 = sum_scatter(mm(g2_0, wts0[2], 1, 0))
        wts1 = gather_weights(1)
        h1 = (chunk(x_loc).astype(F32) + s0).astype(BF16)
        h1_f, r1, n1 = rms(h1, norm_gain[1])
        n_own1 = over_z(n1)
        n2_1 = pair_up(n_own1)
        nr_0 = rms(rest[0], norm_gain[0])[2]
        ar_0, br_0, gr_0 = fwd(nr_0, wts0)
        a2_1, b2_1, g2_1 = fwd(n2_1, wts1)
        d2_1 = bwd(o2_1, a2_1, b2_1, wts1)
        m1 = sum_scatter(mm(d2_1[0], wts1[0], 1, 1) + mm(d2_1[1], wts1[1], 1, 1))
        nr_1 = plane_rest(n_own1)
        s1 = sum_scatter(mm(g2_1, wts1[2], 1, 0))
        y_out = over_z((h1_f + s1).astype(BF16))
        xh1 = h1_f * r1
        dgain1 = jnp.sum(m1 * xh1, axis=0)
        v = m1 * norm_gain[1]
        e = chunk(dy_loc).astype(F32) + r1 * (v - xh1 * jnp.mean(v * xh1, axis=-1, keepdims=True))
        o_own0 = over_z(e.astype(BF16))
        o2_0 = pair_up(o_own0)
        or_0 = plane_rest(o_own0)
        ar_1, br_1, gr_1 = fwd(nr_1, wts1)
        dr_1 = bwd(rest[1], ar_1, br_1, wts1)
        grads1 = weight_grads(n2_1, nr_1, o2_1, rest[1], g2_1, gr_1, d2_1, dr_1)
        d2_0 = bwd(o2_0, a2_0, b2_0, wts0)
        m0 = mm(d2_0[0], wts0[0], 1, 1) + mm(d2_0[1], wts0[1], 1, 1)
        dgain0 = jnp.sum(m0 * (xf2 * r2), axis=0)
        d_gain = lax.psum(jnp.stack([dgain0, dgain1]), AXES)
        dr_0 = bwd(or_0, ar_0, br_0, wts0)
        grads0 = weight_grads(n2_0, nr_0, o2_0, or_0, g2_0, gr_0, d2_0, dr_0)
        return (y_out, jnp.stack([grads0[0], grads1[0]]), jnp.stack([grads0[1], grads1[1]]), jnp.stack([grads0[2], grads1[2]]), d_gain)

    return jax.shard_map(device_fn, mesh=mesh, in_specs=(tok_spec, tok_spec, wide_spec, wide_spec, down_spec, gain_spec), out_specs=(tok_spec, wide_spec, wide_spec, down_spec, gain_spec), check_vma=False)
```

```python
import functools

import jax
import jax.numpy as jnp
from jax import lax
from jax.experimental import pallas as pl
from jax.experimental.pallas import tpu as pltpu
from jax.sharding import PartitionSpec as P

F32 = jnp.float32
BF16 = jnp.bfloat16
MESH = pl.DeviceIdType.MESH
NSEM = 160
NLOC = 48


def mm(lhs, rhs, ldim, rdim):
    return lax.dot_general(lhs, rhs, (((ldim,), (rdim,)), ((), ())), preferred_element_type=F32)


def kernel(
    x_in, dy_in, wg_in, wu_in, wd_in, gain,
    y_out, dwg_out, dwu_out, dwd_out, dgain_out, n0_buf, n1_buf, o1_buf, o0_buf, a_save, b_save, x_part,
    wg, wu, wd, acc_g, acc_u, acc_d, nb, ob, a_t, b_t, g_t, g_keep, part, from_core, from_z, n_own, o_own,
    x_ch, dy_ch, h1_ch, y_ch, r_own, dg, dg_core, dg_x, dg_y, dg_z, ssem, rsem, lsem,
):
    td, d = x_in.shape
    rb = wg_in.shape[1]
    fb = wg_in.shape[2] // 4
    hh = 2 * fb
    t2, ch, half = 2 * td, td // 4, td // 2
    tile = min(512, fb)
    z = lax.axis_index("tensor")
    y = lax.axis_index("replica")
    f = lax.axis_index("fsdp")
    x, c = f // 2, f % 2
    xo, yo, co = 1 - x, 1 - y, 1 - c
    q, qx, qy, qd = 2 * y + x, 2 * y + xo, 2 * yo + x, 2 * yo + xo
    cs = (c + y) % 2
    cso = 1 - cs
    to_c, to_x, to_xs, to_y = {"fsdp": 2 * x + co}, {"fsdp": 2 * xo + c}, {"fsdp": 2 * xo + cs}, {"replica": yo}

    def to_z(dz):
        return {"tensor": (z + dz) % 4}

    def rows(start, size):
        return pl.ds(pl.multiple_of(start, size if size % 16 == 0 else 8), size)

    def cols(start, size):
        return pl.ds(pl.multiple_of(start, 128), size)

    ids, lids, sent = {}, {}, {}

    def remote(key, src, dst, dev):
        i = ids.setdefault(key, len(ids))
        assert i < NSEM
        return pltpu.make_async_remote_copy(src_ref=src, dst_ref=dst, send_sem=ssem.at[i], recv_sem=rsem.at[i], device_id=dev, device_id_type=MESH)

    def push(key, src, dst, dev, again=None):
        copy = remote(key, src, dst, dev)
        copy.start()
        sent[key] = again or (lambda: copy)

    def got(key, dst):
        remote(key, dst, dst, to_c).wait_recv()

    def send_done(key):
        sent.pop(key)().wait_send()

    def local(key, src, dst):
        i = lids.setdefault(key, len(lids))
        assert i < NLOC
        return pltpu.make_async_copy(src, dst, lsem.at[i])

    def wview(ref, l, row, xb):
        return ref.at[l, rows(row * rb, rb), cols(xb * fb, fb)]

    def wsrc(ref, l, xb, core):
        return ref.at[l, :, cols((2 * xb + core) * fb, fb)]

    gu = ((wg_in, wg), (wu_in, wu))

    barrier = pltpu.get_barrier_semaphore()
    for dev in (to_c, to_x, {"fsdp": 2 * xo + co}, to_y, to_z(1), to_z(2), to_z(3)):
        pl.semaphore_signal(barrier, inc=1, device_id=dev, device_id_type=MESH)
    pl.semaphore_wait(barrier, 7)

    loads = [local("x", x_in, n_own.at[pl.ds(0, td)])]
    loads[0].start()
    for l in range(2):
        for m in range(2):
            for xb in range(2):
                push(("wx", l, m, xb), wsrc(gu[m][0], l, xb, cs), wview(gu[m][1], l, f, xb), to_xs)
        for k in range(2):
            r0 = y * (fb // 2) + k * (fb // 4)
            push(("wdx", l, k), wd_in.at[l, rows(r0, fb // 4)], wd.at[l, rows(x * fb + r0, fb // 4)], to_x)
        for m in range(2):
            for xb in range(2):
                push(("wc", l, m, xb), wsrc(gu[m][0], l, xb, co), wview(gu[m][1], l, f, xb), to_c)
                local(("w", l, m, xb), wsrc(gu[m][0], l, xb, c), wview(gu[m][1], l, f, xb)).start()
        local(("wd", l), wd_in.at[l], wd.at[l, rows(x * fb, fb)]).start()
    push("xp", x_in, x_part, to_c)
    push("dyp", dy_in, o1_buf.at[q, c], to_c)
    local("xc", x_in.at[rows(z * ch, ch)], x_ch).start()
    local("dyc", dy_in.at[rows(z * ch, ch)], dy_ch).start()
    local("dy_own", dy_in, ob.at[0, rows(c * td, td)]).start()

    def ag_x(a, buf, src, h):
        push((a, "x", h), src.at[pl.ds(h * half, half)], buf.at[q, c, pl.ds(h * half, half)], to_x)

    def ag_y(a, buf, src, h):
        push((a, "y", h), src.at[pl.ds(h * half, half)], buf.at[q, c, pl.ds(h * half, half)], to_y)

    def piece(buf, block, core, h):
        return buf.at[block, core, pl.ds(h * half, half)]

    def share(a, buf, j, block, h):
        key = (a, "c", j, h)
        push(key, piece(buf, block, c, h), piece(buf, block, c, h), to_c, lambda: remote(key, piece(buf, block, c, h), piece(buf, block, c, h), to_c))

    def ag_relay_x(a, buf):
        got((a, "y", 0), piece(buf, qy, c, 0))
        push((a, "dx"), piece(buf, qy, c, 0), piece(buf, qy, c, 0), to_x)
        share(a, buf, 1, qy, 0)

    def ag_relay_y(a, buf):
        got((a, "x", 1), piece(buf, qx, c, 1))
        push((a, "dy"), piece(buf, qx, c, 1), piece(buf, qx, c, 1), to_y)
        share(a, buf, 0, qx, 1)

    def ag_share_rest(a, buf):
        got((a, "x", 0), piece(buf, qx, c, 0))
        share(a, buf, 0, qx, 0)
        got((a, "y", 1), piece(buf, qy, c, 1))
        share(a, buf, 1, qy, 1)

    def ag_share_diag(a, buf):
        got((a, "dx"), piece(buf, qd, c, 0))
        share(a, buf, 2, qd, 0)
        got((a, "dy"), piece(buf, qd, c, 1))
        share(a, buf, 2, qd, 1)

    def block_of(j):
        return 2 * ((y + (j + 1) // 2) % 2) + (x + (j + 1) % 2) % 2

    def ag_wait_partner(a, buf, j):
        base = ids.setdefault((a, "c", 0, 0), len(ids))
        for jj in range(3):
            for h in range(2):
                assert ids.setdefault((a, "c", jj, h), len(ids)) == base + 2 * jj + h
        for h in range(2):
            ref = piece(buf, block_of(j), co, h)
            i = base + 2 * j + h
            pltpu.make_async_remote_copy(src_ref=ref, dst_ref=ref, send_sem=ssem.at[i], recv_sem=rsem.at[i], device_id=to_c, device_id_type=MESH).wait_recv()

    for a in ("n0", "o1", "n1", "o0"):
        for j in range(3):
            for h in range(2):
                ids.setdefault((a, "c", j, h), len(ids))

    def fwd(l, n_ref, g_ref):
        def step(i, carry):
            w = cols(i * tile, tile)
            a = mm(n_ref[...], wg[l, :, w], 1, 0).astype(BF16)
            b = mm(n_ref[...], wu[l, :, w], 1, 0).astype(BF16)
            a_t[:, w] = a
            b_t[:, w] = b
            if g_ref is not None:
                a_f = a.astype(F32)
                g_ref[:, w] = (a_f * jax.nn.sigmoid(a_f) * b.astype(F32)).astype(BF16)
            return carry

        lax.fori_loop(0, hh // tile, step, 0)

    def down(l, g_ref):
        def step(i, carry):
            w = cols(i * tile, tile)
            part[:, w] = mm(g_ref[...], wd[l, :, w], 1, 0)
            return carry

        lax.fori_loop(0, d // tile, step, 0)

    def bwd_hidden(l, o_ref):
        tile = min(512, fb)

        def step(i, carry):
            w = cols(i * tile, tile)
            q_f = mm(o_ref[...], wd[l, rows(i * tile, tile)], 1, 1).astype(BF16).astype(F32)
            a_f = a_t[:, w].astype(F32)
            b_f = b_t[:, w].astype(F32)
            s = jax.nn.sigmoid(a_f)
            g_t[:, w] = (a_f * s * b_f).astype(BF16)
            a_t[:, w] = (q_f * b_f * s * (1.0 + a_f * (1.0 - s))).astype(BF16)
            b_t[:, w] = (q_f * a_f * s).astype(BF16)
            return carry

        lax.fori_loop(0, hh // tile, step, 0)

    def m_tile(l, i):
        return mm(a_t[...], wg[l, rows(i * tile, tile)], 1, 1) + mm(b_t[...], wu[l, rows(i * tile, tile)], 1, 1)

    def m_part(l):
        def step(i, carry):
            part[:, cols(i * tile, tile)] = m_tile(l, i)
            return carry

        lax.fori_loop(0, d // tile, step, 0)

    def weight_grads(n_ref, o_ref):
        def step(i, carry):
            w = rows(i * tile, tile)
            n_rows = n_ref[:, cols(x * hh_rows + i * tile, tile)]
            acc_g[w, :] += mm(n_rows, a_t[...], 0, 0)
            acc_u[w, :] += mm(n_rows, b_t[...], 0, 0)
            return carry

        hh_rows = 2 * rb
        lax.fori_loop(0, hh_rows // tile, step, 0)

        def step_d(i, carry):
            acc_d[rows(i * tile_d, tile_d), :] += mm(g_t[:, cols(x * fb + i * tile_d, tile_d)], o_ref[...], 0, 0)
            return carry

        tile_d = min(256, fb)
        lax.fori_loop(0, fb // tile_d, step_d, 0)

    def zero_acc():
        for ref in (acc_g, acc_u, acc_d):
            def step(i, carry, ref=ref):
                ref[rows(i * 16, 16), :] = jnp.zeros((16, ref.shape[1]), F32)
                return carry

            lax.fori_loop(0, ref.shape[0] // 16, step, 0)

    def rinv(h_f):
        return lax.rsqrt(jnp.mean(h_f * h_f, axis=-1, keepdims=True) + 1e-6)

    def core_sum(key):
        push(key, part.at[rows(co * td, td)], from_core, to_c)
        got(key, from_core)

        def step(i, carry):
            r = rows(c * td + i * 16, 16)
            part[r, :] = part[r, :] + from_core[rows(i * 16, 16), :]
            return carry

        lax.fori_loop(0, td // 16, step, 0)

    def z_send(key):
        for dz in (2, 1, 3):
            zt = (z + dz) % 4
            push((key, dz), part.at[rows(c * td + zt * ch, ch)], from_z.at[dz - 1], to_z(dz))

    def z_got(key):
        for dz in (1, 3, 2):
            got((key, dz), from_z.at[dz - 1])

    def z_sum(i):
        r = rows(i * 16, 16)
        return part[rows(c * td + z * ch + i * 16, 16), :] + from_z[0, r, :] + from_z[1, r, :] + from_z[2, r, :]

    def sum_sends_done(ckey, zkey):
        send_done(ckey)
        for dz in (1, 2, 3):
            send_done((zkey, dz))

    def z_gather(key, ref):
        for dz in (2, 1, 3):
            own = ref.at[rows(c * td + z * ch, ch)]
            push((key, dz), own, own, to_z(dz))

    def z_gathered(key, ref):
        for dz in (1, 3, 2):
            got((key, dz), ref.at[rows(c * td + ((z + 4 - dz) % 4) * ch, ch)])

    loads[0].wait()

    def n0_step(i, carry):
        h_f = n_own[rows(i * 16, 16), :].astype(F32)
        nb[0, rows(c * td + i * 16, 16), :] = (h_f * rinv(h_f) * gain[0:1, :]).astype(BF16)
        return carry

    lax.fori_loop(0, td // 16, n0_step, 0)
    n0_mine = nb.at[0, rows(c * td, td)]
    push("n0p", n0_mine, n0_mine, to_c)
    keep = local("n0k", n0_mine, n0_buf.at[q, c])
    keep.start()
    keep.wait()
    ag_y("n0", n0_buf, n0_buf.at[q, c], 0)
    for h in range(2):
        ag_x("n0", n0_buf, n0_buf.at[q, c], h)
    for h in range(2):
        ag_x("o1", o1_buf, dy_in, h)

    def relay_gu(l, m, xb):
        ref = wview(gu[m][1], l, 2 * xo + cs, xb)
        got(("wx", l, m, xb), ref)
        push(("wy", l, m, xb), ref, ref, to_y)

    def relay_d(l, k):
        ref = wd.at[l, rows(xo * fb + y * (fb // 2) + k * (fb // 4), fb // 4)]
        got(("wdx", l, k), ref)
        push(("wdy", l, k), ref, ref, to_y)

    def have_gu(l):
        for m in range(2):
            for xb in range(2):
                local(("w", l, m, xb), wsrc(gu[m][0], l, xb, c), wview(gu[m][1], l, f, xb)).wait()
                got(("wc", l, m, xb), wview(gu[m][1], l, 2 * x + co, xb))
                got(("wy", l, m, xb), wview(gu[m][1], l, 2 * xo + cso, xb))

    def have_d(l):
        local(("wd", l), wd_in.at[l], wd.at[l, rows(x * fb, fb)]).wait()
        for k in range(2):
            got(("wdy", l, k), wd.at[l, rows(xo * fb + yo * (fb // 2) + k * (fb // 4), fb // 4)])

    for m in range(2):
        for xb in range(2):
            relay_gu(0, m, xb)
    got("n0p", nb.at[0, rows(co * td, td)])
    keep2 = local("n0k2", nb.at[0, rows(co * td, td)], n0_buf.at[q, co])
    keep2.start()
    have_gu(0)
    fwd(0, nb.at[0], g_t)
    saves = [local("sa", a_t, a_save.at[q]), local("sb", b_t, b_save.at[q])]
    for s in saves:
        s.start()
    relay_d(0, 0)
    relay_d(0, 1)
    have_d(0)
    down(0, g_t)
    core_sum("d0")
    z_send("z0")
    for m in range(2):
        for xb in range(2):
            relay_gu(1, m, xb)
    for k in range(2):
        relay_d(1, k)
    ag_y("n0", n0_buf, n0_buf.at[q, c], 1)

    local("xc", x_in.at[rows(z * ch, ch)], x_ch).wait()
    z_got("z0")

    def h1_step(i, carry):
        r = rows(i * 16, 16)
        h1 = (x_ch[r, :].astype(F32) + z_sum(i)).astype(BF16)
        h1_ch[r, :] = h1
        h_f = h1.astype(F32)
        n_own[rows(c * td + z * ch + i * 16, 16), :] = (h_f * rinv(h_f) * gain[1:2, :]).astype(BF16)
        return carry

    lax.fori_loop(0, ch // 16, h1_step, 0)
    z_gather("n1z", n_own)
    ag_relay_y("n0", n0_buf)
    ag_relay_x("n0", n0_buf)
    for h in range(2):
        ag_y("o1", o1_buf, dy_in, h)
    z_gathered("n1z", n_own)
    n1_mine = n_own.at[rows(c * td, td)]
    push("n1p", n1_mine, n1_mine, to_c)
    for h in range(2):
        ag_x("n1", n1_buf, n1_mine, h)
        ag_y("n1", n1_buf, n1_mine, h)
    got("dyp", o1_buf.at[q, co])
    dy_other = local("dy_other", o1_buf.at[q, co], ob.at[0, rows(co * td, td)])
    dy_other.start()
    got("n1p", n_own.at[rows(co * td, td)])

    have_gu(1)
    for s in saves:
        s.wait()
    fwd(1, n_own, g_keep)
    local("dy_own", dy_in, ob.at[0, rows(c * td, td)]).wait()
    dy_other.wait()
    have_d(1)
    bwd_hidden(1, ob.at[0])
    sum_sends_done("d0", "z0")
    m_part(1)
    core_sum("d1")
    z_send("z1")
    zero_acc()
    weight_grads(n_own, ob.at[0])
    keep2.wait()
    send_done("n0p")

    ag_share_rest("n0", n0_buf)
    ag_share_diag("n0", n0_buf)

    def load_n(buf, j, s):
        return local("ln", buf.at[j], nb_block.at[s])

    nb_block = nb

    def stage(buf, block, slot_ref, key):
        for core in range(2):
            local((key, core), buf.at[block, core], slot_ref.at[pl.ds(core * td, td)]).start()

    def staged(buf, block, slot_ref, key):
        for core in range(2):
            local((key, core), buf.at[block, core], slot_ref.at[pl.ds(core * td, td)]).wait()

    def f0_step(j, carry):
        blk = block_of(j)
        ag_wait_partner("n0", n0_buf, j)
        stage(n0_buf, blk, nb.at[0], "sn")
        staged(n0_buf, blk, nb.at[0], "sn")
        fwd(0, nb.at[0], None)
        out = (local("sa", a_t, a_save.at[blk]), local("sb", b_t, b_save.at[blk]))
        for s in out:
            s.start()
        for s in out:
            s.wait()
        return carry

    lax.fori_loop(0, 3, f0_step, 0)
    ag_relay_x("o1", o1_buf)
    ag_relay_y("o1", o1_buf)
    ag_share_rest("o1", o1_buf)

    local("dyc", dy_in.at[rows(z * ch, ch)], dy_ch).wait()
    z_got("z1")

    def e_step(i, dg1):
        r = rows(i * 16, 16)
        m = z_sum(i)
        h_f = h1_ch[r, :].astype(F32)
        r_inv = rinv(h_f)
        xh = h_f * r_inv
        v = m * gain[1:2, :]
        e = dy_ch[r, :].astype(F32) + r_inv * (v - xh * jnp.mean(v * xh, axis=-1, keepdims=True))
        o_own[rows(c * td + z * ch + i * 16, 16), :] = e.astype(BF16)
        return dg1 + jnp.sum(m * xh, axis=0, keepdims=True)

    dg[1:2, :] = lax.fori_loop(0, ch // 16, e_step, jnp.zeros((1, d), F32))
    z_gather("o0z", o_own)
    sum_sends_done("d1", "z1")
    down(1, g_keep)
    core_sum("d2")
    ag_relay_x("n1", n1_buf)
    ag_relay_y("n1", n1_buf)
    ag_share_diag("o1", o1_buf)
    ag_share_rest("n1", n1_buf)
    z_gathered("o0z", o_own)
    o0_mine = o_own.at[rows(c * td, td)]
    push("o0p", o0_mine, o0_mine, to_c)
    for h in range(2):
        ag_x("o0", o0_buf, o0_mine, h)
        ag_y("o0", o0_buf, o0_mine, h)
    z_send("z2")

    def l1_step(j, carry):
        blk = block_of(j)

        @pl.when(j == 2)
        def _():
            ag_share_diag("n1", n1_buf)

        ag_wait_partner("n1", n1_buf, j)
        ag_wait_partner("o1", o1_buf, j)
        stage(n1_buf, blk, nb.at[0], "sn")
        stage(o1_buf, blk, ob.at[0], "so")
        staged(n1_buf, blk, nb.at[0], "sn")
        staged(o1_buf, blk, ob.at[0], "so")
        fwd(1, nb.at[0], None)
        bwd_hidden(1, ob.at[0])
        weight_grads(nb.at[0], ob.at[0])
        return carry

    lax.fori_loop(0, 3, l1_step, 0)

    def grads_out(l):
        for i, (acc, out) in enumerate(((acc_g, dwg_out), (acc_u, dwu_out))):
            for xb in range(2):
                dst = out.at[l, :, cols((2 * xb + c) * fb, fb)]
                push(("q", l, i, xb), acc.at[rows(co * rb, rb), cols(xb * fb, fb)], dst, to_c)
                local(("qo", l, i, xb), acc.at[rows(c * rb, rb), cols(xb * fb, fb)], dst).start()
        local(("qd", l), acc_d, dwd_out.at[l]).start()

    def grads_out_done(l):
        for i, (acc, out) in enumerate(((acc_g, dwg_out), (acc_u, dwu_out))):
            for xb in range(2):
                dst = out.at[l, :, cols((2 * xb + c) * fb, fb)]
                local(("qo", l, i, xb), acc.at[rows(c * rb, rb), cols(xb * fb, fb)], dst).wait()
                send_done(("q", l, i, xb))
                got(("q", l, i, xb), out.at[l, :, cols((2 * xb + co) * fb, fb)])
        local(("qd", l), acc_d, dwd_out.at[l]).wait()

    grads_out(1)
    got("o0p", o_own.at[rows(co * td, td)])
    o_keep = [local(("ok", k), o_own.at[pl.ds(k * td, td)], o0_buf.at[q, k]) for k in range(2)]
    for s in o_keep:
        s.start()
    ag_relay_x("o0", o0_buf)
    ag_relay_y("o0", o0_buf)
    ag_share_rest("o0", o0_buf)
    got("xp", x_part)
    for key in ["n1p"] + [("n1z", dz) for dz in (1, 2, 3)] + [("n1", axis, h) for axis in "xy" for h in range(2)]:
        send_done(key)
    xl = [local("xl0", x_in, n_own.at[rows(c * td, td)]), local("xl1", x_part, n_own.at[rows(co * td, td)])]
    for s in xl:
        s.start()
    for s in xl:
        s.wait()

    def r_step(i, carry):
        h_f = n_own[rows(i * 16, 16), :].astype(F32)
        r_own[rows(i * 16, 16), :] = jnp.broadcast_to(rinv(h_f), (16, 128))
        return carry

    lax.fori_loop(0, t2 // 16, r_step, 0)
    for s in o_keep:
        s.wait()
    grads_out_done(1)
    zero_acc()

    def l0_step(j, carry):
        blk = 2 * ((y + j // 2) % 2) + (x + j % 2) % 2

        @pl.when(j == 2)
        def _():
            ag_share_diag("o0", o0_buf)

        @pl.when(j > 0)
        def _():
            ag_wait_partner("o0", o0_buf, j - 1)

        stage(n0_buf, blk, nb.at[0], "sn")
        stage(o0_buf, blk, ob.at[0], "so")
        back = (local("sa", a_save.at[blk], a_t), local("sb", b_save.at[blk], b_t))
        for s in back:
            s.start()
        for s in back:
            s.wait()
        staged(n0_buf, blk, nb.at[0], "sn")
        staged(o0_buf, blk, ob.at[0], "so")
        bwd_hidden(0, ob.at[0])

        @pl.when(j == 0)
        def _():
            def dg_step(i, carry):
                w = cols(i * tile, tile)
                m = m_tile(0, i)
                xh = n_own[:, w].astype(F32) * r_own[:, 0:1]
                dg[0:1, w] = jnp.sum(m * xh, axis=0, keepdims=True)
                return carry

            lax.fori_loop(0, d // tile, dg_step, 0)
            push("gc", dg, dg_core, to_c, lambda: remote("gc", dg, dg_core, to_c))

        weight_grads(nb.at[0], ob.at[0])
        return carry

    lax.fori_loop(0, 4, l0_step, 0)
    grads_out(0)

    got("gc", dg_core)
    send_done("gc")
    dg[...] = dg[...] + dg_core[...]
    push("gx", dg, dg_x, to_x)
    got("gx", dg_x)
    send_done("gx")
    dg[...] = dg[...] + dg_x[...]
    push("gy", dg, dg_y, to_y)
    got("gy", dg_y)
    send_done("gy")
    dg_z[z] = dg[...] + dg_y[...]
    for dz in (1, 2, 3):
        push(("gz", dz), dg_z.at[z], dg_z.at[z], to_z(dz))

    z_got("z2")

    def y_step(i, carry):
        r = rows(i * 16, 16)
        y_ch[r, :] = (h1_ch[r, :].astype(F32) + z_sum(i)).astype(BF16)
        return carry

    lax.fori_loop(0, ch // 16, y_step, 0)
    y_keep = local("yk", y_ch, y_out.at[rows(z * ch, ch)])
    y_keep.start()
    for dz in (1, 2, 3):
        push(("yz", dz), y_ch, y_out.at[rows(z * ch, ch)], to_z(dz))
    for dz in (1, 2, 3):
        got(("gz", dz), dg_z.at[(z + 4 - dz) % 4])
    dgain_out[...] = dg_z[0] + dg_z[1] + dg_z[2] + dg_z[3]
    for dz in (1, 2, 3):
        got(("yz", dz), y_out.at[rows(((z + 4 - dz) % 4) * ch, ch)])
    y_keep.wait()
    grads_out_done(0)
    for key in list(sent):
        send_done(key)


def make_call(td, d, rb, hs):
    fb = hs // 4
    hh, t2, ch = 2 * fb, 2 * td, td // 4
    shape = jax.ShapeDtypeStruct
    hbm = pl.BlockSpec(memory_space=pl.ANY)
    vmem = pl.BlockSpec(memory_space=pltpu.VMEM)
    block = shape((4, 2, td, d), BF16)
    outs = [
        shape((td, d), BF16), shape((2, rb, hs), F32), shape((2, rb, hs), F32), shape((2, fb, d), F32), shape((2, d), F32),
        block, block, block, block, shape((4, t2, hh), BF16), shape((4, t2, hh), BF16), shape((td, d), BF16),
    ]
    scratch = [
        pltpu.VMEM((2, d, hh), BF16), pltpu.VMEM((2, d, hh), BF16), pltpu.VMEM((2, hh, d), BF16),
        pltpu.VMEM((2 * rb, hh), F32), pltpu.VMEM((2 * rb, hh), F32), pltpu.VMEM((fb, d), F32),
        pltpu.VMEM((1, t2, d), BF16), pltpu.VMEM((1, t2, d), BF16),
        pltpu.VMEM((t2, hh), BF16), pltpu.VMEM((t2, hh), BF16), pltpu.VMEM((t2, hh), BF16), pltpu.VMEM((t2, hh), BF16),
        pltpu.VMEM((t2, d), F32), pltpu.VMEM((td, d), F32), pltpu.VMEM((3, ch, d), F32),
        pltpu.VMEM((t2, d), BF16), pltpu.VMEM((t2, d), BF16),
        pltpu.VMEM((ch, d), BF16), pltpu.VMEM((ch, d), BF16), pltpu.VMEM((ch, d), BF16), pltpu.VMEM((ch, d), BF16),
        pltpu.VMEM((t2, 128), F32),
        pltpu.VMEM((2, d), F32), pltpu.VMEM((2, d), F32), pltpu.VMEM((2, d), F32), pltpu.VMEM((2, d), F32), pltpu.VMEM((4, 2, d), F32),
        pltpu.SemaphoreType.DMA((NSEM,)), pltpu.SemaphoreType.DMA((NSEM,)), pltpu.SemaphoreType.DMA((NLOC,)),
    ]
    return pl.pallas_call(
        kernel,
        out_shape=outs,
        in_specs=[hbm] * 5 + [vmem],
        out_specs=[hbm] * 4 + [vmem] + [hbm] * 7,
        scratch_shapes=scratch,
        compiler_params=pltpu.CompilerParams(collective_id=0, has_side_effects=True, vmem_limit_bytes=67043328),
    )


def solution(mesh):
    tok_spec = P(("replica", "fsdp"), None)
    wide_spec = P(None, "fsdp", "tensor")
    down_spec = P(None, ("tensor", "fsdp"), None)
    gain_spec = P(None, None)

    def device_fn(x_loc, dy_loc, w_gate, w_up, w_down, norm_gain):
        call = make_call(x_loc.shape[0], x_loc.shape[1], w_gate.shape[1], w_gate.shape[2])
        return tuple(call(x_loc, dy_loc, w_gate, w_up, w_down, norm_gain)[:5])

    return jax.shard_map(device_fn, mesh=mesh, in_specs=(tok_spec, tok_spec, wide_spec, wide_spec, down_spec, gain_spec), out_specs=(tok_spec, wide_spec, wide_spec, down_spec, gain_spec), check_vma=False)
```

```python
import jax
import jax.numpy as jnp
from jax import lax
from jax.experimental import pallas as pl
from jax.experimental.pallas import tpu as pltpu
from jax.sharding import PartitionSpec as P

F32 = jnp.float32
BF16 = jnp.bfloat16
MESH = pl.DeviceIdType.MESH
NSEM = 300
NLOC = 64


def mm(lhs, rhs, ldim, rdim):
    return lax.dot_general(lhs, rhs, (((ldim,), (rdim,)), ((), ())), preferred_element_type=F32)


def kernel(
    x_in, dy_in, wg_in, wu_in, wd_in, gain,
    y_out, dwg_out, dwu_out, dwd_out, dgain_out, n0_buf, n1_buf, o1_buf, o0_buf, a_save, b_save, x_part,
    wg, wu, wd, acc_g, acc_u, acc_d, nb, ob, a_t, b_t, g_t, g_keep, part, from_core, from_z, n_own, o_own,
    x_ch, dy_ch, h1_ch, y_ch, r_own, dg, dg_core, dg_x, dg_y, dg_z, ssem, rsem, lsem,
):
    td, d = x_in.shape
    rb = wg_in.shape[1]
    fb = wg_in.shape[2] // 4
    hh = 2 * fb
    t2, ch, half = 2 * td, td // 4, td // 2
    hc = ch // 2
    tile = min(512, fb)
    z = lax.axis_index("tensor")
    y = lax.axis_index("replica")
    f = lax.axis_index("fsdp")
    x, c = f // 2, f % 2
    xo, yo, co = 1 - x, 1 - y, 1 - c
    q, qx, qy, qd = 2 * y + x, 2 * y + xo, 2 * yo + x, 2 * yo + xo
    cs = (c + y) % 2
    cso = 1 - cs
    to_c, to_x, to_xs, to_y = {"fsdp": 2 * x + co}, {"fsdp": 2 * xo + c}, {"fsdp": 2 * xo + cs}, {"replica": yo}
    inner = ((z + 1) // 2) % 2
    outer = 1 - inner
    up = z // 2
    pair = z + 1 - 2 * (z % 2)
    far_outer, far_inner = 3 - 3 * up, 2 - up
    order = (outer * far_outer + inner * pair, outer * far_inner + inner * far_outer, outer * pair + inner * far_inner, z)

    def at_z(i):
        return {"tensor": i}

    def z_other(k):
        return (z + 4 + k * (1 - 2 * up)) % 4

    def rows(start, size):
        return pl.ds(pl.multiple_of(start, size if size % 16 == 0 else 8), size)

    def cols(start, size):
        return pl.ds(pl.multiple_of(start, 128), size)

    ids, lids, sent = {}, {}, {}

    def sid(key):
        i = ids.setdefault(key, len(ids))
        assert i < NSEM, i
        return i

    def name_of(key):
        return key if isinstance(key, str) else "_".join(map(str, key))

    def copy_of(skey, rkey, src, dst, dev):
        return pltpu.make_async_remote_copy(
            src_ref=src, dst_ref=dst, send_sem=ssem.at[sid(skey)], recv_sem=rsem.at[rkey if not isinstance(rkey, (str, tuple)) else sid(rkey)],
            device_id=dev, device_id_type=MESH,
        )

    def push(key, make, rkey=None):
        copy_of(key, key if rkey is None else rkey, *make()).start()
        sent[key] = make

    def got(key, dst):
        with jax.named_scope("got_" + (name_of(key) if isinstance(key, (str, tuple)) else "dyn")):
            copy_of("none", key, dst, dst, to_c).wait_recv()

    def send_done(key):
        copy_of(key, key, *sent.pop(key)()).wait_send()

    def local(key, src, dst):
        i = lids.setdefault(key, len(lids))
        assert i < NLOC
        return pltpu.make_async_copy(src, dst, lsem.at[i])

    def scoped(fn):
        def run(*args):
            with jax.named_scope(fn.__name__):
                return fn(*args)

        return run

    gu = ((wg_in, wg), (wu_in, wu))
    pieces = (2, 2)

    def wview(m, l, row, xb, k=0, n=1):
        return gu[m][1].at[l, rows(row * rb + k * (rb // n), rb // n), cols(xb * fb, fb)]

    def wsrc(m, l, xb, core, k=0, n=1):
        return gu[m][0].at[l, pl.ds(k * (rb // n), rb // n), cols((2 * xb + core) * fb, fb)]

    def push_w(l):
        n = pieces[l]
        for m in range(2):
            for xb in range(2):
                for k in range(n):
                    push(("wx", l, m, xb, k), lambda m=m, xb=xb, k=k: (wsrc(m, l, xb, cs, k, n), wview(m, l, f, xb, k, n), to_xs))
        for k in range(4):
            r0 = y * (fb // 2) + k * (fb // 8)
            push(("wdx", l, k), lambda r0=r0: (wd_in.at[l, rows(r0, fb // 8)], wd.at[l, rows(x * fb + r0, fb // 8)], to_x))

    def push_wc(l):
        for m in range(2):
            for xb in range(2):
                push(("wc", l, m, xb), lambda m=m, xb=xb: (wsrc(m, l, xb, co), wview(m, l, f, xb), to_c))
                local(("w", l, m, xb), wsrc(m, l, xb, c), wview(m, l, f, xb)).start()
        local(("wd", l), wd_in.at[l], wd.at[l, rows(x * fb, fb)]).start()

    def relay_gu(l, m, xb):
        n = pieces[l]
        for k in range(n):
            ref = lambda k=k: wview(m, l, 2 * xo + cs, xb, k, n)
            got(("wx", l, m, xb, k), ref())
            push(("wy", l, m, xb, k), lambda k=k: (ref(k), ref(k), to_y))

    def relay_d(l, k):
        ref = lambda: wd.at[l, rows(xo * fb + y * (fb // 2) + k * (fb // 8), fb // 8)]
        got(("wdx", l, k), ref())
        push(("wdy", l, k), lambda: (ref(), ref(), to_y))

    def have_gu(l, m, xb):
        n = pieces[l]
        local(("w", l, m, xb), wsrc(m, l, xb, c), wview(m, l, f, xb)).wait()
        got(("wc", l, m, xb), wview(m, l, 2 * x + co, xb))
        for k in range(n):
            got(("wy", l, m, xb, k), wview(m, l, 2 * xo + cso, xb, k, n))

    def have_d_own(l):
        local(("wd", l), wd_in.at[l], wd.at[l, rows(x * fb, fb)]).wait()

    def have_d(l):
        for k in range(4):
            got(("wdy", l, k), wd.at[l, rows(xo * fb + yo * (fb // 2) + k * (fb // 8), fb // 8)])

    def piece(buf, block, core, start, size):
        return buf.at[block, core, pl.ds(start, size)]

    def chunk(buf, block, core, zi):
        return buf.at[block, core, rows(zi * ch, ch)]

    def part_id(a, j):
        base = sid((a, "p", 0))
        for jj in range(3):
            assert sid((a, "p", jj)) == base + jj
        return base + j

    def share(a, j, tag, ref):
        push((a, "s", j, tag), lambda: (ref(), ref(), to_c), (a, "p", j))

    def ag_x(a, buf, src, h):
        push((a, "x", h), lambda: (src().at[pl.ds(h * half, half)], piece(buf, q, c, h * half, half), to_x))

    def ag_y(a, buf, src, h):
        push((a, "y", h), lambda: (src().at[pl.ds(h * half, half)], piece(buf, q, c, h * half, half), to_y))

    def ag_yc(a, buf, src):
        push((a, "yc"), lambda: (src().at[rows(z * ch, ch)], chunk(buf, q, c, z), to_y))

    def zb_id(a, zi):
        base = sid((a, "zb", 0))
        for i in range(4):
            assert sid((a, "zb", i)) == base + i
        return base + zi

    def ag_spread(a, buf):
        got((a, "yc"), chunk(buf, qy, c, z))
        for k in (1, 2, 3):
            push((a, "zs", k), lambda: (chunk(buf, qy, c, z), chunk(buf, qy, c, z), at_z(z_other(k))), zb_id(a, z))

    def ag_spread_got(a, buf, cut):
        for k in (1, 2, 3):
            with jax.named_scope("got_zb_" + a):
                got(zb_id(a, z_other(k)), chunk(buf, qy, c, z_other(k)))
        share(a, 0, 0, lambda: buf.at[qy, c])

    def ag_dx(a, buf, cut):
        push((a, "dx"), lambda: (piece(buf, qy, c, 0, cut), piece(buf, qy, c, 0, cut), to_x))

    def ag_got_y(a, buf, h):
        got((a, "y", h), piece(buf, qy, c, h * half, half))
        share(a, 0, h, lambda: piece(buf, qy, c, h * half, half))
        if h == 0:
            ag_dx(a, buf, half)

    def diag_piece(h, cut):
        start = max(cut, h * half)
        return start, (h + 1) * half - start

    def ag_got_x(a, buf, h, cut):
        got((a, "x", h), piece(buf, qx, c, h * half, half))
        start, size = diag_piece(h, cut)
        if size:
            push((a, "dy", h), lambda: (piece(buf, qx, c, start, size), piece(buf, qx, c, start, size), to_y))
        share(a, 1, h, lambda: piece(buf, qx, c, h * half, half))

    def ag_got_dx(a, buf, cut):
        got((a, "dx"), piece(buf, qd, c, 0, cut))
        share(a, 2, "x", lambda: piece(buf, qd, c, 0, cut))

    def ag_got_dy(a, buf, h, cut):
        start, size = diag_piece(h, cut)
        if size:
            got((a, "dy", h), piece(buf, qd, c, start, size))
            share(a, 2, h, lambda: piece(buf, qd, c, start, size))

    def block_of(j):
        return 2 * ((y + (j + 1) % 2) % 2) + (x + (j + 1) // 2) % 2

    def partner_has(a, buf, j):
        with jax.named_scope("got_p_" + a):
            got(part_id(a, j), buf.at[block_of(j), co])

    for a in ("n0", "o1", "n1", "o0"):
        for j in range(3):
            sid((a, "p", j))
        for i in range(4):
            sid((a, "zb", i))

    def fwd_tile(l, n_ref, g_ref, i):
        w = cols(i * tile, tile)
        a = mm(n_ref[...], wg[l, :, w], 1, 0).astype(BF16)
        b = mm(n_ref[...], wu[l, :, w], 1, 0).astype(BF16)
        a_t[:, w] = a
        b_t[:, w] = b
        if g_ref is not None:
            a_f = a.astype(F32)
            g_ref[:, w] = (a_f * jax.nn.sigmoid(a_f) * b.astype(F32)).astype(BF16)

    @scoped
    def fwd(l, n_ref, g_ref):
        def step(i, carry):
            fwd_tile(l, n_ref, g_ref, i)
            return carry

        lax.fori_loop(0, hh // tile, step, 0)

    @scoped
    def down_rows(l, g_ref, core):
        def step(i, carry):
            w = cols(i * tile, tile)
            part[rows(core * td, td), w] = mm(g_ref[rows(core * td, td), :], wd[l, :, w], 1, 0)
            return carry

        lax.fori_loop(0, d // tile, step, 0)

    @scoped
    def m_rows(l, core):
        r = rows(core * td, td)

        def step(i, carry):
            w = rows(i * tile, tile)
            part[r, cols(i * tile, tile)] = mm(a_t[r, :], wg[l, w], 1, 1) + mm(b_t[r, :], wu[l, w], 1, 1)
            return carry

        lax.fori_loop(0, d // tile, step, 0)

    @scoped
    def bwd_hidden(l, o_ref):
        def step(i, carry):
            w = cols(i * tile, tile)
            q_f = mm(o_ref[...], wd[l, rows(i * tile, tile)], 1, 1).astype(BF16).astype(F32)
            a_f = a_t[:, w].astype(F32)
            b_f = b_t[:, w].astype(F32)
            s = jax.nn.sigmoid(a_f)
            g_t[:, w] = (a_f * s * b_f).astype(BF16)
            a_t[:, w] = (q_f * b_f * s * (1.0 + a_f * (1.0 - s))).astype(BF16)
            b_t[:, w] = (q_f * a_f * s).astype(BF16)
            return carry

        lax.fori_loop(0, hh // tile, step, 0)

    @scoped
    def weight_grads(n_ref, o_ref):
        def step(i, carry):
            w = rows(i * tile, tile)
            n_rows = n_ref[:, cols(x * (2 * rb) + i * tile, tile)]
            acc_g[w, :] += mm(n_rows, a_t[...], 0, 0)
            acc_u[w, :] += mm(n_rows, b_t[...], 0, 0)
            return carry

        lax.fori_loop(0, 2 * rb // tile, step, 0)
        tile_d = min(256, fb)

        def step_d(i, carry):
            acc_d[rows(i * tile_d, tile_d), :] += mm(g_t[:, cols(x * fb + i * tile_d, tile_d)], o_ref[...], 0, 0)
            return carry

        lax.fori_loop(0, fb // tile_d, step_d, 0)

    @scoped
    def zero_acc():
        for ref in (acc_g, acc_u, acc_d):
            def step(i, carry, ref=ref):
                ref[rows(i * 16, 16), :] = jnp.zeros((16, ref.shape[1]), F32)
                return carry

            lax.fori_loop(0, ref.shape[0] // 16, step, 0)

    def rinv(h_f):
        return lax.rsqrt(jnp.mean(h_f * h_f, axis=-1, keepdims=True) + 1e-6)

    def core_push(key):
        for k in range(4):
            push((key, "c", k), lambda k=k: (part.at[rows(co * td + order[k] * ch, ch)], from_core.at[rows(order[k] * ch, ch)], to_c))

    def z_ids(key):
        base = sid((key, "A", 0))
        for h in range(2):
            for i, s in enumerate("ABCD"):
                assert sid((key, s, h)) == base + 4 * h + i
        return base

    def mine(zi, h):
        return part.at[rows(c * td + zi * ch + h * hc, hc)]

    def slot(i, h):
        return from_z.at[i, pl.ds(h * hc, hc)]

    @scoped
    def core_sum_send(key):
        z_ids(key)
        for k in range(4):
            got((key, "c", k), from_core.at[rows(order[k] * ch, ch)])

            def step(i, carry):
                r = order[k] * ch + i * 16
                mine_r = rows(c * td + r, 16)
                part[mine_r, :] = part[mine_r, :] + from_core[rows(r, 16), :]
                return carry

            lax.fori_loop(0, ch // 16, step, 0)
            if k == 0:
                for h in range(2):
                    push((key, "A", h), lambda: (mine(order[0], h), slot(0, h), at_z(pair)))
            elif k < 3:
                @pl.when(outer == 1)
                def _():
                    for h in range(2):
                        copy_of((key, "BC"[k - 1], h), (key, "BC"[k - 1], h), mine(order[k], h), slot(k, h), at_z(pair)).start()

                for h in range(2):
                    sent[(key, "BC"[k - 1], h)] = lambda: (mine(order[k], h), slot(k, h), at_z(pair))

    def z_relay(key, n, h):
        @pl.when(inner == 1)
        def _():
            got((key, "AB"[n], h), slot(n, h))
            zi = (far_outer, far_inner)[n]

            def step(i, carry):
                r = pl.ds(h * hc + i * 8, 8)
                from_z[n, pl.ds(pl.multiple_of(h * hc + i * 8, 8), 8), :] += part[rows(c * td + zi * ch + h * hc + i * 8, 8), :]
                return carry

            lax.fori_loop(0, hc // 8, step, 0)
            if n == 0:
                copy_of((key, "B", h), (key, "B", h), slot(0, h), slot(1, h), at_z(far_outer)).start()
            else:
                copy_of((key, "C", h), (key, "D", h), slot(1, h), slot(3, h), at_z(far_inner)).start()

    def z_got(key):
        base = z_ids(key)
        for h in range(2):
            for i in range(2):
                with jax.named_scope("got_" + key):
                    got(base + 4 * h + 2 * inner + i, slot(2 * inner + i, h))

    def z_sum(i):
        r = rows(i * 16, 16)
        return part[rows(c * td + z * ch + i * 16, 16), :] + from_z[2 * inner, r, :] + from_z[2 * inner + 1, r, :]

    def sum_sends_done(key):
        for k in range(4):
            send_done((key, "c", k))
        for s in "ABC":
            for h in range(2):
                send_done((key, s, h))

    def quarter(ref, core, zi):
        return ref.at[rows(core * td + zi * ch, ch)]

    def zg_id(key, zi):
        base = sid((key, "z", 0))
        for i in range(4):
            assert sid((key, "z", i)) == base + i
        return base + zi

    def z_gather(key, ref):
        for k in (1, 2, 3):
            push((key, "zs", k), lambda: (quarter(ref, c, z), quarter(ref, c, z), at_z(z_other(k))), zg_id(key, z))
        push((key, "s", 0), lambda: (quarter(ref, c, z), quarter(ref, c, z), to_c))

    def z_gathered(key, ref):
        for k in (1, 2, 3):
            with jax.named_scope("got_" + key):
                got(zg_id(key, z_other(k)), quarter(ref, c, z_other(k)))
            push((key, "s", k), lambda: (quarter(ref, c, z_other(k)), quarter(ref, c, z_other(k)), to_c))

    def z_gathered_partner(key, ref):
        got((key, "s", 0), quarter(ref, co, z))
        for k in (1, 2, 3):
            got((key, "s", k), quarter(ref, co, z_other(k)))

    def stage(buf, block, slot_ref, key):
        for core in range(2):
            local((key, core), buf.at[block, core], slot_ref.at[pl.ds(core * td, td)]).start()

    def staged(buf, block, slot_ref, key):
        for core in range(2):
            local((key, core), buf.at[block, core], slot_ref.at[pl.ds(core * td, td)]).wait()

    def save_ab(block):
        return (local("sa", a_t, a_save.at[block]), local("sb", b_t, b_save.at[block]))

    @scoped
    def f0_other(j):
        block = block_of(j)
        partner_has("n0", n0_buf, j)
        stage(n0_buf, block, nb.at[0], "sn")
        staged(n0_buf, block, nb.at[0], "sn")
        fwd(0, nb.at[0], None)
        for s in save_ab(block):
            s.start()
        for s in save_ab(block):
            s.wait()

    def grads_out(l):
        for i, (acc, out) in enumerate(((acc_g, dwg_out), (acc_u, dwu_out))):
            for xb in range(2):
                dst = lambda: out.at[l, :, cols((2 * xb + c) * fb, fb)]
                push(("q", l, i, xb), lambda: (acc.at[rows(co * rb, rb), cols(xb * fb, fb)], dst(), to_c))
                local(("qo", l, i, xb), acc.at[rows(c * rb, rb), cols(xb * fb, fb)], dst()).start()
        local(("qd", l), acc_d, dwd_out.at[l]).start()

    @scoped
    def grads_out_done(l):
        for i, (acc, out) in enumerate(((acc_g, dwg_out), (acc_u, dwu_out))):
            for xb in range(2):
                local(("qo", l, i, xb), acc.at[rows(c * rb, rb), cols(xb * fb, fb)], out.at[l, :, cols((2 * xb + c) * fb, fb)]).wait()
                send_done(("q", l, i, xb))
                got(("q", l, i, xb), out.at[l, :, cols((2 * xb + co) * fb, fb)])
        local(("qd", l), acc_d, dwd_out.at[l]).wait()

    barrier = pltpu.get_barrier_semaphore()
    for dev in (to_c, to_x, {"fsdp": 2 * xo + co}, to_y, at_z((z + 1) % 4), at_z((z + 2) % 4), at_z((z + 3) % 4)):
        pl.semaphore_signal(barrier, inc=1, device_id=dev, device_id_type=MESH)
    x_load = local("x", x_in, n_own.at[pl.ds(0, td)])
    x_load.start()
    with jax.named_scope("barrier"):
        pl.semaphore_wait(barrier, 7)

    dy_src = lambda: dy_in
    n0_src = lambda: n0_buf.at[q, c]
    n1_src = lambda: n_own.at[rows(c * td, td)]
    o0_src = lambda: o_own.at[rows(c * td, td)]
    cut = ch

    push_w(0)
    ag_yc("o1", o1_buf, dy_src)
    push_wc(0)
    x_load.wait()

    def n0_step(i, carry):
        h_f = n_own[rows(i * 16, 16), :].astype(F32)
        nb[0, rows(c * td + i * 16, 16), :] = (h_f * rinv(h_f) * gain[0:1, :]).astype(BF16)
        return carry

    lax.fori_loop(0, td // 16, n0_step, 0)
    n0_mine = lambda: nb.at[0, rows(c * td, td)]
    push("n0p", lambda: (n0_mine(), n0_mine(), to_c))
    keep = local("n0k", n0_mine(), n0_buf.at[q, c])
    keep.start()
    keep.wait()
    ag_yc("n0", n0_buf, n0_src)
    push_w(1)
    ag_x("o1", o1_buf, dy_src, 0)
    push("xp", lambda: (x_in, x_part, to_c))
    push("dyp", lambda: (dy_in, o1_buf.at[q, c], to_c))
    push_wc(1)
    local("xc", x_in.at[rows(z * ch, ch)], x_ch).start()
    local("dyc", dy_in.at[rows(z * ch, ch)], dy_ch).start()
    local("dy_own", dy_in, ob.at[0, rows(c * td, td)]).start()

    relay_gu(0, 0, 0)
    ag_spread("o1", o1_buf)
    ag_spread("n0", n0_buf)
    relay_gu(0, 0, 1)
    relay_gu(0, 1, 0)
    relay_gu(0, 1, 1)
    got("n0p", nb.at[0, rows(co * td, td)])
    keep2 = local("n0k2", nb.at[0, rows(co * td, td)], n0_buf.at[q, co])
    keep2.start()
    have_gu(0, 0, 0)
    have_gu(0, 1, 0)
    with jax.named_scope("fwd_tile0"):
        fwd_tile(0, nb.at[0], g_t, 0)
    relay_d(0, 0)
    relay_d(0, 1)
    have_gu(0, 0, 1)
    have_gu(0, 1, 1)
    with jax.named_scope("fwd_tile1"):
        for i in range(1, hh // tile):
            fwd_tile(0, nb.at[0], g_t, i)
    for s in save_ab(q):
        s.start()
    relay_d(0, 2)
    relay_d(0, 3)
    have_d_own(0)
    have_d(0)
    down_rows(0, g_t, co)
    core_push("d0")
    down_rows(0, g_t, c)
    core_sum_send("d0")
    relay_gu(1, 0, 0)
    z_relay("d0", 0, 0)
    relay_gu(1, 0, 1)
    z_relay("d0", 0, 1)
    keep2.wait()
    send_done("n0p")
    for s in save_ab(q):
        s.wait()
    ag_spread_got("n0", n0_buf, cut)
    ag_spread_got("o1", o1_buf, cut)
    z_relay("d0", 1, 0)
    relay_gu(1, 1, 0)
    z_relay("d0", 1, 1)
    relay_gu(1, 1, 1)

    local("xc", x_in.at[rows(z * ch, ch)], x_ch).wait()
    z_got("d0")
    sum_sends_done("d0")

    @scoped
    def h1_calc():
        def h1_step(i, carry):
            r = rows(i * 16, 16)
            h1 = (x_ch[r, :].astype(F32) + z_sum(i)).astype(BF16)
            h1_ch[r, :] = h1
            h_f = h1.astype(F32)
            n_own[rows(c * td + z * ch + i * 16, 16), :] = (h_f * rinv(h_f) * gain[1:2, :]).astype(BF16)
            return carry

        lax.fori_loop(0, ch // 16, h1_step, 0)

    h1_calc()
    z_gather("n1z", n_own)
    relay_d(1, 0)
    relay_d(1, 1)
    relay_d(1, 2)
    relay_d(1, 3)
    z_gathered("n1z", n_own)
    for h in range(2):
        ag_x("n1", n1_buf, n1_src, h)
    ag_x("o1", o1_buf, dy_src, 1)
    for h in range(2):
        ag_y("n1", n1_buf, n1_src, h)
    got("dyp", o1_buf.at[q, co])
    dy_other = local("dy_other", o1_buf.at[q, co], ob.at[0, rows(co * td, td)])
    dy_other.start()
    z_gathered_partner("n1z", n_own)

    for m in range(2):
        for xb in range(2):
            have_gu(1, m, xb)
    fwd(1, n_own, g_keep)
    local("dy_own", dy_in, ob.at[0, rows(c * td, td)]).wait()
    dy_other.wait()
    have_d_own(1)
    have_d(1)
    bwd_hidden(1, ob.at[0])
    m_rows(1, co)
    core_push("d1")
    m_rows(1, c)
    core_sum_send("d1")
    zero_acc()
    weight_grads(n_own, ob.at[0])
    ag_got_x("o1", o1_buf, 0, cut)
    ag_got_x("n1", n1_buf, 0, half)
    z_relay("d1", 0, 0)
    ag_got_y("n1", n1_buf, 0)
    ag_dx("o1", o1_buf, cut)
    for h in range(2):
        ag_x("n0", n0_buf, n0_src, h)
    ag_dx("n0", n0_buf, cut)
    f0_other(0)
    z_relay("d1", 0, 1)
    ag_got_y("n1", n1_buf, 1)
    ag_got_x("n1", n1_buf, 1, half)
    z_relay("d1", 1, 0)
    local("dyc", dy_in.at[rows(z * ch, ch)], dy_ch).wait()

    @scoped
    def e_calc():
        def e_step(i, dg1):
            r = rows(i * 16, 16)
            m = z_sum(i)
            h_f = h1_ch[r, :].astype(F32)
            r_inv = rinv(h_f)
            xh = h_f * r_inv
            v = m * gain[1:2, :]
            e = dy_ch[r, :].astype(F32) + r_inv * (v - xh * jnp.mean(v * xh, axis=-1, keepdims=True))
            o_own[rows(c * td + z * ch + i * 16, 16), :] = e.astype(BF16)
            return dg1 + jnp.sum(m * xh, axis=0, keepdims=True)

        dg[1:2, :] = lax.fori_loop(0, ch // 16, e_step, jnp.zeros((1, d), F32))

    def at_step(j, k):
        return pl.when(j == k)

    def l1_step(j, carry):
        block = block_of(j)

        @at_step(j, 2)
        def _():
            ag_got_dx("n1", n1_buf, half)
            ag_got_dy("n1", n1_buf, 1, half)
            ag_got_dx("o1", o1_buf, cut)
            for h in range(2):
                ag_got_dy("o1", o1_buf, h, cut)
            down_rows(1, g_keep, co)
            core_push("d2")
            down_rows(1, g_keep, c)

        partner_has("n1", n1_buf, j)
        stage(n1_buf, block, nb.at[0], "sn")
        partner_has("o1", o1_buf, j)
        stage(o1_buf, block, ob.at[0], "so")
        staged(n1_buf, block, nb.at[0], "sn")
        fwd(1, nb.at[0], None)

        @at_step(j, 0)
        def _():
            z_relay("d1", 1, 1)

        @at_step(j, 1)
        def _():
            z_got("d1")
            sum_sends_done("d1")
            e_calc()
            z_gather("o0z", o_own)

        staged(o1_buf, block, ob.at[0], "so")
        bwd_hidden(1, ob.at[0])

        @at_step(j, 0)
        def _():
            ag_got_x("o1", o1_buf, 1, cut)

        @at_step(j, 2)
        def _():
            ag_got_x("n0", n0_buf, 0, cut)
            ag_got_x("n0", n0_buf, 1, cut)

        weight_grads(nb.at[0], ob.at[0])
        return carry

    lax.fori_loop(0, 3, l1_step, 0)
    grads_out(1)
    z_gathered("o0z", o_own)
    for h in range(2):
        ag_x("o0", o0_buf, o0_src, h)
        ag_y("o0", o0_buf, o0_src, h)
    core_sum_send("d2")
    got("xp", x_part)
    xl = [local("xl0", x_in, nb.at[1, rows(c * td, td)]), local("xl1", x_part, nb.at[1, rows(co * td, td)])]
    for s in xl:
        s.start()
    stage(n0_buf, q, nb.at[0], "sn")
    back = lambda block: (local("sa", a_save.at[block], a_t), local("sb", b_save.at[block], b_t))
    for s in back(q):
        s.start()
    for s in xl:
        s.wait()

    def r_step(i, carry):
        h_f = nb[1, rows(i * 16, 16), :].astype(F32)
        r_own[rows(i * 16, 16), :] = jnp.broadcast_to(rinv(h_f), (16, 128))
        return carry

    lax.fori_loop(0, t2 // 16, r_step, 0)
    z_gathered_partner("o0z", o_own)
    for s in back(q):
        s.wait()

    def gz_id(zi):
        base = sid(("gz", 0))
        for i in range(4):
            assert sid(("gz", i)) == base + i
        return base + zi

    def yz_id(zi):
        base = sid(("yz", 0))
        for i in range(4):
            assert sid(("yz", i)) == base + i
        return base + zi

    def y_rows(zi):
        return y_out.at[rows(zi * ch, ch)]

    gz_id(0)
    yz_id(0)

    bwd_hidden(0, o_own)

    @scoped
    def dgain0():
        def dg_step(i, carry):
            w = cols(i * tile, tile)
            m = mm(a_t[...], wg[0, rows(i * tile, tile)], 1, 1) + mm(b_t[...], wu[0, rows(i * tile, tile)], 1, 1)
            xh = nb[1, :, w].astype(F32) * r_own[:, 0:1]
            dg[0:1, w] = jnp.sum(m * xh, axis=0, keepdims=True)
            return carry

        lax.fori_loop(0, d // tile, dg_step, 0)

    dgain0()
    push("gc", lambda: (dg, dg_core, to_c))
    z_relay("d2", 0, 0)
    z_relay("d2", 0, 1)
    staged(n0_buf, q, nb.at[0], "sn")
    grads_out_done(1)
    zero_acc()
    weight_grads(nb.at[0], o_own)
    z_relay("d2", 1, 0)
    ag_got_y("o0", o0_buf, 0)
    z_relay("d2", 1, 1)
    ag_got_dx("n0", n0_buf, cut)
    for h in range(2):
        ag_got_dy("n0", n0_buf, h, cut)

    def f0_step(j, carry):
        f0_other(j)
        return carry

    lax.fori_loop(1, 3, f0_step, 0)
    ag_got_y("o0", o0_buf, 1)
    ag_got_x("o0", o0_buf, 0, half)

    def l0_body(j, carry):
        block = block_of(j)

        @at_step(j, 2)
        def _():
            ag_got_dx("o0", o0_buf, half)
            ag_got_dy("o0", o0_buf, 1, half)

        for s in back(block):
            s.start()
        stage(n0_buf, block, nb.at[0], "sn")
        partner_has("o0", o0_buf, j)
        stage(o0_buf, block, ob.at[0], "so")
        for s in back(block):
            s.wait()
        staged(o0_buf, block, ob.at[0], "so")
        bwd_hidden(0, ob.at[0])

        @at_step(j, 0)
        def _():
            ag_got_x("o0", o0_buf, 1, half)
            got("gc", dg_core)
            copy_of("gc", "gc", dg, dg_core, to_c).wait_send()
            dg[...] = dg[...] + dg_core[...]
            push("gx", lambda: (dg, dg_x, to_x))
            z_got("d2")

            def y_step(i, carry):
                r = rows(i * 16, 16)
                y_ch[r, :] = (h1_ch[r, :].astype(F32) + z_sum(i)).astype(BF16)
                return carry

            lax.fori_loop(0, ch // 16, y_step, 0)
            local("yk", y_ch, y_rows(z)).start()
            for k in (1, 2, 3):
                push(("ys", k), lambda: (y_ch, y_rows(z), at_z(z_other(k))), yz_id(z))

        @at_step(j, 1)
        def _():
            got("gx", dg_x)
            copy_of("gx", "gx", dg, dg_x, to_x).wait_send()
            dg[...] = dg[...] + dg_x[...]
            push("gy", lambda: (dg, dg_y, to_y))

        @at_step(j, 2)
        def _():
            got("gy", dg_y)
            copy_of("gy", "gy", dg, dg_y, to_y).wait_send()
            dg_z[z] = dg[...] + dg_y[...]
            for k in (1, 2, 3):
                push(("gs", k), lambda: (dg_z.at[z], dg_z.at[z], at_z(z_other(k))), gz_id(z))

        staged(n0_buf, block, nb.at[0], "sn")
        weight_grads(nb.at[0], ob.at[0])
        return carry

    lax.fori_loop(0, 3, l0_body, 0)
    grads_out(0)
    for key in ("gc", "gx", "gy"):
        sent.pop(key)
    for k in (1, 2, 3):
        with jax.named_scope("got_gz"):
            got(gz_id(z_other(k)), dg_z.at[z_other(k)])
    dgain_out[...] = dg_z[0] + dg_z[1] + dg_z[2] + dg_z[3]
    for k in (1, 2, 3):
        with jax.named_scope("got_yz"):
            got(yz_id(z_other(k)), y_rows(z_other(k)))
    local("yk", y_ch, y_rows(z)).wait()
    grads_out_done(0)
    for key in list(sent):
        send_done(key)


def make_call(td, d, rb, hs):
    fb = hs // 4
    hh, t2, ch = 2 * fb, 2 * td, td // 4
    shape = jax.ShapeDtypeStruct
    hbm = pl.BlockSpec(memory_space=pl.ANY)
    vmem = pl.BlockSpec(memory_space=pltpu.VMEM)
    block = shape((4, 2, td, d), BF16)
    outs = [
        shape((td, d), BF16), shape((2, rb, hs), F32), shape((2, rb, hs), F32), shape((2, fb, d), F32), shape((2, d), F32),
        block, block, block, block, shape((4, t2, hh), BF16), shape((4, t2, hh), BF16), shape((td, d), BF16),
    ]
    scratch = [
        pltpu.VMEM((2, d, hh), BF16), pltpu.VMEM((2, d, hh), BF16), pltpu.VMEM((2, hh, d), BF16),
        pltpu.VMEM((2 * rb, hh), F32), pltpu.VMEM((2 * rb, hh), F32), pltpu.VMEM((fb, d), F32),
        pltpu.VMEM((2, t2, d), BF16), pltpu.VMEM((1, t2, d), BF16),
        pltpu.VMEM((t2, hh), BF16), pltpu.VMEM((t2, hh), BF16), pltpu.VMEM((t2, hh), BF16), pltpu.VMEM((t2, hh), BF16),
        pltpu.VMEM((t2, d), F32), pltpu.VMEM((td, d), F32), pltpu.VMEM((4, ch, d), F32),
        pltpu.VMEM((t2, d), BF16), pltpu.VMEM((t2, d), BF16),
        pltpu.VMEM((ch, d), BF16), pltpu.VMEM((ch, d), BF16), pltpu.VMEM((ch, d), BF16), pltpu.VMEM((ch, d), BF16),
        pltpu.VMEM((t2, 128), F32),
        pltpu.VMEM((2, d), F32), pltpu.VMEM((2, d), F32), pltpu.VMEM((2, d), F32), pltpu.VMEM((2, d), F32), pltpu.VMEM((4, 2, d), F32),
        pltpu.SemaphoreType.DMA((NSEM,)), pltpu.SemaphoreType.DMA((NSEM,)), pltpu.SemaphoreType.DMA((NLOC,)),
    ]
    return pl.pallas_call(
        kernel,
        out_shape=outs,
        in_specs=[hbm] * 5 + [vmem],
        out_specs=[hbm] * 4 + [vmem] + [hbm] * 7,
        scratch_shapes=scratch,
        compiler_params=pltpu.CompilerParams(collective_id=0, has_side_effects=True, vmem_limit_bytes=67043328),
    )


def solution(mesh):
    tok_spec = P(("replica", "fsdp"), None)
    wide_spec = P(None, "fsdp", "tensor")
    down_spec = P(None, ("tensor", "fsdp"), None)
    gain_spec = P(None, None)

    def device_fn(x_loc, dy_loc, w_gate, w_up, w_down, norm_gain):
        call = make_call(x_loc.shape[0], x_loc.shape[1], w_gate.shape[1], w_gate.shape[2])
        return tuple(call(x_loc, dy_loc, w_gate, w_up, w_down, norm_gain)[:5])

    return jax.shard_map(device_fn, mesh=mesh, in_specs=(tok_spec, tok_spec, wide_spec, wide_spec, down_spec, gain_spec), out_specs=(tok_spec, wide_spec, wide_spec, down_spec, gain_spec), check_vma=False)
```

```python
import jax
import jax.numpy as jnp
from jax import lax
from jax.experimental import pallas as pl
from jax.experimental.pallas import tpu as pltpu
from jax.sharding import PartitionSpec as P

F32 = jnp.float32
BF16 = jnp.bfloat16
MESH = pl.DeviceIdType.MESH
NSEM = 340
NLOC = 96


def mm(lhs, rhs, ldim, rdim):
    return lax.dot_general(lhs, rhs, (((ldim,), (rdim,)), ((), ())), preferred_element_type=F32)


def kernel(
    x_in, dy_in, wg_in, wu_in, wd_in, gain,
    y_out, dwg_out, dwu_out, dwd_out, dgain_out, n0_buf, n1_buf, o1_buf, o0_buf, a_save, b_save, x_part, g_save, core_hbm,
    wg, wu, wd, acc_g, acc_u, acc_d, nb, ob, a_t, b_t, g_t, part, from_z,
    x_ch, h1_ch, r_own, dg, dg_core, dg_x, dg_y, dg_z, ssem, rsem, lsem, credit,
):
    td, d = x_in.shape
    rb = wg_in.shape[1]
    fb = wg_in.shape[2] // 4
    hh = 2 * fb
    t2, ch, half = 2 * td, td // 4, td // 2
    hc = ch // 2
    tile = min(512, fb)
    z = lax.axis_index("tensor")
    y = lax.axis_index("replica")
    f = lax.axis_index("fsdp")
    x, c = f // 2, f % 2
    xo, yo, co = 1 - x, 1 - y, 1 - c
    q, qx, qy, qd = 2 * y + x, 2 * y + xo, 2 * yo + x, 2 * yo + xo
    cs = (c + y) % 2
    cso = 1 - cs
    to_c, to_x, to_xs, to_y = {"fsdp": 2 * x + co}, {"fsdp": 2 * xo + c}, {"fsdp": 2 * xo + cs}, {"replica": yo}
    inner = ((z + 1) // 2) % 2
    outer = 1 - inner
    up = z // 2
    pair = z + 1 - 2 * (z % 2)
    far_outer, far_inner = 3 - 3 * up, 2 - up
    order = (outer * far_outer + inner * pair, outer * far_inner + inner * far_outer, outer * pair + inner * far_inner, z)

    n_own, o_own = nb.at[1], ob.at[1]

    def at_z(i):
        return {"tensor": i}

    def z_other(k):
        return (z + 4 + k * (1 - 2 * up)) % 4

    others = tuple(z_other(k) for k in (1, 2, 3))
    toward = outer * pair + inner * far_inner

    def rows(start, size):
        return pl.ds(start if isinstance(start, int) else pl.multiple_of(start, size if size % 16 == 0 else 8), size)

    def cols(start, size):
        return pl.ds(start if isinstance(start, int) else pl.multiple_of(start, 128), size)

    ids, lids, sent, passed = {}, {}, {}, {}

    def sid(key):
        i = ids.setdefault(key, len(ids))
        assert i < NSEM, i
        return i

    def name_of(key):
        return key if isinstance(key, str) else "_".join(map(str, key))

    def copy_of(skey, rkey, src, dst, dev):
        return pltpu.make_async_remote_copy(
            src_ref=src, dst_ref=dst, send_sem=ssem.at[sid(skey)], recv_sem=rsem.at[rkey if not isinstance(rkey, (str, tuple)) else sid(rkey)],
            device_id=dev, device_id_type=MESH,
        )

    def push(key, make, rkey=None):
        copy_of(key, key if rkey is None else rkey, *make()).start()
        sent[key] = make

    def got(key, dst):
        with jax.named_scope("got_" + (name_of(key) if isinstance(key, (str, tuple)) else "dyn")):
            copy_of("none", key, dst, dst, to_c).wait_recv()

    def send_done(key):
        copy_of(key, key, *sent.pop(key)()).wait_send()

    def local(key, src, dst):
        i = lids.setdefault(key, len(lids))
        assert i < NLOC, i
        return pltpu.make_async_copy(src, dst, lsem.at[i])

    def scoped(fn):
        def run(*args):
            with jax.named_scope(fn.__name__):
                return fn(*args)

        return run

    gu = ((wg_in, wg), (wu_in, wu))
    pieces = (2, 2)

    def wview(m, l, row, xb, k=0, n=1):
        return gu[m][1].at[l, rows(row * rb + k * (rb // n), rb // n), cols(xb * fb, fb)]

    def wsrc(m, l, xb, core, k=0, n=1):
        return gu[m][0].at[l, pl.ds(k * (rb // n), rb // n), cols((2 * xb + core) * fb, fb)]

    def push_w(l, m):
        n = pieces[l]
        for xb in range(2):
            for k in range(n):
                push(("wx", l, m, xb, k), lambda xb=xb, k=k: (wsrc(m, l, xb, cs, k, n), wview(m, l, f, xb, k, n), to_xs))
        for k in range(4 * m):
            r0 = y * (fb // 2) + k * (fb // 8)
            push(("wdx", l, k), lambda r0=r0: (wd_in.at[l, rows(r0, fb // 8)], wd.at[l, rows(x * fb + r0, fb // 8)], to_x))
        if (l, m) == (1, 1):
            r1 = yo * (fb // 2) + 3 * (fb // 8)
            push("wdx_last", lambda: (wd_in.at[l, rows(r1, fb // 8)], wd.at[l, rows(x * fb + r1, fb // 8)], to_x))

    def push_wc(l):
        for m in range(2):
            for xb in range(2):
                push(("wc", l, m, xb), lambda m=m, xb=xb: (wsrc(m, l, xb, co), wview(m, l, f, xb), to_c))
                local(("w", l, m, xb), wsrc(m, l, xb, c), wview(m, l, f, xb)).start()
        local(("wd", l), wd_in.at[l], wd.at[l, rows(x * fb, fb)]).start()

    def relay_gu(l, m, xb):
        n = pieces[l]
        for k in range(n):
            ref = lambda k=k: wview(m, l, 2 * xo + cs, xb, k, n)
            got(("wx", l, m, xb, k), ref())
            push(("wy", l, m, xb, k), lambda k=k: (ref(k), ref(k), to_y))

    def relay_d(l, k):
        ref = lambda: wd.at[l, rows(xo * fb + y * (fb // 2) + k * (fb // 8), fb // 8)]
        got(("wdx", l, k), ref())
        push(("wdy", l, k), lambda: (ref(), ref(), to_y))

    def have_gu(l, m, xb):
        n = pieces[l]
        local(("w", l, m, xb), wsrc(m, l, xb, c), wview(m, l, f, xb)).wait()
        got(("wc", l, m, xb), wview(m, l, 2 * x + co, xb))
        for k in range(n):
            got(("wy", l, m, xb, k), wview(m, l, 2 * xo + cso, xb, k, n))

    def have_d_own(l):
        local(("wd", l), wd_in.at[l], wd.at[l, rows(x * fb, fb)]).wait()

    def have_d(l):
        for k in range(4 - l):
            got(("wdy", l, k), wd.at[l, rows(xo * fb + yo * (fb // 2) + k * (fb // 8), fb // 8)])
        if l == 1:
            got(("wdx", 1, 3), wd.at[1, rows(xo * fb + y * (fb // 2) + 3 * (fb // 8), fb // 8)])
            got("wdx_last", wd.at[1, rows(xo * fb + yo * (fb // 2) + 3 * (fb // 8), fb // 8)])

    def piece(buf, block, core, start, size):
        return buf.at[block, core, pl.ds(start, size)]

    def chunk(buf, block, core, zi):
        return buf.at[block, core, rows(zi * ch, ch)]

    def part_id(a, j):
        base = sid((a, "p", 0))
        for jj in range(3):
            assert sid((a, "p", jj)) == base + jj
        return base + j

    def share(a, j, tag, ref):
        push((a, "s", j, tag), lambda: (ref(), ref(), to_c), (a, "p", j))

    def ag_x(a, buf, src, h):
        push((a, "x", h), lambda: (src().at[pl.ds(h * half, half)], piece(buf, q, c, h * half, half), to_x))

    def ag_y(a, buf, src, h):
        push((a, "y", h), lambda: (src().at[pl.ds(h * half, half)], piece(buf, q, c, h * half, half), to_y))

    def ag_quarter(a, buf, src, axis):
        push((a, axis + "c"), lambda: (src().at[rows(z * ch, ch)], chunk(buf, q, c, z), to_y if axis == "y" else to_x))

    def zb_id(a, axis, zi):
        base = sid((a, axis, "zb", 0))
        for i in range(4):
            assert sid((a, axis, "zb", i)) == base + i
        return base + zi

    def ag_spread(a, buf, axis):
        block = qy if axis == "y" else qx
        got((a, axis + "c"), chunk(buf, block, c, z))
        for k in (1, 2, 3):
            push((a, axis, "zs", k), lambda k=k: (chunk(buf, block, c, z), chunk(buf, block, c, z), at_z(z_other(k))), zb_id(a, axis, z))

    def ag_spread_got(a, buf, axis):
        block = qy if axis == "y" else qx
        for k in (1, 2, 3):
            with jax.named_scope("got_zb_" + a + axis):
                got(zb_id(a, axis, z_other(k)), chunk(buf, block, c, z_other(k)))
        share(a, 0 if axis == "y" else 1, 0, lambda: buf.at[block, c])

    def ag_dx(a, buf, cut):
        push((a, "dx"), lambda: (piece(buf, qy, c, 0, cut), piece(buf, qy, c, 0, cut), to_x))

    def ag_got_y(a, buf, h):
        got((a, "y", h), piece(buf, qy, c, h * half, half))
        share(a, 0, h, lambda: piece(buf, qy, c, h * half, half))
        if h == 0:
            ag_dx(a, buf, half)

    def ag_dy(a, buf, cut):
        push((a, "dy", 0), lambda: (piece(buf, qx, c, cut, td - cut), piece(buf, qx, c, cut, td - cut), to_y))

    def ag_got_dy_whole(a, buf, cut):
        got((a, "dy", 0), piece(buf, qd, c, cut, td - cut))
        share(a, 2, 0, lambda: piece(buf, qd, c, cut, td - cut))

    def diag_piece(h, cut):
        start = max(cut, h * half)
        return start, (h + 1) * half - start

    def ag_got_x(a, buf, h, cut):
        got((a, "x", h), piece(buf, qx, c, h * half, half))
        start, size = diag_piece(h, cut)
        if size:
            push((a, "dy", h), lambda: (piece(buf, qx, c, start, size), piece(buf, qx, c, start, size), to_y))
        share(a, 1, h, lambda: piece(buf, qx, c, h * half, half))

    def ag_got_dx(a, buf, cut):
        got((a, "dx"), piece(buf, qd, c, 0, cut))
        share(a, 2, "x", lambda: piece(buf, qd, c, 0, cut))

    def ag_got_dy(a, buf, h, cut):
        start, size = diag_piece(h, cut)
        if size:
            got((a, "dy", h), piece(buf, qd, c, start, size))
            share(a, 2, h, lambda: piece(buf, qd, c, start, size))

    def block_of(j):
        return 2 * ((y + (j + 1) % 2) % 2) + (x + (j + 1) // 2) % 2

    def partner_has(a, buf, j):
        with jax.named_scope("got_p_" + a):
            got(part_id(a, j), buf.at[block_of(j), co])

    for a in ("n0", "o1", "n1", "o0"):
        for j in range(3):
            sid((a, "p", j))
        for axis in "xy":
            for i in range(4):
                sid((a, axis, "zb", i))

    def fwd_tile(l, n_ref, g_ref, i, a_ref=None, b_ref=None):
        w = cols(i * tile, tile)
        a = mm(n_ref[...], wg[l, :, w], 1, 0).astype(BF16)
        b = mm(n_ref[...], wu[l, :, w], 1, 0).astype(BF16)
        (a_t if a_ref is None else a_ref)[:, w] = a
        (b_t if b_ref is None else b_ref)[:, w] = b
        if g_ref is not None:
            a_f = a.astype(F32)
            g_ref[:, w] = (a_f * jax.nn.sigmoid(a_f) * b.astype(F32)).astype(BF16)

    @scoped
    def fwd(l, n_ref, g_ref, a_ref=None, b_ref=None):
        def step(i, carry):
            fwd_tile(l, n_ref, g_ref, i, a_ref, b_ref)
            return carry

        lax.fori_loop(0, hh // tile, step, 0)

    @scoped
    def down_half(l, g_ref, kb, start, size, add):
        r, k = rows(start, size), pl.ds(pl.multiple_of(kb * fb, fb), fb)

        def step(i, carry):
            w = cols(i * tile, tile)
            new = mm(g_ref[r, k], wd[l, k, w], 1, 0)
            part[r, w] = part[r, w] + new if add else new
            return carry

        lax.fori_loop(0, d // tile, step, 0)

    @scoped
    def down_rows(l, g_ref, core):
        r = rows(core * td, td)

        def step(i, carry):
            w = cols(i * tile, tile)
            part[r, w] = mm(g_ref[r, :], wd[l, :, w], 1, 0)
            return carry

        lax.fori_loop(0, d // tile, step, 0)

    @scoped
    def m_half(l, kb, start, size, add):
        r, k = rows(start, size), pl.ds(pl.multiple_of(kb * fb, fb), fb)

        def step(i, carry):
            w = rows(i * tile, tile)
            new = mm(a_t[r, k], wg[l, w, k], 1, 1) + mm(b_t[r, k], wu[l, w, k], 1, 1)
            o = cols(i * tile, tile)
            part[r, o] = part[r, o] + new if add else new
            return carry

        lax.fori_loop(0, d // tile, step, 0)

    def bwd_tile(l, o_ref, i, a_ref, b_ref):
        w = cols(i * tile, tile)
        q_f = mm(o_ref[...], wd[l, rows(i * tile, tile)], 1, 1).astype(BF16).astype(F32)
        a_f, b_f = a_ref[:, w].astype(F32), b_ref[:, w].astype(F32)
        s = jax.nn.sigmoid(a_f)
        g_t[:, w] = (a_f * s * b_f).astype(BF16)
        a_t[:, w] = (q_f * b_f * s * (1.0 + a_f * (1.0 - s))).astype(BF16)
        b_t[:, w] = (q_f * a_f * s).astype(BF16)

    @scoped
    def bwd_hidden(l, o_ref, a_ref, b_ref):
        for i in range(hh // tile):
            bwd_tile(l, o_ref, i, a_ref, b_ref)

    @scoped
    def weight_grads(n_ref, col, o_ref, between):
        t = min(256, fb)

        def half_rows(core):
            for i in range(rb // t):
                n_rows = n_ref[:, cols(col + core * rb + i * t, t)]
                w = rows(core * rb + i * t, t)
                acc_g[w, :] += mm(n_rows, a_t[...], 0, 0)
                acc_u[w, :] += mm(n_rows, b_t[...], 0, 0)

        half_rows(co)
        if between is not None:
            between()
        half_rows(c)
        for i in range(fb // t):
            acc_d[pl.ds(i * t, t), :] += mm(g_t[:, cols(x * fb + i * t, t)], o_ref[...], 0, 0)

    @scoped
    def zero_acc():
        for ref in (acc_g, acc_u, acc_d):
            def step(i, carry, ref=ref):
                ref[rows(i * 16, 16), :] = jnp.zeros((16, ref.shape[1]), F32)
                return carry

            lax.fori_loop(0, ref.shape[0] // 16, step, 0)

    def rinv(h_f):
        return lax.rsqrt(jnp.mean(h_f * h_f, axis=-1, keepdims=True) + 1e-6)

    def core_land(key):
        return core_hbm if key == "d2" else acc_d

    def core_push(key):
        for k in range(4):
            push((key, "c", k), lambda k=k: (part.at[rows(co * td + order[k] * ch, ch)], core_land(key).at[rows(order[k] * ch, ch)], to_c))

    def z_ids(key):
        base = sid((key, "A", 0))
        for h in range(2):
            for i, s in enumerate("ABCD"):
                assert sid((key, s, h)) == base + 4 * h + i
        return base

    for sum_key in ("d0", "d1", "d2"):
        z_ids(sum_key)

    def mine(zi, h):
        return part.at[rows(c * td + zi * ch + h * hc, hc)]

    def slot(key, i, h):
        return from_z.at[i, pl.ds(h * hc, hc)]

    def core_back(k):
        return local(("cl", k), core_hbm.at[rows(order[k] * ch, ch)], part.at[rows(co * td + order[k] * ch, ch)])

    def core_back_start(key):
        for k in range(4):
            got((key, "c", k), core_land(key).at[rows(order[k] * ch, ch)])
            send_done((key, "c", k))
            core_back(k).start()

    @scoped
    def core_sum_send(key):
        z_ids(key)
        for k in range(4):
            if key == "d2":
                core_back(k).wait()
            else:
                got((key, "c", k), core_land(key).at[rows(order[k] * ch, ch)])

            def step(i, carry):
                r = order[k] * ch + i * 16
                mine_r = rows(c * td + r, 16)
                part[mine_r, :] = part[mine_r, :] + (part[rows(co * td + r, 16), :] if key == "d2" else acc_d[rows(r, 16), :])
                return carry

            lax.fori_loop(0, ch // 16, step, 0)
            if k == 0:
                for h in range(2):
                    push((key, "A", h), lambda h=h: (mine(order[0], h), slot(key, 0, h), at_z(pair)))
            elif k < 3:
                @pl.when(outer == 1)
                def _():
                    for h in range(2):
                        copy_of((key, "BC"[k - 1], h), (key, "BC"[k - 1], h), mine(order[k], h), slot(key, k, h), at_z(pair)).start()


    def z_relay(key, n, h):
        @pl.when(inner == 1)
        def _():
            got((key, "AB"[n], h), slot(key, n, h))
            zi = (far_outer, far_inner)[n]
            work = slot(key, n, h)

            def step(i, carry):
                r = rows(i * 8, 8)
                work[r, :] = work[r, :] + part[rows(c * td + zi * ch + h * hc + i * 8, 8), :]
                return carry

            lax.fori_loop(0, hc // 8, step, 0)
            if n == 0:
                copy_of((key, "B", h), (key, "B", h), work, slot(key, 1, h), at_z(far_outer)).start()
            else:
                copy_of((key, "C", h), (key, "D", h), work, slot(key, 3, h), at_z(far_inner)).start()

    def z_got(key):
        base = z_ids(key)
        for h in range(2):
            for i in range(2):
                with jax.named_scope("got_" + key):
                    got(base + 4 * h + 2 * inner + i, slot(key, 2 * inner + i, h))

    def z_sum(key, i):
        r = rows(i * 16, 16)
        return part[rows(c * td + z * ch + i * 16, 16), :] + from_z[2 * inner, r, :] + from_z[2 * inner + 1, r, :]

    def relay_sends_done(key):
        @pl.when(inner == 1)
        def _():
            for s in "BC":
                for h in range(2):
                    copy_of((key, s, h), (key, s, h), mine(0, h), slot(key, 0, h), at_z(pair)).wait_send()

    def sum_sends_done(key):
        for part_key in [(key, "c", k) for k in range(4)] + [(key, "A", h) for h in range(2)]:
            send_done(part_key)

        @pl.when(outer == 1)
        def _():
            for s in "BC":
                for h in range(2):
                    copy_of((key, s, h), (key, s, h), mine(0, h), slot(key, 0, h), at_z(pair)).wait_send()

    def quarter(ref, core, zi):
        return ref.at[rows(core * td + zi * ch, ch)]

    def zg_id(key, zi):
        base = sid((key, "z", 0))
        for i in range(4):
            assert sid((key, "z", i)) == base + i
        return base + zi

    relayed = ("n1z",)

    def takes(key):
        return (pair, far_inner, far_outer) if key in relayed else others

    def z_push(key, make, zi):
        for k, dev in enumerate((toward,) if key in relayed else others):
            push((key, "zs", k), lambda dev=dev: (*make(zi), at_z(dev)), zg_id(key, zi))
        if key in relayed:
            z_forward(key, 3, make(zi)[1], zg_id(key, zi), pair)
            passed[(key, "fw", 3)] = lambda: make(z)[1]

    def z_forward(key, i, ref, rkey, dev):
        @pl.when(inner == 1)
        def _():
            copy_of((key, "fw", i), rkey, ref, ref, at_z(dev)).start()

    def z_pass(key, make, i):
        zi = takes(key)[i]
        with jax.named_scope("got_%s_%d" % (key, i)):
            got(zg_id(key, zi), make(zi)[1])
        if key in relayed:
            z_forward(key, i, make(zi)[1], zg_id(key, zi), (far_inner, pair, pair)[i])
            passed[(key, "fw", i)] = lambda: make(zi)[1]

    def passed_done(which):
        @pl.when(inner == 1)
        def _():
            for key in [k1 for k1 in passed if k1[0] == which]:
                ref = passed.pop(key)
                copy_of(key, key, ref(), ref(), to_c).wait_send()

    def z_gather(key, ref):
        z_push(key, lambda zi: (quarter(ref, c, zi), quarter(ref, c, zi)), z)
        push((key, "s", 0), lambda: (quarter(ref, c, z), quarter(ref, c, z), to_c))

    def z_take(key, ref, i):
        z_pass(key, lambda zi: (quarter(ref, c, zi), quarter(ref, c, zi)), i)
        push((key, "s", 1 + i), lambda: (quarter(ref, c, takes(key)[i]), quarter(ref, c, takes(key)[i]), to_c))

    def z_gathered_partner(key, ref):
        got((key, "s", 0), quarter(ref, co, z))
        for i in range(3):
            got((key, "s", 1 + i), quarter(ref, co, takes(key)[i]))

    def stage(buf, block, slot_ref, key):
        for core in range(2):
            local((key, core), buf.at[block, core], slot_ref.at[pl.ds(core * td, td)]).start()

    def staged(buf, block, slot_ref, key):
        for core in range(2):
            local((key, core), buf.at[block, core], slot_ref.at[pl.ds(core * td, td)]).wait()

    def save_ab(block):
        return (local("sa", a_t, a_save.at[block]), local("sb", b_t, b_save.at[block]))

    @scoped
    def f0_other(j, slot):
        fwd(0, nb.at[slot], None)
        for s in save_ab(block_of(j)):
            s.start()

    def saves_done(block):
        for s in save_ab(block):
            s.wait()

    def a_kept(k):
        return wg.at[1, rows(k * t2, t2)]

    def b_kept(k):
        return wd.at[1, rows((k // 2) * t2, t2), cols((k % 2) * hh, hh)]

    def load_ab(block, k):
        return (local(("la", k), a_save.at[block], a_kept(k)), local(("lb", k), b_save.at[block], b_kept(k)))

    def grads_push(l):
        for i, (acc, out) in enumerate(((acc_g, dwg_out), (acc_u, dwu_out))):
            for xb in range(2):
                push(("q", l, i, xb), lambda acc=acc, out=out, xb=xb: (acc.at[rows(co * rb, rb), cols(xb * fb, fb)], out.at[l, :, cols((2 * xb + c) * fb, fb)], to_c))

    def grads_out(l):
        for i, (acc, out) in enumerate(((acc_g, dwg_out), (acc_u, dwu_out))):
            for xb in range(2):
                local(("qo", l, i, xb), acc.at[rows(c * rb, rb), cols(xb * fb, fb)], out.at[l, :, cols((2 * xb + c) * fb, fb)]).start()
        local(("qd", l), acc_d, dwd_out.at[l]).start()

    @scoped
    def grads_out_done(l):
        for i, (acc, out) in enumerate(((acc_g, dwg_out), (acc_u, dwu_out))):
            for xb in range(2):
                local(("qo", l, i, xb), acc.at[rows(c * rb, rb), cols(xb * fb, fb)], out.at[l, :, cols((2 * xb + c) * fb, fb)]).wait()
                send_done(("q", l, i, xb))
                got(("q", l, i, xb), out.at[l, :, cols((2 * xb + co) * fb, fb)])
        local(("qd", l), acc_d, dwd_out.at[l]).wait()

    barrier = pltpu.get_barrier_semaphore()
    for dev in (to_c, to_x, {"fsdp": 2 * xo + co}, to_y, at_z((z + 1) % 4), at_z((z + 2) % 4), at_z((z + 3) % 4)):
        pl.semaphore_signal(barrier, inc=1, device_id=dev, device_id_type=MESH)
    x_load = local("x", x_in, nb.at[1, pl.ds(0, td)])
    x_load.start()
    with jax.named_scope("barrier"):
        pl.semaphore_wait(barrier, 7)

    dy_src = lambda: dy_in
    n0_src = lambda: n0_buf.at[q, c]
    n1_src = lambda: n_own.at[rows(c * td, td)]
    o0_src = lambda: o_own.at[rows(c * td, td)]
    cut_n, cut_o = ch, ch

    push_w(0, 0)
    push_wc(0)
    x_load.wait()

    def n0_step(i, carry):
        h_f = n_own[rows(i * 16, 16), :].astype(F32)
        r_inv = rinv(h_f)
        nb[0, rows(c * td + i * 16, 16), :] = (h_f * r_inv * gain[0:1, :]).astype(BF16)
        r_own[rows(c * td + i * 16, 16), :] = jnp.broadcast_to(r_inv, (16, 128))
        return carry

    lax.fori_loop(0, td // 16, n0_step, 0)
    n0_mine = lambda: nb.at[0, rows(c * td, td)]
    push("n0p", lambda: (n0_mine(), n0_mine(), to_c))
    r_mine = lambda: r_own.at[rows(c * td, td)]
    push("rp", lambda: (r_mine(), r_mine(), to_c))
    keep = local("n0k", n0_mine(), n0_buf.at[q, c])
    keep.start()
    keep.wait()
    ag_quarter("n0", n0_buf, n0_src, "y")
    ag_quarter("n0", n0_buf, n0_src, "x")
    ag_quarter("o1", o1_buf, dy_src, "y")
    push_w(0, 1)
    push_w(1, 0)
    push_w(1, 1)
    ag_x("o1", o1_buf, dy_src, 0)
    push("xp", lambda: (x_in, x_part, to_c))
    push("dyp", lambda: (dy_in, o1_buf.at[q, c], to_c))
    push_wc(1)
    local("xc", x_in.at[rows(z * ch, ch)], x_ch).start()
    local("dy_own", dy_in, ob.at[0, rows(c * td, td)]).start()

    @scoped
    def h1_calc():
        def h1_step(i, carry):
            r = rows(i * 16, 16)
            h1 = (x_ch[r, :].astype(F32) + z_sum("d0", i)).astype(BF16)
            h1_ch[r, :] = h1
            h_f = h1.astype(F32)
            n_own[rows(c * td + z * ch + i * 16, 16), :] = (h_f * rinv(h_f) * gain[1:2, :]).astype(BF16)
            return carry

        lax.fori_loop(0, ch // 16, h1_step, 0)

    def h1_done():
        z_got("d0")
        relay_sends_done("d0")
        h1_calc()
        z_gather("n1z", n_own)

    relay_gu(0, 0, 0)
    ag_spread("n0", n0_buf, "y")
    ag_spread("o1", o1_buf, "y")
    relay_gu(0, 0, 1)
    ag_spread("n0", n0_buf, "x")
    relay_gu(0, 1, 0)
    relay_gu(0, 1, 1)
    got("n0p", nb.at[0, rows(co * td, td)])
    got("rp", r_own.at[rows(co * td, td)])
    keep2 = local("n0k2", nb.at[0, rows(co * td, td)], n0_buf.at[q, co])
    keep2.start()
    have_gu(0, 0, 0)
    have_gu(0, 1, 0)
    with jax.named_scope("fwd_tile0"):
        fwd_tile(0, nb.at[0], g_t, 0)
    relay_d(0, 0)
    relay_d(0, 1)
    have_gu(0, 0, 1)
    have_gu(0, 1, 1)
    with jax.named_scope("fwd_tile1"):
        for i in range(1, hh // tile):
            fwd_tile(0, nb.at[0], g_t, i)
    for s in save_ab(q):
        s.start()
    have_d_own(0)
    relay_d(0, 2)
    down_half(0, g_t, x, 0, t2, False)
    relay_d(0, 3)
    ag_spread_got("n0", n0_buf, "y")
    have_d(0)
    down_half(0, g_t, xo, co * td, td, True)
    core_push("d0")
    down_half(0, g_t, xo, c * td, td, True)
    core_sum_send("d0")
    keep2.wait()
    send_done("n0p")
    saves_done(q)
    partner_has("n0", n0_buf, 0)
    stage(n0_buf, block_of(0), nb.at[0], "sn")
    relay_gu(1, 0, 0)
    staged(n0_buf, block_of(0), nb.at[0], "sn")
    f0_other(0, 0)
    z_relay("d0", 0, 0)
    relay_gu(1, 0, 1)
    z_relay("d0", 0, 1)
    ag_spread_got("n0", n0_buf, "x")
    ag_spread_got("o1", o1_buf, "y")
    partner_has("n0", n0_buf, 1)
    stage(n0_buf, block_of(1), nb.at[0], "sn")
    z_relay("d0", 1, 0)
    relay_gu(1, 1, 0)
    z_relay("d0", 1, 1)
    local("xc", x_in.at[rows(z * ch, ch)], x_ch).wait()

    @pl.when(outer == 1)
    def _():
        h1_done()

    relay_gu(1, 1, 1)

    @pl.when(inner == 1)
    def _():
        h1_done()

    local("dyc", dy_in.at[rows(z * ch, ch)], x_ch).start()
    relay_d(1, 0)
    z_take("n1z", n_own, 0)
    z_take("n1z", n_own, 1)
    relay_d(1, 1)
    z_take("n1z", n_own, 2)
    relay_d(1, 2)
    saves_done(block_of(0))
    for h in range(2):
        ag_x("n1", n1_buf, n1_src, h)
    ag_x("o1", o1_buf, dy_src, 1)
    for h in range(2):
        ag_y("n1", n1_buf, n1_src, h)
    got("dyp", o1_buf.at[q, co])
    dy_other = local("dy_other", o1_buf.at[q, co], ob.at[0, rows(co * td, td)])
    dy_other.start()
    z_gathered_partner("n1z", n_own)

    for m in range(2):
        for xb in range(2):
            have_gu(1, m, xb)
    fwd(1, n_own, g_t)
    local("dy_own", dy_in, ob.at[0, rows(c * td, td)]).wait()
    dy_other.wait()
    have_d_own(1)
    bwd_tile(1, ob.at[0], x, a_t, b_t)
    sum_sends_done("d0")
    m_half(1, x, 0, t2, False)
    have_d(1)
    bwd_tile(1, ob.at[0], xo, a_t, b_t)
    g_keep = local("gk", g_t, g_save)
    g_keep.start()
    m_half(1, xo, co * td, td, True)
    core_push("d1")
    m_half(1, xo, c * td, td, True)
    core_sum_send("d1")
    zero_acc()
    g_keep.wait()
    local("dyc", dy_in.at[rows(z * ch, ch)], x_ch).wait()

    @scoped
    def e_calc():
        def e_step(i, dg1):
            r = rows(i * 16, 16)
            m = z_sum("d1", i)
            h_f = h1_ch[r, :].astype(F32)
            r_inv = rinv(h_f)
            xh = h_f * r_inv
            v = m * gain[1:2, :]
            e = x_ch[r, :].astype(F32) + r_inv * (v - xh * jnp.mean(v * xh, axis=-1, keepdims=True))
            o_own[rows(c * td + z * ch + i * 16, 16), :] = e.astype(BF16)
            return dg1 + jnp.sum(m * xh, axis=0, keepdims=True)

        dg[1:2, :] = lax.fori_loop(0, ch // 16, e_step, jnp.zeros((1, d), F32))

    def at_step(k, n):
        return pl.when(k == n)

    def stage_n(buf, block, slot):
        stage(buf, block, nb.at[slot], ("n", slot))

    def staged_n(buf, block, slot):
        staged(buf, block, nb.at[slot], ("n", slot))

    def stage_o(buf, block, slot):
        stage(buf, block, ob.at[slot], ("o", slot))

    def staged_o(buf, block, slot):
        staged(buf, block, ob.at[slot], ("o", slot))

    xl = lambda: [local("xl0", x_in, nb.at[0, rows(c * td, td)]), local("xl1", x_part, nb.at[0, rows(co * td, td)])]

    def n_half(slot):
        return wu.at[1, rows(slot * t2, t2)]

    def n_half_copies(block, slot):
        return [local(("nh", slot, core), n0_buf.at[block, core, :, cols(2 * x * rb, 2 * rb)], wu.at[1, rows(slot * t2 + core * td, td)]) for core in range(2)]

    def load_n_half(block, slot):
        for s in n_half_copies(block, slot):
            s.start()

    own_g = nb.at[1, :, pl.ds(0, hh)]

    def e_done():
        z_got("d1")
        relay_sends_done("d1")
        e_calc()
        z_gather("o0z", o_own)
        for dev in others:
            pl.semaphore_signal(credit, inc=1, device_id=at_z(dev), device_id_type=MESH)

    def l1_step(k, carry):
        slot = 1 - (k + 3) // 4

        @pl.when(k > 0)
        def _():
            @at_step(k, 1)
            def _():
                partner_has("o1", o1_buf, 0)
                stage_o(o1_buf, block_of(0), 0)

            @pl.when(k * inner == 2)
            def _():
                e_done()

            @at_step(k, 2)
            def _():
                ag_got_x("o1", o1_buf, 1, cut_o)
                ag_dy("n0", n0_buf, cut_n)

            staged_n(n1_buf, block_of(k - 1), 0)
            fwd(1, nb.at[0], None)

            @pl.when(k > 1)
            def _():
                partner_has("o1", o1_buf, k - 1)
                stage_o(o1_buf, block_of(k - 1), 0)

            @at_step(k, 1)
            def _():
                z_relay("d1", 1, 0)
                ag_got_x("n1", n1_buf, 1, half)

            @at_step(k, 3)
            def _():
                for i in range(3):
                    z_take("o0z", o_own, i)
                for h in range(2):
                    ag_x("o0", o0_buf, o0_src, h)
                    ag_y("o0", o0_buf, o0_src, h)
                z_relay("d2", 0, 0)

            staged_o(o1_buf, block_of(k - 1), 0)
            bwd_hidden(1, ob.at[0], a_t, b_t)

            @at_step(k, 1)
            def _():
                z_relay("d1", 1, 1)

                @pl.when(outer == 1)
                def _():
                    e_done()

                partner_has("n1", n1_buf, 1)

            @at_step(k, 2)
            def _():
                local("gl", g_save, own_g).wait()
                sum_sends_done("d1")
                down_rows(1, own_g, co)
                core_push("d2")
                ag_got_dx("n1", n1_buf, half)
                ag_got_dy("n1", n1_buf, 1, half)
                down_rows(1, own_g, c)
                core_back_start("d2")

            @at_step(k, 1)
            def _():
                for key in [("n1z", "zs", 0)] + [("n1z", "s", i) for i in range(4)] + [("n1", axis, h) for axis in "xy" for h in range(2)]:
                    send_done(key)
                passed_done("n1z")
                local("gl", g_save, own_g).start()

            @at_step(k, 3)
            def _():
                z_relay("d2", 0, 1)
                for key in [k1 for k1 in sent if k1[0] in ("wy", "wdy") and k1[1] == 1]:
                    send_done(key)
                for i in range(3):
                    for s in load_ab(block_of(i - 1) if i else q, i):
                        s.start()
                    load_n_half(block_of(i - 1) if i else q, i)

        weight_grads(nb.at[slot], 2 * x * rb, ob.at[0], None)

        @at_step(k, 1)
        def _():
            stage_n(n1_buf, block_of(1), 0)

        @at_step(k, 2)
        def _():
            ag_got_dx("o1", o1_buf, cut_o)
            for h in range(2):
                ag_got_dy("o1", o1_buf, h, cut_o)
            partner_has("n1", n1_buf, 2)
            stage_n(n1_buf, block_of(2), 0)
            pl.semaphore_wait(credit, 3)
            core_sum_send("d2")

        @at_step(k, 0)
        def _():
            staged(n0_buf, block_of(1), nb.at[0], "sn")
            f0_other(1, 0)
            ag_got_x("o1", o1_buf, 0, cut_o)
            ag_got_x("n1", n1_buf, 0, half)
            z_relay("d1", 0, 0)
            ag_got_y("n1", n1_buf, 0)
            ag_dx("o1", o1_buf, cut_o)
            ag_dx("n0", n0_buf, cut_n)
            z_relay("d1", 0, 1)
            ag_got_y("n1", n1_buf, 1)
            partner_has("n1", n1_buf, 0)
            stage_n(n1_buf, block_of(0), 0)
            saves_done(block_of(1))

        return carry

    lax.fori_loop(0, 4, l1_step, 0)
    got("xp", x_part)
    for s in xl():
        s.start()
    for s in load_ab(q, 0):
        s.wait()
    z_gathered_partner("o0z", o_own)
    grads_push(1)
    grads_out(1)

    def gz_id(zi):
        base = sid(("gz", 0))
        for i in range(4):
            assert sid(("gz", i)) == base + i
        return base + zi

    def y_rows(zi):
        return y_out.at[rows(zi * ch, ch)]

    gz_id(0)
    zg_id("y", 0)

    @scoped
    def dgain0():
        def dg_step(i, carry):
            w = cols(i * tile, tile)
            m = mm(a_t[...], wg[0, rows(i * tile, tile)], 1, 1) + mm(b_t[...], wu[0, rows(i * tile, tile)], 1, 1)
            xh = nb[0, :, w].astype(F32) * r_own[:, 0:1]
            dg[0:1, w] = jnp.sum(m * xh, axis=0, keepdims=True)
            return carry

        lax.fori_loop(0, d // tile, dg_step, 0)

    def y_done():
        z_got("d2")

        def y_step(i, carry):
            r = rows(i * 16, 16)
            x_ch[r, :] = (h1_ch[r, :].astype(F32) + z_sum("d2", i)).astype(BF16)
            return carry

        lax.fori_loop(0, ch // 16, y_step, 0)
        local("yk", x_ch, y_rows(z)).start()
        z_push("y", lambda zi: (x_ch, y_rows(zi)), z)

    def l0_step(k, carry):
        oslot = (k + 1) % 2

        @pl.when(k > 0)
        def _():
            staged_o_any(k)

        bwd_hidden(0, ob.at[oslot], a_kept(k), b_kept(k))

        @at_step(k, 0)
        def _():
            for s in xl():
                s.wait()
            ag_got_dx("n0", n0_buf, cut_n)
            ag_got_dy_whole("n0", n0_buf, cut_n)
            z_relay("d2", 1, 0)
            dgain0()
            dg_z[z] = dg[...]
            for i in range(3):
                push(("gs", i), lambda i=i: (dg_z.at[z], dg_z.at[z], at_z(others[i])), gz_id(z))
            z_relay("d2", 1, 1)
            partner_has("n0", n0_buf, 2)
            stage_n(n0_buf, block_of(2), 0)
            load_n_half(block_of(2), 3)
            ag_got_y("o0", o0_buf, 0)
            grads_out_done(1)
            zero_acc()
            for i in range(4):
                for s in n_half_copies(block_of(i - 1) if i else q, i):
                    s.wait()
            for i in range(1, 3):
                for s in load_ab(block_of(i - 1), i):
                    s.wait()

        @at_step(k, 1)
        def _():
            @pl.when(inner == 1)
            def _():
                y_done()

            partner_has("o0", o0_buf, 1)
            for key in [("o0z", "zs", i) for i in range(3)] + [("o0z", "s", i) for i in range(4)] + [("o0", axis, h) for axis in "xy" for h in range(2)]:
                send_done(key)
            stage_o(o0_buf, block_of(1), 1)
            for i in range(3):
                with jax.named_scope("got_gz"):
                    got(gz_id(others[i]), dg_z.at[others[i]])
                send_done(("gs", i))
            dg[...] = dg_z[0] + dg_z[1] + dg_z[2] + dg_z[3]
            push("gc", lambda: (dg, dg_core, to_c))

        @at_step(k, 2)
        def _():
            got("gc", dg_core)
            copy_of("gc", "gc", dg, dg_core, to_c).wait_send()
            dg[...] = dg[...] + dg_core[...]
            push("gx", lambda: (dg, dg_x, to_x))
            ag_got_dx("o0", o0_buf, half)
            ag_got_dy("o0", o0_buf, 1, half)
            partner_has("o0", o0_buf, 2)
            stage_o(o0_buf, block_of(2), 0)

        @at_step(k, 3)
        def _():
            got("gx", dg_x)
            copy_of("gx", "gx", dg, dg_x, to_x).wait_send()
            dg[...] = dg[...] + dg_x[...]
            push("gy", lambda: (dg, dg_y, to_y))

        def between():
            @at_step(k, 3)
            def _():
                grads_push(0)

        weight_grads(n_half(k), 0, ob.at[oslot], between)

        @at_step(k, 0)
        def _():
            staged_n(n0_buf, block_of(2), 0)
            with jax.named_scope("f0_last"):
                fwd(0, nb.at[0], None, a_kept(3), b_kept(3))

            @pl.when(outer == 1)
            def _():
                y_done()

            ag_got_x("o0", o0_buf, 0, half)
            ag_got_y("o0", o0_buf, 1)
            ag_got_x("o0", o0_buf, 1, half)
            partner_has("o0", o0_buf, 0)
            stage_o(o0_buf, block_of(0), 0)

        return carry

    def staged_o_any(k):
        for n, slot in ((1, 0), (2, 1), (3, 0)):
            @at_step(k, n)
            def _(n=n, slot=slot):
                staged_o(o0_buf, block_of(n - 1), slot)

    lax.fori_loop(0, 4, l0_step, 0)
    grads_out(0)
    for key in ("gc", "gx", "gy"):
        sent.pop(key)
    got("gy", dg_y)
    copy_of("gy", "gy", dg, dg_y, to_y).wait_send()
    dgain_out[...] = dg[...] + dg_y[...]
    for i in range(3):
        with jax.named_scope("got_y"):
            z_pass("y", lambda zi: (x_ch, y_rows(zi)), i)
    local("yk", x_ch, y_rows(z)).wait()
    grads_out_done(0)
    for key in list(sent):
        send_done(key)
    for s in "BC":
        for h in range(2):
            copy_of(("d2", s, h), ("d2", s, h), mine(0, h), slot("d2", 0, h), at_z(pair)).wait_send()

    assert not passed


def make_call(td, d, rb, hs):
    fb = hs // 4
    hh, t2, ch = 2 * fb, 2 * td, td // 4
    shape = jax.ShapeDtypeStruct
    hbm = pl.BlockSpec(memory_space=pl.ANY)
    vmem = pl.BlockSpec(memory_space=pltpu.VMEM)
    block = shape((4, 2, td, d), BF16)
    outs = [
        shape((td, d), BF16), shape((2, rb, hs), F32), shape((2, rb, hs), F32), shape((2, fb, d), F32), shape((2, d), F32),
        block, block, block, block, shape((4, t2, hh), BF16), shape((4, t2, hh), BF16), shape((td, d), BF16), shape((t2, hh), BF16), shape((td, d), F32),
    ]
    scratch = [
        pltpu.VMEM((2, d, hh), BF16), pltpu.VMEM((2, d, hh), BF16), pltpu.VMEM((2, hh, d), BF16),
        pltpu.VMEM((2 * rb, hh), F32), pltpu.VMEM((2 * rb, hh), F32), pltpu.VMEM((fb, d), F32),
        pltpu.VMEM((2, t2, d), BF16), pltpu.VMEM((2, t2, d), BF16),
        pltpu.VMEM((t2, hh), BF16), pltpu.VMEM((t2, hh), BF16), pltpu.VMEM((t2, hh), BF16),
        pltpu.VMEM((t2, d), F32), pltpu.VMEM((4, ch, d), F32),
        pltpu.VMEM((ch, d), BF16), pltpu.VMEM((ch, d), BF16),
        pltpu.VMEM((t2, 128), F32),
        pltpu.VMEM((2, d), F32), pltpu.VMEM((2, d), F32), pltpu.VMEM((2, d), F32), pltpu.VMEM((2, d), F32), pltpu.VMEM((4, 2, d), F32),
        pltpu.SemaphoreType.DMA((NSEM,)), pltpu.SemaphoreType.DMA((NSEM,)), pltpu.SemaphoreType.DMA((NLOC,)), pltpu.SemaphoreType.REGULAR,
    ]
    return pl.pallas_call(
        kernel,
        out_shape=outs,
        in_specs=[hbm] * 5 + [vmem],
        out_specs=[hbm] * 4 + [vmem] + [hbm] * 9,
        scratch_shapes=scratch,
        compiler_params=pltpu.CompilerParams(collective_id=0, has_side_effects=True, vmem_limit_bytes=67043328),
    )


def solution(mesh):
    tok_spec = P(("replica", "fsdp"), None)
    wide_spec = P(None, "fsdp", "tensor")
    down_spec = P(None, ("tensor", "fsdp"), None)
    gain_spec = P(None, None)

    def device_fn(x_loc, dy_loc, w_gate, w_up, w_down, norm_gain):
        call = make_call(x_loc.shape[0], x_loc.shape[1], w_gate.shape[1], w_gate.shape[2])
        return tuple(call(x_loc, dy_loc, w_gate, w_up, w_down, norm_gain)[:5])

    return jax.shard_map(device_fn, mesh=mesh, in_specs=(tok_spec, tok_spec, wide_spec, wide_spec, down_spec, gain_spec), out_specs=(tok_spec, wide_spec, wide_spec, down_spec, gain_spec), check_vma=False)
```

```python
import jax
import jax.numpy as jnp
from jax import lax
from jax.experimental import pallas as pl
from jax.experimental.pallas import tpu as pltpu
from jax.sharding import PartitionSpec as P

F32 = jnp.float32
BF16 = jnp.bfloat16
MESH = pl.DeviceIdType.MESH
NSEND = 174
NRECV = 176
NLOC = 55
VLIM = 67043328 - 16 * 2**20 - 2**17
VLIM2 = 14 * 2**20


def mm(lhs, rhs, ldim, rdim):
    return lax.dot_general(lhs, rhs, (((ldim,), (rdim,)), ((), ())), preferred_element_type=F32)


def kernel(
    x_in, dy_in, wg_in, wu_in, wd_in, gain,
    y_out, dwg1, dwu1, dwd1, dgain_out, acc_g, acc_u, acc_d, part, n0_buf, n1_buf, o1_buf, o0_buf, a_save, b_save, x_part, g_save, core_hbm,
    wg, wu, wd, nb, ob, a_t, b_t, g_t, from_z,
    x_ch, h1_ch, r_own, dg, dg_core, dg_x, dg_y, dg_z, ssem, rsem, lsem, credit,
):
    td, d = x_in.shape
    rb = wg_in.shape[1]
    fb = wg_in.shape[2] // 4
    hh = 2 * fb
    t2, ch, half = 2 * td, td // 4, td // 2
    hc = ch // 2
    tile = min(512, fb)
    z = lax.axis_index("tensor")
    y = lax.axis_index("replica")
    f = lax.axis_index("fsdp")
    x, c = f // 2, f % 2
    xo, yo, co = 1 - x, 1 - y, 1 - c
    q, qx, qy, qd = 2 * y + x, 2 * y + xo, 2 * yo + x, 2 * yo + xo
    cs = (c + y) % 2
    cso = 1 - cs
    to_c, to_x, to_xs, to_y = {"fsdp": 2 * x + co}, {"fsdp": 2 * xo + c}, {"fsdp": 2 * xo + cs}, {"replica": yo}
    inner = ((z + 1) // 2) % 2
    outer = 1 - inner
    up = z // 2
    pair = z + 1 - 2 * (z % 2)
    far_outer, far_inner = 3 - 3 * up, 2 - up
    order = (outer * far_outer + inner * pair, outer * far_inner + inner * far_outer, outer * pair + inner * far_inner, z)

    n_own, o_own = nb.at[1], ob.at[1]

    def at_z(i):
        return {"tensor": i}

    def z_other(k):
        return (z + 4 + k * (1 - 2 * up)) % 4

    others = tuple(z_other(k) for k in (1, 2, 3))
    toward = outer * pair + inner * far_inner

    def rows(start, size):
        return pl.ds(start if isinstance(start, int) else pl.multiple_of(start, size if size % 16 == 0 else 8), size)

    def cols(start, size):
        return pl.ds(start if isinstance(start, int) else pl.multiple_of(start, 128), size)

    ids, sids, lids, sent, passed = {}, {}, {}, {}, {}

    def numbered(table, key, limit):
        i = table.setdefault(key, len(table))
        assert i < limit, i
        return i

    def sid(key):
        return numbered(ids, key, NRECV)

    def name_of(key):
        return key if isinstance(key, str) else "_".join(map(str, key))

    def copy_of(skey, rkey, src, dst, dev):
        send = 0 if skey is None else numbered(sids, skey, NSEND)
        recv = sid(rkey) if isinstance(rkey, (str, tuple)) else rkey
        return pltpu.make_async_remote_copy(src_ref=src, dst_ref=dst, send_sem=ssem.at[send], recv_sem=rsem.at[recv], device_id=dev, device_id_type=MESH)

    def push(key, make, rkey=None):
        copy_of(key, key if rkey is None else rkey, *make()).start()
        sent[key] = make

    def got(key, dst):
        with jax.named_scope("got_" + (name_of(key) if isinstance(key, (str, tuple)) else "dyn")):
            copy_of(None, key, dst, dst, to_c).wait_recv()

    def send_done(key):
        copy_of(key, 0, *sent.pop(key)()).wait_send()

    def flush(heads, layer=None):
        for key in list(sent):
            parts = (key,) if isinstance(key, str) else key
            if parts[0] in heads and (layer is None or parts[0][0] != "w" or parts[1] == layer):
                send_done(key)

    def local(key, src, dst):
        i = numbered(lids, key, NLOC)
        return pltpu.make_async_copy(src, dst, lsem.at[i])

    def scoped(fn):
        def run(*args):
            with jax.named_scope(fn.__name__):
                return fn(*args)

        return run

    gu = ((wg_in, wg), (wu_in, wu))
    pieces = (2, 2)

    def wview(m, l, row, xb, k=0, n=1):
        return gu[m][1].at[l, rows(row * rb + k * (rb // n), rb // n), cols(xb * fb, fb)]

    def wsrc(m, l, xb, core, k=0, n=1):
        return gu[m][0].at[l, pl.ds(k * (rb // n), rb // n), cols((2 * xb + core) * fb, fb)]

    def push_w(l, m):
        n = pieces[l]
        for xb in range(2):
            for k in range(n):
                push(("wx", l, m, xb, k), lambda xb=xb, k=k: (wsrc(m, l, xb, cs, k, n), wview(m, l, f, xb, k, n), to_xs))
        for k in range(4 * m):
            r0 = y * (fb // 2) + k * (fb // 8)
            push(("wdx", l, k), lambda r0=r0: (wd_in.at[l, rows(r0, fb // 8)], wd.at[l, rows(x * fb + r0, fb // 8)], to_x))
        if (l, m) == (1, 1):
            r1 = yo * (fb // 2) + 3 * (fb // 8)
            push("wdx_last", lambda: (wd_in.at[l, rows(r1, fb // 8)], wd.at[l, rows(x * fb + r1, fb // 8)], to_x))

    def push_wc(l):
        for m in range(2):
            for xb in range(2):
                push(("wc", l, m, xb), lambda m=m, xb=xb: (wsrc(m, l, xb, co), wview(m, l, f, xb), to_c))
                local(("w", l, m, xb), wsrc(m, l, xb, c), wview(m, l, f, xb)).start()
        local(("wd", l), wd_in.at[l], wd.at[l, rows(x * fb, fb)]).start()

    def relay_gu(l, m, xb):
        n = pieces[l]
        for k in range(n):
            ref = lambda k=k: wview(m, l, 2 * xo + cs, xb, k, n)
            got(("wx", l, m, xb, k), ref())
            push(("wy", l, m, xb, k), lambda k=k: (ref(k), ref(k), to_y))

    def relay_d(l, k):
        ref = lambda: wd.at[l, rows(xo * fb + y * (fb // 2) + k * (fb // 8), fb // 8)]
        got(("wdx", l, k), ref())
        push(("wdy", l, k), lambda: (ref(), ref(), to_y))

    def have_gu(l, m, xb):
        n = pieces[l]
        local(("w", l, m, xb), wsrc(m, l, xb, c), wview(m, l, f, xb)).wait()
        got(("wc", l, m, xb), wview(m, l, 2 * x + co, xb))
        for k in range(n):
            got(("wy", l, m, xb, k), wview(m, l, 2 * xo + cso, xb, k, n))

    def have_d_own(l):
        local(("wd", l), wd_in.at[l], wd.at[l, rows(x * fb, fb)]).wait()

    def have_d(l):
        for k in range(4 - l):
            got(("wdy", l, k), wd.at[l, rows(xo * fb + yo * (fb // 2) + k * (fb // 8), fb // 8)])
        if l == 1:
            got(("wdx", 1, 3), wd.at[1, rows(xo * fb + y * (fb // 2) + 3 * (fb // 8), fb // 8)])
            got("wdx_last", wd.at[1, rows(xo * fb + yo * (fb // 2) + 3 * (fb // 8), fb // 8)])

    def piece(buf, block, core, start, size):
        return buf.at[block, core, pl.ds(start, size)]

    def chunk(buf, block, core, zi):
        return buf.at[block, core, rows(zi * ch, ch)]

    def part_id(a, j):
        base = sid((a, "p", 0))
        for jj in range(3):
            assert sid((a, "p", jj)) == base + jj
        return base + j

    def share(a, j, tag, ref):
        push((a, "s", j, tag), lambda: (ref(), ref(), to_c), (a, "p", j))

    def ag_x(a, buf, src, h):
        push((a, "x", h), lambda: (src().at[pl.ds(h * half, half)], piece(buf, q, c, h * half, half), to_x))

    def ag_y(a, buf, src, h):
        push((a, "y", h), lambda: (src().at[pl.ds(h * half, half)], piece(buf, q, c, h * half, half), to_y))

    def ag_quarter(a, buf, src, axis):
        push((a, axis + "c"), lambda: (src().at[rows(z * ch, ch)], chunk(buf, q, c, z), to_y if axis == "y" else to_x))

    def zb_id(a, axis, zi):
        base = sid((a, axis, "zb", 0))
        for i in range(4):
            assert sid((a, axis, "zb", i)) == base + i
        return base + zi

    def ag_spread(a, buf, axis):
        block = qy if axis == "y" else qx
        got((a, axis + "c"), chunk(buf, block, c, z))
        for k in (1, 2, 3):
            push((a, axis, "zs", k), lambda k=k: (chunk(buf, block, c, z), chunk(buf, block, c, z), at_z(z_other(k))), zb_id(a, axis, z))

    def ag_spread_got(a, buf, axis):
        block = qy if axis == "y" else qx
        for k in (1, 2, 3):
            with jax.named_scope("got_zb_" + a + axis):
                got(zb_id(a, axis, z_other(k)), chunk(buf, block, c, z_other(k)))
        share(a, 0 if axis == "y" else 1, 0, lambda: buf.at[block, c])

    def ag_dx(a, buf, cut):
        push((a, "dx"), lambda: (piece(buf, qy, c, 0, cut), piece(buf, qy, c, 0, cut), to_x))

    def ag_got_y(a, buf, h):
        got((a, "y", h), piece(buf, qy, c, h * half, half))
        share(a, 0, h, lambda: piece(buf, qy, c, h * half, half))
        if h == 0:
            ag_dx(a, buf, half)

    def ag_dy(a, buf, cut):
        push((a, "dy", 0), lambda: (piece(buf, qx, c, cut, td - cut), piece(buf, qx, c, cut, td - cut), to_y))

    def ag_got_dy_whole(a, buf, cut):
        got((a, "dy", 0), piece(buf, qd, c, cut, td - cut))
        share(a, 2, 0, lambda: piece(buf, qd, c, cut, td - cut))

    def diag_piece(h, cut):
        start = max(cut, h * half)
        return start, (h + 1) * half - start

    def ag_got_x(a, buf, h, cut):
        got((a, "x", h), piece(buf, qx, c, h * half, half))
        start, size = diag_piece(h, cut)
        if size:
            push((a, "dy", h), lambda: (piece(buf, qx, c, start, size), piece(buf, qx, c, start, size), to_y))
        share(a, 1, h, lambda: piece(buf, qx, c, h * half, half))

    def ag_got_dx(a, buf, cut):
        got((a, "dx"), piece(buf, qd, c, 0, cut))
        share(a, 2, "x", lambda: piece(buf, qd, c, 0, cut))

    def ag_got_dy(a, buf, h, cut):
        start, size = diag_piece(h, cut)
        if size:
            got((a, "dy", h), piece(buf, qd, c, start, size))
            share(a, 2, h, lambda: piece(buf, qd, c, start, size))

    def block_of(j):
        return 2 * ((y + (j + 1) % 2) % 2) + (x + (j + 1) // 2) % 2

    def partner_has(a, buf, j):
        with jax.named_scope("got_p_" + a):
            got(part_id(a, j), buf.at[block_of(j), co])

    for a in ("n0", "o1", "n1", "o0"):
        for j in range(3):
            sid((a, "p", j))
    for a, axis in (("n0", "y"), ("n0", "x"), ("o1", "y")):
        for i in range(4):
            sid((a, axis, "zb", i))

    def fwd_tile(l, n_ref, g_ref, i, a_ref=None, b_ref=None):
        w = cols(i * tile, tile)
        a = mm(n_ref[...], wg[l, :, w], 1, 0).astype(BF16)
        b = mm(n_ref[...], wu[l, :, w], 1, 0).astype(BF16)
        (a_t if a_ref is None else a_ref)[:, w] = a
        (b_t if b_ref is None else b_ref)[:, w] = b
        if g_ref is not None:
            a_f = a.astype(F32)
            g_ref[:, w] = (a_f * jax.nn.sigmoid(a_f) * b.astype(F32)).astype(BF16)

    @scoped
    def fwd(l, n_ref, g_ref, a_ref=None, b_ref=None):
        def step(i, carry):
            fwd_tile(l, n_ref, g_ref, i, a_ref, b_ref)
            return carry

        lax.fori_loop(0, hh // tile, step, 0)

    @scoped
    def down_half(l, g_ref, kb, start, size, add):
        r, k = rows(start, size), pl.ds(pl.multiple_of(kb * fb, fb), fb)

        def step(i, carry):
            w = cols(i * tile, tile)
            new = mm(g_ref[r, k], wd[l, k, w], 1, 0)
            part[r, w] = part[r, w] + new if add else new
            return carry

        lax.fori_loop(0, d // tile, step, 0)

    @scoped
    def down_rows(l, g_ref, core):
        r = rows(core * td, td)

        def step(i, carry):
            w = cols(i * tile, tile)
            part[r, w] = mm(g_ref[r, :], wd[l, :, w], 1, 0)
            return carry

        lax.fori_loop(0, d // tile, step, 0)

    @scoped
    def m_half(l, kb, start, size, add):
        r, k = rows(start, size), pl.ds(pl.multiple_of(kb * fb, fb), fb)

        def step(i, carry):
            w = rows(i * tile, tile)
            new = mm(a_t[r, k], wg[l, w, k], 1, 1) + mm(b_t[r, k], wu[l, w, k], 1, 1)
            o = cols(i * tile, tile)
            part[r, o] = part[r, o] + new if add else new
            return carry

        lax.fori_loop(0, d // tile, step, 0)

    def bwd_tile(l, o_ref, i, a_ref, b_ref):
        w = cols(i * tile, tile)
        q_f = mm(o_ref[...], wd[l, rows(i * tile, tile)], 1, 1).astype(BF16).astype(F32)
        a_f, b_f = a_ref[:, w].astype(F32), b_ref[:, w].astype(F32)
        s = jax.nn.sigmoid(a_f)
        g_t[:, w] = (a_f * s * b_f).astype(BF16)
        a_t[:, w] = (q_f * b_f * s * (1.0 + a_f * (1.0 - s))).astype(BF16)
        b_t[:, w] = (q_f * a_f * s).astype(BF16)

    @scoped
    def bwd_hidden(l, o_ref, a_ref, b_ref):
        for i in range(hh // tile):
            bwd_tile(l, o_ref, i, a_ref, b_ref)

    @scoped
    def weight_grads(n_ref, col, o_ref, between):
        t = min(256, fb)

        def half_rows(core):
            for i in range(rb // t):
                n_rows = n_ref[:, cols(col + core * rb + i * t, t)]
                w = rows(core * rb + i * t, t)
                acc_g[w, :] += mm(n_rows, a_t[...], 0, 0)
                acc_u[w, :] += mm(n_rows, b_t[...], 0, 0)

        half_rows(co)
        if between is not None:
            between()
        half_rows(c)
        for i in range(fb // t):
            acc_d[pl.ds(i * t, t), :] += mm(g_t[:, cols(x * fb + i * t, t)], o_ref[...], 0, 0)

    @scoped
    def zero_acc():
        for ref in (acc_g, acc_u, acc_d):
            def step(i, carry, ref=ref):
                ref[rows(i * 16, 16), :] = jnp.zeros((16, ref.shape[1]), F32)
                return carry

            lax.fori_loop(0, ref.shape[0] // 16, step, 0)

    def rinv(h_f):
        return lax.rsqrt(jnp.mean(h_f * h_f, axis=-1, keepdims=True) + 1e-6)

    def core_land(key):
        return core_hbm if key == "d2" else acc_d

    def core_push(key):
        for k in range(4):
            push((key, "c", k), lambda k=k: (part.at[rows(co * td + order[k] * ch, ch)], core_land(key).at[rows(order[k] * ch, ch)], to_c))

    def z_ids(key):
        base = sid((key, "A", 0))
        for h in range(2):
            for i, s in enumerate("ABCD"):
                assert sid((key, s, h)) == base + 4 * h + i
        return base

    for sum_key in ("d0", "d1", "d2"):
        z_ids(sum_key)

    def mine(zi, h):
        return part.at[rows(c * td + zi * ch + h * hc, hc)]

    def slot(key, i, h):
        return from_z.at[i, pl.ds(h * hc, hc)]

    def core_back(k):
        return local(("cl", k), core_hbm.at[rows(order[k] * ch, ch)], part.at[rows(co * td + order[k] * ch, ch)])

    def core_back_start(key):
        for k in range(4):
            got((key, "c", k), core_land(key).at[rows(order[k] * ch, ch)])
            send_done((key, "c", k))
            core_back(k).start()

    @scoped
    def core_sum_send(key):
        z_ids(key)
        for k in range(4):
            if key == "d2":
                core_back(k).wait()
            else:
                got((key, "c", k), core_land(key).at[rows(order[k] * ch, ch)])

            def step(i, carry):
                r = order[k] * ch + i * 16
                mine_r = rows(c * td + r, 16)
                part[mine_r, :] = part[mine_r, :] + (part[rows(co * td + r, 16), :] if key == "d2" else acc_d[rows(r, 16), :])
                return carry

            lax.fori_loop(0, ch // 16, step, 0)
            if k == 0:
                for h in range(2):
                    push((key, "A", h), lambda h=h: (mine(order[0], h), slot(key, 0, h), at_z(pair)))
            elif k < 3:
                @pl.when(outer == 1)
                def _():
                    for h in range(2):
                        copy_of((key, "BC"[k - 1], h), (key, "BC"[k - 1], h), mine(order[k], h), slot(key, k, h), at_z(pair)).start()


    def z_relay(key, n, h):
        @pl.when(inner == 1)
        def _():
            got((key, "AB"[n], h), slot(key, n, h))
            zi = (far_outer, far_inner)[n]
            work = slot(key, n, h)

            def step(i, carry):
                r = rows(i * 8, 8)
                work[r, :] = work[r, :] + part[rows(c * td + zi * ch + h * hc + i * 8, 8), :]
                return carry

            lax.fori_loop(0, hc // 8, step, 0)
            if n == 0:
                copy_of((key, "B", h), (key, "B", h), work, slot(key, 1, h), at_z(far_outer)).start()
            else:
                copy_of((key, "C", h), (key, "D", h), work, slot(key, 3, h), at_z(far_inner)).start()

    def z_got(key):
        base = z_ids(key)
        for h in range(2):
            for i in range(2):
                with jax.named_scope("got_" + key):
                    got(base + 4 * h + 2 * inner + i, slot(key, 2 * inner + i, h))

    def z_sum(key, i):
        r = rows(i * 16, 16)
        return part[rows(c * td + z * ch + i * 16, 16), :] + from_z[2 * inner, r, :] + from_z[2 * inner + 1, r, :]

    def relay_sends_done(key):
        @pl.when(inner == 1)
        def _():
            for s in "BC":
                for h in range(2):
                    copy_of((key, s, h), 0, mine(0, h), slot(key, 0, h), at_z(pair)).wait_send()

    def sum_sends_done(key):
        for part_key in [(key, "c", k) for k in range(4)] + [(key, "A", h) for h in range(2)]:
            send_done(part_key)

        @pl.when(outer == 1)
        def _():
            for s in "BC":
                for h in range(2):
                    copy_of((key, s, h), 0, mine(0, h), slot(key, 0, h), at_z(pair)).wait_send()

    def quarter(ref, core, zi):
        return ref.at[rows(core * td + zi * ch, ch)]

    def zg_id(key, zi):
        base = sid((key, "z", 0))
        for i in range(4):
            assert sid((key, "z", i)) == base + i
        return base + zi

    relayed = ("n1z",)

    def takes(key):
        return (pair, far_inner, far_outer) if key in relayed else others

    def z_push(key, make, zi):
        for k, dev in enumerate((toward,) if key in relayed else others):
            push((key, "zs", k), lambda dev=dev: (*make(zi), at_z(dev)), zg_id(key, zi))
        if key in relayed:
            z_forward(key, 3, make(zi)[1], zg_id(key, zi), pair)
            passed[(key, "fw", 3)] = lambda: make(z)[1]

    def z_forward(key, i, ref, rkey, dev):
        @pl.when(inner == 1)
        def _():
            copy_of((key, "fw", i), rkey, ref, ref, at_z(dev)).start()

    def z_pass(key, make, i):
        zi = takes(key)[i]
        with jax.named_scope("got_%s_%d" % (key, i)):
            got(zg_id(key, zi), make(zi)[1])
        if key in relayed:
            z_forward(key, i, make(zi)[1], zg_id(key, zi), (far_inner, pair, pair)[i])
            passed[(key, "fw", i)] = lambda: make(zi)[1]

    def passed_done(which):
        @pl.when(inner == 1)
        def _():
            for key in [k1 for k1 in passed if k1[0] == which]:
                ref = passed.pop(key)
                copy_of(key, 0, ref(), ref(), to_c).wait_send()

    def z_gather(key, ref):
        z_push(key, lambda zi: (quarter(ref, c, zi), quarter(ref, c, zi)), z)
        push((key, "s", 0), lambda: (quarter(ref, c, z), quarter(ref, c, z), to_c))

    def z_take(key, ref, i):
        z_pass(key, lambda zi: (quarter(ref, c, zi), quarter(ref, c, zi)), i)
        push((key, "s", 1 + i), lambda: (quarter(ref, c, takes(key)[i]), quarter(ref, c, takes(key)[i]), to_c))

    def z_gathered_partner(key, ref):
        got((key, "s", 0), quarter(ref, co, z))
        for i in range(3):
            got((key, "s", 1 + i), quarter(ref, co, takes(key)[i]))

    def stage(buf, block, slot_ref, key):
        for core in range(2):
            local((key, core), buf.at[block, core], slot_ref.at[pl.ds(core * td, td)]).start()

    def staged(buf, block, slot_ref, key):
        for core in range(2):
            local((key, core), buf.at[block, core], slot_ref.at[pl.ds(core * td, td)]).wait()

    def save_ab(block):
        return (local("sa", a_t, a_save.at[block]), local("sb", b_t, b_save.at[block]))

    @scoped
    def f0_other(j, slot):
        fwd(0, nb.at[slot], None)
        for s in save_ab(block_of(j)):
            s.start()

    def saves_done(block):
        for s in save_ab(block):
            s.wait()

    def a_kept(k):
        return wg.at[1, rows(k * t2, t2)]

    def b_kept(k):
        return wd.at[1, rows((k // 2) * t2, t2), cols((k % 2) * hh, hh)]

    def load_ab(block, k):
        return (local(("la", k), a_save.at[block], a_kept(k)), local(("lb", k), b_save.at[block], b_kept(k)))

    def grad_piece(i, xb, core):
        return (acc_g, acc_u)[i].at[rows(core * rb, rb), cols(xb * fb, fb)]

    def grad_land(l, i, xb, core):
        if l == 1:
            return (dwg1, dwu1)[i].at[:, cols((2 * xb + core) * fb, fb)]
        return part.at[:, cols(i * hh + xb * fb, fb)]

    def grads_push(l):
        for i in range(2):
            for xb in range(2):
                push(("q", l, i, xb), lambda i=i, xb=xb: (grad_piece(i, xb, co), grad_land(l, i, xb, c), to_c))

    def grads_out():
        for i in range(2):
            for xb in range(2):
                local(("qo", i, xb), grad_piece(i, xb, c), grad_land(1, i, xb, c)).start()
        local("qd", acc_d, dwd1).start()

    @scoped
    def grads_out_done(l):
        for i in range(2):
            for xb in range(2):
                if l == 1:
                    local(("qo", i, xb), grad_piece(i, xb, c), grad_land(1, i, xb, c)).wait()
                send_done(("q", l, i, xb))
                got(("q", l, i, xb), grad_land(l, i, xb, co))
        if l == 1:
            local("qd", acc_d, dwd1).wait()

    barrier = pltpu.get_barrier_semaphore()
    for dev in (to_c, to_x, {"fsdp": 2 * xo + co}, to_y, at_z((z + 1) % 4), at_z((z + 2) % 4), at_z((z + 3) % 4)):
        pl.semaphore_signal(barrier, inc=1, device_id=dev, device_id_type=MESH)
    x_load = local("x", x_in, nb.at[1, pl.ds(0, td)])
    x_load.start()
    with jax.named_scope("barrier"):
        pl.semaphore_wait(barrier, 7)

    dy_src = lambda: dy_in
    n0_src = lambda: n0_buf.at[q, c]
    n1_src = lambda: n_own.at[rows(c * td, td)]
    o0_src = lambda: o_own.at[rows(c * td, td)]
    cut_n, cut_o = ch, half

    push_w(0, 0)
    push_wc(0)
    x_load.wait()

    def n0_step(i, carry):
        h_f = n_own[rows(i * 16, 16), :].astype(F32)
        r_inv = rinv(h_f)
        nb[0, rows(c * td + i * 16, 16), :] = (h_f * r_inv * gain[0:1, :]).astype(BF16)
        r_own[rows(c * td + i * 16, 16), :] = jnp.broadcast_to(r_inv, (16, 128))
        return carry

    lax.fori_loop(0, td // 16, n0_step, 0)
    n0_mine = lambda: nb.at[0, rows(c * td, td)]
    push("n0p", lambda: (n0_mine(), n0_mine(), to_c))
    r_mine = lambda: r_own.at[rows(c * td, td)]
    push("rp", lambda: (r_mine(), r_mine(), to_c))
    keep = local("n0k", n0_mine(), n0_buf.at[q, c])
    keep.start()
    keep.wait()
    ag_quarter("n0", n0_buf, n0_src, "y")
    ag_quarter("n0", n0_buf, n0_src, "x")
    ag_quarter("o1", o1_buf, dy_src, "y")
    push_w(0, 1)
    push_w(1, 0)
    push_w(1, 1)
    ag_x("o1", o1_buf, dy_src, 0)
    push("xp", lambda: (x_in, x_part, to_c))
    push("dyp", lambda: (dy_in, o1_buf.at[q, c], to_c))
    push_wc(1)
    local("xc", x_in.at[rows(z * ch, ch)], x_ch).start()
    local("dy_own", dy_in, ob.at[0, rows(c * td, td)]).start()

    @scoped
    def h1_calc():
        def h1_step(i, carry):
            r = rows(i * 16, 16)
            h1 = (x_ch[r, :].astype(F32) + z_sum("d0", i)).astype(BF16)
            h1_ch[r, :] = h1
            h_f = h1.astype(F32)
            n_own[rows(c * td + z * ch + i * 16, 16), :] = (h_f * rinv(h_f) * gain[1:2, :]).astype(BF16)
            return carry

        lax.fori_loop(0, ch // 16, h1_step, 0)

    def h1_done():
        z_got("d0")
        relay_sends_done("d0")
        h1_calc()
        z_gather("n1z", n_own)

    relay_gu(0, 0, 0)
    ag_spread("n0", n0_buf, "y")
    ag_spread("o1", o1_buf, "y")
    relay_gu(0, 0, 1)
    ag_spread("n0", n0_buf, "x")
    relay_gu(0, 1, 0)
    relay_gu(0, 1, 1)
    got("n0p", nb.at[0, rows(co * td, td)])
    got("rp", r_own.at[rows(co * td, td)])
    keep2 = local("n0k2", nb.at[0, rows(co * td, td)], n0_buf.at[q, co])
    keep2.start()
    have_gu(0, 0, 0)
    have_gu(0, 1, 0)
    with jax.named_scope("fwd_tile0"):
        fwd_tile(0, nb.at[0], g_t, 0)
    relay_d(0, 0)
    relay_d(0, 1)
    have_gu(0, 0, 1)
    have_gu(0, 1, 1)
    with jax.named_scope("fwd_tile1"):
        for i in range(1, hh // tile):
            fwd_tile(0, nb.at[0], g_t, i)
    for s in save_ab(q):
        s.start()
    have_d_own(0)
    relay_d(0, 2)
    down_half(0, g_t, x, 0, t2, False)
    relay_d(0, 3)
    ag_spread_got("n0", n0_buf, "y")
    have_d(0)
    down_half(0, g_t, xo, co * td, td, True)
    core_push("d0")
    down_half(0, g_t, xo, c * td, td, True)
    core_sum_send("d0")
    keep2.wait()
    send_done("n0p")
    saves_done(q)
    partner_has("n0", n0_buf, 0)
    stage(n0_buf, block_of(0), nb.at[0], "sn")
    relay_gu(1, 0, 0)
    staged(n0_buf, block_of(0), nb.at[0], "sn")
    f0_other(0, 0)
    z_relay("d0", 0, 0)
    relay_gu(1, 0, 1)
    z_relay("d0", 0, 1)
    ag_spread_got("n0", n0_buf, "x")
    ag_spread_got("o1", o1_buf, "y")
    partner_has("n0", n0_buf, 1)
    stage(n0_buf, block_of(1), nb.at[0], "sn")
    z_relay("d0", 1, 0)
    relay_gu(1, 1, 0)
    z_relay("d0", 1, 1)
    local("xc", x_in.at[rows(z * ch, ch)], x_ch).wait()

    @pl.when(outer == 1)
    def _():
        h1_done()

    relay_gu(1, 1, 1)

    @pl.when(inner == 1)
    def _():
        h1_done()

    local("dyc", dy_in.at[rows(z * ch, ch)], x_ch).start()
    flush(("wx", "wdx", "wc", "wy", "wdy", "xp", "dyp", "rp"), 0)
    relay_d(1, 0)
    z_take("n1z", n_own, 0)
    z_take("n1z", n_own, 1)
    relay_d(1, 1)
    z_take("n1z", n_own, 2)
    relay_d(1, 2)
    saves_done(block_of(0))
    for h in range(2):
        ag_x("n1", n1_buf, n1_src, h)
    ag_x("o1", o1_buf, dy_src, 1)
    for h in range(2):
        ag_y("n1", n1_buf, n1_src, h)
    got("dyp", o1_buf.at[q, co])
    dy_other = local("dy_other", o1_buf.at[q, co], ob.at[0, rows(co * td, td)])
    dy_other.start()
    z_gathered_partner("n1z", n_own)

    for m in range(2):
        for xb in range(2):
            have_gu(1, m, xb)
    fwd(1, n_own, g_t)
    local("dy_own", dy_in, ob.at[0, rows(c * td, td)]).wait()
    dy_other.wait()
    have_d_own(1)
    bwd_tile(1, ob.at[0], x, a_t, b_t)
    sum_sends_done("d0")
    m_half(1, x, 0, t2, False)
    have_d(1)
    bwd_tile(1, ob.at[0], xo, a_t, b_t)
    g_keep = local("gk", g_t, g_save)
    g_keep.start()
    m_half(1, xo, co * td, td, True)
    core_push("d1")
    m_half(1, xo, c * td, td, True)
    core_sum_send("d1")
    zero_acc()
    g_keep.wait()
    local("dyc", dy_in.at[rows(z * ch, ch)], x_ch).wait()

    @scoped
    def e_calc():
        def e_step(i, dg1):
            r = rows(i * 16, 16)
            m = z_sum("d1", i)
            h_f = h1_ch[r, :].astype(F32)
            r_inv = rinv(h_f)
            xh = h_f * r_inv
            v = m * gain[1:2, :]
            e = x_ch[r, :].astype(F32) + r_inv * (v - xh * jnp.mean(v * xh, axis=-1, keepdims=True))
            o_own[rows(c * td + z * ch + i * 16, 16), :] = e.astype(BF16)
            return dg1 + jnp.sum(m * xh, axis=0, keepdims=True)

        dg[1:2, :] = lax.fori_loop(0, ch // 16, e_step, jnp.zeros((1, d), F32))

    def at_step(k, n):
        return pl.when(k == n)

    def stage_n(buf, block, slot):
        stage(buf, block, nb.at[slot], ("n", slot))

    def staged_n(buf, block, slot):
        staged(buf, block, nb.at[slot], ("n", slot))

    def stage_o(buf, block, slot):
        stage(buf, block, ob.at[slot], ("o", slot))

    def staged_o(buf, block, slot):
        staged(buf, block, ob.at[slot], ("o", slot))

    xl = lambda: [local("xl0", x_in, nb.at[0, rows(c * td, td)]), local("xl1", x_part, nb.at[0, rows(co * td, td)])]

    def n_half(slot):
        return wu.at[1, rows(slot * t2, t2)]

    def n_half_copies(block, slot):
        return [local(("nh", slot, core), n0_buf.at[block, core, :, cols(2 * x * rb, 2 * rb)], wu.at[1, rows(slot * t2 + core * td, td)]) for core in range(2)]

    def load_n_half(block, slot):
        for s in n_half_copies(block, slot):
            s.start()

    own_g = nb.at[1, :, pl.ds(0, hh)]

    def e_done():
        z_got("d1")
        relay_sends_done("d1")
        e_calc()
        z_gather("o0z", o_own)
        for dev in others:
            pl.semaphore_signal(credit, inc=1, device_id=at_z(dev), device_id_type=MESH)

    def l1_step(k, carry):
        slot = 1 - (k + 3) // 4

        @pl.when(k > 0)
        def _():
            @at_step(k, 1)
            def _():
                partner_has("o1", o1_buf, 0)
                stage_o(o1_buf, block_of(0), 0)

            staged_n(n1_buf, block_of(k - 1), 0)
            with jax.named_scope("fwd_a"):
                fwd_tile(1, nb.at[0], None, 0)

            @at_step(k, 2)
            def _():
                ag_got_x("o1", o1_buf, 1, cut_o)

            @at_step(k, 3)
            def _():
                ag_got_dx("o1", o1_buf, cut_o)
                for h in range(2):
                    ag_got_dy("o1", o1_buf, h, cut_o)

            with jax.named_scope("fwd_b"):
                for i in range(1, hh // tile):
                    fwd_tile(1, nb.at[0], None, i)

            @pl.when(k * inner == 2)
            def _():
                e_done()

            @pl.when(k > 1)
            def _():
                partner_has("o1", o1_buf, k - 1)
                stage_o(o1_buf, block_of(k - 1), 0)

            @at_step(k, 3)
            def _():
                for i in range(3):
                    z_take("o0z", o_own, i)
                for h in range(2):
                    ag_x("o0", o0_buf, o0_src, h)
                    ag_y("o0", o0_buf, o0_src, h)

            @at_step(k, 1)
            def _():
                z_relay("d1", 1, 0)
                ag_got_x("n1", n1_buf, 1, half)

            staged_o(o1_buf, block_of(k - 1), 0)
            bwd_hidden(1, ob.at[0], a_t, b_t)

            @at_step(k, 1)
            def _():
                z_relay("d1", 1, 1)

                @pl.when(outer == 1)
                def _():
                    e_done()

                partner_has("n1", n1_buf, 1)

            @at_step(k, 2)
            def _():
                local("gl", g_save, own_g).wait()
                sum_sends_done("d1")
                down_rows(1, own_g, co)
                core_push("d2")
                ag_got_dx("n1", n1_buf, half)
                ag_got_dy("n1", n1_buf, 1, half)
                down_rows(1, own_g, c)
                core_back_start("d2")

            @at_step(k, 1)
            def _():
                for key in [("n1z", "zs", 0)] + [("n1z", "s", i) for i in range(4)] + [("n1", axis, h) for axis in "xy" for h in range(2)]:
                    send_done(key)
                passed_done("n1z")
                local("gl", g_save, own_g).start()

            @at_step(k, 3)
            def _():
                z_relay("d2", 0, 0)
                for key in [k1 for k1 in sent if k1[0] in ("wy", "wdy") and k1[1] == 1]:
                    send_done(key)
                for i in range(3):
                    for s in load_ab(block_of(i - 1) if i else q, i):
                        s.start()
                    load_n_half(block_of(i - 1) if i else q, i)

        weight_grads(nb.at[slot], 2 * x * rb, ob.at[0], None)

        @at_step(k, 1)
        def _():
            stage_n(n1_buf, block_of(1), 0)

        @at_step(k, 2)
        def _():
            partner_has("n1", n1_buf, 2)
            stage_n(n1_buf, block_of(2), 0)
            pl.semaphore_wait(credit, 3)
            core_sum_send("d2")

        @at_step(k, 0)
        def _():
            staged(n0_buf, block_of(1), nb.at[0], "sn")
            f0_other(1, 0)
            ag_got_x("o1", o1_buf, 0, cut_o)
            ag_got_x("n1", n1_buf, 0, half)
            z_relay("d1", 0, 0)
            ag_got_y("n1", n1_buf, 0)
            ag_dx("o1", o1_buf, cut_o)
            ag_dx("n0", n0_buf, cut_n)
            ag_dy("n0", n0_buf, cut_n)
            z_relay("d1", 0, 1)
            ag_got_y("n1", n1_buf, 1)
            partner_has("n1", n1_buf, 0)
            stage_n(n1_buf, block_of(0), 0)
            saves_done(block_of(1))

        return carry

    lax.fori_loop(0, 4, l1_step, 0)
    got("xp", x_part)
    for s in xl():
        s.start()
    for s in load_ab(q, 0):
        s.wait()
    z_gathered_partner("o0z", o_own)
    z_relay("d2", 0, 1)
    grads_push(1)
    grads_out()

    def gz_id(zi):
        base = sid(("gz", 0))
        for i in range(4):
            assert sid(("gz", i)) == base + i
        return base + zi

    def y_rows(zi):
        return y_out.at[rows(zi * ch, ch)]

    gz_id(0)
    zg_id("y", 0)

    @scoped
    def dgain0():
        def dg_step(i, carry):
            w = cols(i * tile, tile)
            m = mm(a_t[...], wg[0, rows(i * tile, tile)], 1, 1) + mm(b_t[...], wu[0, rows(i * tile, tile)], 1, 1)
            xh = nb[0, :, w].astype(F32) * r_own[:, 0:1]
            dg[0:1, w] = jnp.sum(m * xh, axis=0, keepdims=True)
            return carry

        lax.fori_loop(0, d // tile, dg_step, 0)

    def y_done():
        z_got("d2")

        def y_step(i, carry):
            r = rows(i * 16, 16)
            x_ch[r, :] = (h1_ch[r, :].astype(F32) + z_sum("d2", i)).astype(BF16)
            return carry

        lax.fori_loop(0, ch // 16, y_step, 0)
        local("yk", x_ch, y_rows(z)).start()
        z_push("y", lambda zi: (x_ch, y_rows(zi)), z)

    def l0_step(k, carry):
        oslot = (k + 1) % 2

        @pl.when(k > 0)
        def _():
            staged_o_any(k)

        bwd_hidden(0, ob.at[oslot], a_kept(k), b_kept(k))

        @at_step(k, 0)
        def _():
            for s in xl():
                s.wait()
            ag_got_dx("n0", n0_buf, cut_n)
            ag_got_dy_whole("n0", n0_buf, cut_n)
            z_relay("d2", 1, 0)
            dgain0()
            dg_z[z] = dg[...]
            for i in range(3):
                push(("gs", i), lambda i=i: (dg_z.at[z], dg_z.at[z], at_z(others[i])), gz_id(z))
            z_relay("d2", 1, 1)
            partner_has("n0", n0_buf, 2)
            stage_n(n0_buf, block_of(2), 0)
            load_n_half(block_of(2), 3)
            ag_got_y("o0", o0_buf, 0)
            grads_out_done(1)
            zero_acc()
            for i in range(4):
                for s in n_half_copies(block_of(i - 1) if i else q, i):
                    s.wait()
            for i in range(1, 3):
                for s in load_ab(block_of(i - 1), i):
                    s.wait()

        @at_step(k, 1)
        def _():
            @pl.when(inner == 1)
            def _():
                y_done()

            for h in range(2):
                send_done(("d2", "A", h))
                for s in "BC":
                    copy_of(("d2", s, h), 0, mine(0, h), slot("d2", 0, h), at_z(pair)).wait_send()
            partner_has("o0", o0_buf, 1)
            for key in [("o0z", "zs", i) for i in range(3)] + [("o0z", "s", i) for i in range(4)] + [("o0", axis, h) for axis in "xy" for h in range(2)]:
                send_done(key)
            stage_o(o0_buf, block_of(1), 1)
            for i in range(3):
                with jax.named_scope("got_gz"):
                    got(gz_id(others[i]), dg_z.at[others[i]])
                send_done(("gs", i))
            dg[...] = dg_z[0] + dg_z[1] + dg_z[2] + dg_z[3]
            push("gc", lambda: (dg, dg_core, to_c))

        @at_step(k, 2)
        def _():
            got("gc", dg_core)
            copy_of("gc", 0, dg, dg_core, to_c).wait_send()
            dg[...] = dg[...] + dg_core[...]
            push("gx", lambda: (dg, dg_x, to_x))
            ag_got_dx("o0", o0_buf, half)
            ag_got_dy("o0", o0_buf, 1, half)
            partner_has("o0", o0_buf, 2)
            stage_o(o0_buf, block_of(2), 0)

        @at_step(k, 3)
        def _():
            got("gx", dg_x)
            copy_of("gx", 0, dg, dg_x, to_x).wait_send()
            dg[...] = dg[...] + dg_x[...]
            push("gy", lambda: (dg, dg_y, to_y))

        def between():
            @at_step(k, 3)
            def _():
                grads_push(0)

        weight_grads(n_half(k), 0, ob.at[oslot], between)

        @at_step(k, 0)
        def _():
            staged_n(n0_buf, block_of(2), 0)
            with jax.named_scope("f0_last"):
                fwd(0, nb.at[0], None, a_kept(3), b_kept(3))

            @pl.when(outer == 1)
            def _():
                y_done()

            ag_got_x("o0", o0_buf, 0, half)
            ag_got_y("o0", o0_buf, 1)
            ag_got_x("o0", o0_buf, 1, half)
            flush(("wx", "wdx", "wdx_last", "wc", "n0", "o1", "n1"))
            partner_has("o0", o0_buf, 0)
            stage_o(o0_buf, block_of(0), 0)

        return carry

    def staged_o_any(k):
        for n, slot in ((1, 0), (2, 1), (3, 0)):
            @at_step(k, n)
            def _(n=n, slot=slot):
                staged_o(o0_buf, block_of(n - 1), slot)

    lax.fori_loop(0, 4, l0_step, 0)
    for key in ("gc", "gx", "gy"):
        sent.pop(key)
    got("gy", dg_y)
    copy_of("gy", 0, dg, dg_y, to_y).wait_send()
    dgain_out[...] = dg[...] + dg_y[...]
    for i in range(3):
        with jax.named_scope("got_y"):
            z_pass("y", lambda zi: (x_ch, y_rows(zi)), i)
    local("yk", x_ch, y_rows(z)).wait()
    grads_out_done(0)
    for key in list(sent):
        send_done(key)
    assert not passed


def finish(acc_g, acc_u, acc_d, other, g1, u1, d1, y_in, g_out, u_out, d_out, y_out, buf, ybuf, sem_in, sem_out):
    rb, hh = other.shape[0], acc_g.shape[1]
    fb = hh // 2
    f = lax.axis_index("fsdp")
    c = f % 2
    ins = [pltpu.make_async_copy(src, buf.at[i], sem_in.at[i]) for i, src in enumerate((g1, u1, d1))]
    ins.append(pltpu.make_async_copy(y_in, ybuf, sem_in.at[3]))
    for copy in ins:
        copy.start()
    outs = []

    def out(src, dst):
        copy = pltpu.make_async_copy(src, dst, sem_out.at[len(outs)])
        copy.start()
        outs.append(copy)

    for i, (acc, dst) in enumerate(((acc_g, g_out), (acc_u, u_out))):
        for xb in range(2):
            own = pl.ds(pl.multiple_of((2 * xb + c) * fb, 128), fb)
            out(acc.at[pl.ds(pl.multiple_of(c * rb, rb), rb), pl.ds(xb * fb, fb)], dst.at[0, :, own])
            theirs = pl.ds(pl.multiple_of((2 * xb + 1 - c) * fb, 128), fb)
            out(other.at[:, pl.ds(i * hh + xb * fb, fb)], dst.at[0, :, theirs])
    out(acc_d, d_out.at[0])
    for i, dst in enumerate((g_out, u_out, d_out)):
        ins[i].wait()
        out(buf.at[i], dst.at[1])
    ins[3].wait()
    out(ybuf, y_out)
    for copy in outs:
        copy.wait()


def make_call(td, d, rb, hs):
    fb = hs // 4
    hh, t2, ch = 2 * fb, 2 * td, td // 4
    shape = jax.ShapeDtypeStruct
    hbm = pl.BlockSpec(memory_space=pl.ANY)
    vmem = pl.BlockSpec(memory_space=pltpu.VMEM)
    block = shape((4, 2, td, d), BF16)
    outs = [
        shape((td, d), BF16), shape((rb, hs), F32), shape((rb, hs), F32), shape((fb, d), F32), shape((2, d), F32),
        pltpu.VMEM((2 * rb, hh), F32), pltpu.VMEM((2 * rb, hh), F32), pltpu.VMEM((fb, d), F32), pltpu.VMEM((t2, d), F32),
        block, block, block, block, shape((4, t2, hh), BF16), shape((4, t2, hh), BF16), shape((td, d), BF16), shape((t2, hh), BF16), shape((td, d), F32),
    ]
    scratch = [
        pltpu.VMEM((2, d, hh), BF16), pltpu.VMEM((2, d, hh), BF16), pltpu.VMEM((2, hh, d), BF16),
        pltpu.VMEM((2, t2, d), BF16), pltpu.VMEM((2, t2, d), BF16),
        pltpu.VMEM((t2, hh), BF16), pltpu.VMEM((t2, hh), BF16), pltpu.VMEM((t2, hh), BF16),
        pltpu.VMEM((4, ch, d), F32),
        pltpu.VMEM((ch, d), BF16), pltpu.VMEM((ch, d), BF16),
        pltpu.VMEM((t2, 128), F32),
        pltpu.VMEM((2, d), F32), pltpu.VMEM((2, d), F32), pltpu.VMEM((2, d), F32), pltpu.VMEM((2, d), F32), pltpu.VMEM((4, 2, d), F32),
        pltpu.SemaphoreType.DMA((NSEND,)), pltpu.SemaphoreType.DMA((NRECV,)), pltpu.SemaphoreType.DMA((NLOC,)), pltpu.SemaphoreType.REGULAR,
    ]
    step = pl.pallas_call(
        kernel,
        out_shape=outs,
        in_specs=[hbm] * 5 + [vmem],
        out_specs=[hbm] * 4 + [vmem] * 5 + [hbm] * 9,
        scratch_shapes=scratch,
        compiler_params=pltpu.CompilerParams(collective_id=0, has_side_effects=True, vmem_limit_bytes=VLIM),
    )
    end = pl.pallas_call(
        finish,
        out_shape=[shape((2, rb, hs), F32), shape((2, rb, hs), F32), shape((2, fb, d), F32), shape((td, d), BF16)],
        in_specs=[vmem] * 4 + [hbm] * 4,
        out_specs=[hbm] * 4,
        scratch_shapes=[pltpu.VMEM((3, rb, hs), F32), pltpu.VMEM((td, d), BF16), pltpu.SemaphoreType.DMA((4,)), pltpu.SemaphoreType.DMA((13,))],
        compiler_params=pltpu.CompilerParams(vmem_limit_bytes=VLIM2),
    )

    def call(*args):
        y, g1, u1, d1, dgain, acc_g, acc_u, acc_d, other = step(*args)[:9]
        kept = [pltpu.with_memory_space_constraint(v, pltpu.VMEM) for v in (acc_g, acc_u, acc_d, other)]
        stored = [pltpu.with_memory_space_constraint(v, pltpu.HBM) for v in (g1, u1, d1, y)]
        g, u, dd, y = end(*kept, *stored)
        return y, g, u, dd, dgain

    return call


def solution(mesh):
    tok_spec = P(("replica", "fsdp"), None)
    wide_spec = P(None, "fsdp", "tensor")
    down_spec = P(None, ("tensor", "fsdp"), None)
    gain_spec = P(None, None)

    def device_fn(x_loc, dy_loc, w_gate, w_up, w_down, norm_gain):
        call = make_call(x_loc.shape[0], x_loc.shape[1], w_gate.shape[1], w_gate.shape[2])
        return call(x_loc, dy_loc, w_gate, w_up, w_down, norm_gain)

    return jax.shard_map(device_fn, mesh=mesh, in_specs=(tok_spec, tok_spec, wide_spec, wide_spec, down_spec, gain_spec), out_specs=(tok_spec, wide_spec, wide_spec, down_spec, gain_spec), check_vma=False)
```

```python
import jax
import jax.numpy as jnp
import numpy as np
from jax import lax
from jax.experimental import pallas as pl
from jax.experimental.pallas import tpu as pltpu
from jax.sharding import PartitionSpec as P

F32 = jnp.float32
BF16 = jnp.bfloat16
MESH = pl.DeviceIdType.MESH
NSEND = 62
NRECV = 129
NLOC = 55
VLIM = 67043328 - 16 * 2**20 - 2**17
VLIM2 = 14 * 2**20


def mm(lhs, rhs, ldim, rdim):
    return lax.dot_general(lhs, rhs, (((ldim,), (rdim,)), ((), ())), preferred_element_type=F32)


def kernel(
    x_in, dy_in, wg_in, wu_in, wd_in, gain,
    y_out, dwg1, dwu1, dwd1, dgain_out, acc_g, acc_u, acc_d, part, n0_buf, n1_buf, o1_buf, o0_buf, a_save, b_save, x_part, g_save, core_hbm,
    wg, wu, wd, nb, ob, a_t, b_t, g_t, from_z,
    x_ch, h1_ch, r_own, dg, dg_core, dg_x, dg_y, dg_z, ssem, rsem, lsem, credit,
):
    td, d = x_in.shape
    rb = wg_in.shape[1]
    fb = wg_in.shape[2] // 4
    hh = 2 * fb
    t2, ch, half = 2 * td, td // 4, td // 2
    hc = ch // 2
    tile = min(512, fb)
    z = lax.axis_index("tensor")
    y = lax.axis_index("replica")
    f = lax.axis_index("fsdp")
    x, c = f // 2, f % 2
    xo, yo, co = 1 - x, 1 - y, 1 - c
    q, qx, qy, qd = 2 * y + x, 2 * y + xo, 2 * yo + x, 2 * yo + xo
    cs = (c + y) % 2
    cso = 1 - cs
    to_c, to_x, to_xs, to_y = {"fsdp": 2 * x + co}, {"fsdp": 2 * xo + c}, {"fsdp": 2 * xo + cs}, {"replica": yo}
    inner = ((z + 1) // 2) % 2
    outer = 1 - inner
    up = z // 2
    pair = z + 1 - 2 * (z % 2)
    far_outer, far_inner = 3 - 3 * up, 2 - up
    order = (outer * far_outer + inner * pair, outer * far_inner + inner * far_outer, outer * pair + inner * far_inner, z)

    n_own, o_own = nb.at[1], ob.at[1]

    def at_z(i):
        return {"tensor": i}

    def z_other(k):
        return (z + 4 + k * (1 - 2 * up)) % 4

    others = tuple(z_other(k) for k in (1, 2, 3))
    toward = outer * pair + inner * far_inner

    def rows(start, size):
        return pl.ds(start if isinstance(start, int) else pl.multiple_of(start, size if size % 16 == 0 else 8), size)

    def cols(start, size):
        return pl.ds(start if isinstance(start, int) else pl.multiple_of(start, 128), size)

    ids, sids, lids, sent, passed, groups = {}, {}, {}, {}, {}, {}

    def numbered(table, key, limit):
        i = table.setdefault(key, len(table))
        assert i < limit, i
        return i

    def sid(key):
        return numbered(ids, key, NRECV)

    def name_of(key):
        return key if isinstance(key, str) else "_".join(map(str, key))

    def copy_of(skey, rkey, src, dst, dev):
        send = 0 if skey is None else numbered(sids, skey, NSEND)
        recv = sid(rkey) if isinstance(rkey, (str, tuple)) else rkey
        return pltpu.make_async_remote_copy(src_ref=src, dst_ref=dst, send_sem=ssem.at[send], recv_sem=rsem.at[recv], device_id=dev, device_id_type=MESH)

    def push(key, make, rkey=None, group=None):
        src, dst, dev = make()
        copy_of(group or key, key if rkey is None else rkey, src, dst, dev).start()
        if group is None:
            sent[key] = make
        else:
            groups.setdefault(group, {})[key] = int(np.prod(src.shape))

    def group_done(group):
        n = sum(groups.pop(group).values()) // d
        assert n % 2 == 0 and n <= 2 * hh, n
        view = wd.at[:, pl.ds(0, n // 2)]
        copy_of(group, 0, view, view, to_c).wait_send()

    def got(key, dst):
        with jax.named_scope("got_" + (name_of(key) if isinstance(key, (str, tuple)) else "dyn")):
            copy_of(None, key, dst, dst, to_c).wait_recv()

    def send_done(key):
        copy_of(key, 0, *sent.pop(key)()).wait_send()

    def flush(keys):
        for key in keys:
            send_done(key)

    def local(key, src, dst):
        i = numbered(lids, key, NLOC)
        return pltpu.make_async_copy(src, dst, lsem.at[i])

    def scoped(fn):
        def run(*args):
            with jax.named_scope(fn.__name__):
                return fn(*args)

        return run

    gu = ((wg_in, wg), (wu_in, wu))
    pieces = (2, 2)

    def wview(m, l, row, xb, k=0, n=1):
        return gu[m][1].at[l, rows(row * rb + k * (rb // n), rb // n), cols(xb * fb, fb)]

    def wsrc(m, l, xb, core, k=0, n=1):
        return gu[m][0].at[l, pl.ds(k * (rb // n), rb // n), cols((2 * xb + core) * fb, fb)]

    def push_w(l, m):
        n = pieces[l]
        for xb in range(2):
            for k in range(n):
                push(("wx", l, m, xb, k), lambda xb=xb, k=k: (wsrc(m, l, xb, cs, k, n), wview(m, l, f, xb, k, n), to_xs), group=("W", l))
        for k in range(4 * m):
            r0 = y * (fb // 2) + k * (fb // 8)
            push(("wdx", l, k), lambda r0=r0: (wd_in.at[l, rows(r0, fb // 8)], wd.at[l, rows(x * fb + r0, fb // 8)], to_x), group=("W", l))
        if (l, m) == (1, 1):
            r1 = yo * (fb // 2) + 3 * (fb // 8)
            push("wdx_last", lambda: (wd_in.at[l, rows(r1, fb // 8)], wd.at[l, rows(x * fb + r1, fb // 8)], to_x), group=("W", l))

    def push_wc(l):
        for m in range(2):
            for xb in range(2):
                push(("wc", l, m, xb), lambda m=m, xb=xb: (wsrc(m, l, xb, co), wview(m, l, f, xb), to_c), ("wc", l, xb * (1 - l)), group=("W", l))
                local(("w", l, m, xb), wsrc(m, l, xb, c), wview(m, l, f, xb)).start()
        local(("wd", l), wd_in.at[l], wd.at[l, rows(x * fb, fb)]).start()

    def relay_gu(l, m, xb):
        n = pieces[l]
        for k in range(n):
            ref = lambda k=k: wview(m, l, 2 * xo + cs, xb, k, n)
            got(("wx", l, m, xb, k), ref())
            push(("wy", l, m, xb, k), lambda k=k: (ref(k), ref(k), to_y), ("wy", l, xb * (1 - l)), group=("W", l))

    def relay_d(l, k):
        ref = lambda: wd.at[l, rows(xo * fb + y * (fb // 2) + k * (fb // 8), fb // 8)]
        got(("wdx", l, k), ref())
        push(("wdy", l, k), lambda: (ref(), ref(), to_y), ("wdy", l), group=("W", l))

    def have_gu(l, xbs):
        for m in range(2):
            for xb in xbs:
                local(("w", l, m, xb), wsrc(m, l, xb, c), wview(m, l, f, xb)).wait()
        whole = wd.at[0, pl.ds(0, 2 * len(xbs) * rb // 4)]
        got(("wc", l, xbs[-1] * (1 - l)), whole)
        got(("wy", l, xbs[-1] * (1 - l)), whole)

    def have_d_own(l):
        local(("wd", l), wd_in.at[l], wd.at[l, rows(x * fb, fb)]).wait()

    def have_d(l):
        got(("wdy", l), wd.at[l, pl.ds(0, (4 - l) * (fb // 8))])
        if l == 1:
            got(("wdx", 1, 3), wd.at[1, rows(xo * fb + y * (fb // 2) + 3 * (fb // 8), fb // 8)])
            got("wdx_last", wd.at[1, rows(xo * fb + yo * (fb // 2) + 3 * (fb // 8), fb // 8)])

    def piece(buf, block, core, start, size):
        return buf.at[block, core, pl.ds(start, size)]

    def chunk(buf, block, core, zi):
        return buf.at[block, core, rows(zi * ch, ch)]

    def part_id(a, j):
        base = sid((a, "p", 0))
        for jj in range(3):
            assert sid((a, "p", jj)) == base + jj
        return base + j

    def share(a, j, tag, ref):
        push((a, "s", j, tag), lambda: (ref(), ref(), to_c), (a, "p", j), group=("S", a))

    def ag_x(a, buf, src, h):
        push((a, "x", h), lambda: (src().at[pl.ds(h * half, half)], piece(buf, q, c, h * half, half), to_x), group=("X", a))

    def ag_y(a, buf, src, h):
        push((a, "y", h), lambda: (src().at[pl.ds(h * half, half)], piece(buf, q, c, h * half, half), to_y), group=("X", a))

    def ag_quarter(a, buf, src, axis):
        push((a, axis + "c"), lambda: (src().at[rows(z * ch, ch)], chunk(buf, q, c, z), to_y if axis == "y" else to_x), group=("S", a))

    def ag_spread(a, buf, axis):
        block = qy if axis == "y" else qx
        got((a, axis + "c"), chunk(buf, block, c, z))
        for k in (1, 2, 3):
            push((a, axis, "zs", k), lambda k=k: (chunk(buf, block, c, z), chunk(buf, block, c, z), at_z(z_other(k))), (a, axis, "zb"), group=("S", a))

    def ag_spread_got(a, buf, axis):
        block = qy if axis == "y" else qx
        got((a, axis, "zb"), buf.at[block, c, pl.ds(0, 3 * ch)])
        share(a, 0 if axis == "y" else 1, 0, lambda: buf.at[block, c])

    def ag_dx(a, buf, cut):
        push((a, "dx"), lambda: (piece(buf, qy, c, 0, cut), piece(buf, qy, c, 0, cut), to_x), group=("S", a))

    def ag_got_y(a, buf, h):
        got((a, "y", h), piece(buf, qy, c, h * half, half))
        share(a, 0, h, lambda: piece(buf, qy, c, h * half, half))
        if h == 0:
            ag_dx(a, buf, half)

    def ag_dy(a, buf, cut):
        push((a, "dy", 0), lambda: (piece(buf, qx, c, cut, td - cut), piece(buf, qx, c, cut, td - cut), to_y), group=("S", a))

    def ag_got_dy_whole(a, buf, cut):
        got((a, "dy", 0), piece(buf, qd, c, cut, td - cut))
        share(a, 2, 0, lambda: piece(buf, qd, c, cut, td - cut))

    def diag_piece(h, cut):
        start = max(cut, h * half)
        return start, (h + 1) * half - start

    def ag_got_x(a, buf, h, cut):
        got((a, "x", h), piece(buf, qx, c, h * half, half))
        start, size = diag_piece(h, cut)
        if size:
            push((a, "dy", h), lambda: (piece(buf, qx, c, start, size), piece(buf, qx, c, start, size), to_y), group=("S", a))
        share(a, 1, h, lambda: piece(buf, qx, c, h * half, half))

    def ag_got_dx(a, buf, cut):
        got((a, "dx"), piece(buf, qd, c, 0, cut))
        share(a, 2, "x", lambda: piece(buf, qd, c, 0, cut))

    def ag_got_dy(a, buf, h, cut):
        start, size = diag_piece(h, cut)
        if size:
            got((a, "dy", h), piece(buf, qd, c, start, size))
            share(a, 2, h, lambda: piece(buf, qd, c, start, size))

    def block_of(j):
        return 2 * ((y + (j + 1) % 2) % 2) + (x + (j + 1) // 2) % 2

    def partner_has(a, buf, j):
        with jax.named_scope("got_p_" + a):
            got(part_id(a, j), buf.at[block_of(j), co])

    for a in ("n0", "o1", "n1", "o0"):
        for j in range(3):
            sid((a, "p", j))

    def fwd_tile(l, n_ref, g_ref, i, a_ref=None, b_ref=None):
        w = cols(i * tile, tile)
        a = mm(n_ref[...], wg[l, :, w], 1, 0).astype(BF16)
        b = mm(n_ref[...], wu[l, :, w], 1, 0).astype(BF16)
        (a_t if a_ref is None else a_ref)[:, w] = a
        (b_t if b_ref is None else b_ref)[:, w] = b
        if g_ref is not None:
            a_f = a.astype(F32)
            g_ref[:, w] = (a_f * jax.nn.sigmoid(a_f) * b.astype(F32)).astype(BF16)

    @scoped
    def fwd(l, n_ref, g_ref, a_ref=None, b_ref=None):
        def step(i, carry):
            fwd_tile(l, n_ref, g_ref, i, a_ref, b_ref)
            return carry

        lax.fori_loop(0, hh // tile, step, 0)

    @scoped
    def down_half(l, g_ref, kb, start, size, add):
        r, k = rows(start, size), pl.ds(pl.multiple_of(kb * fb, fb), fb)

        def step(i, carry):
            w = cols(i * tile, tile)
            new = mm(g_ref[r, k], wd[l, k, w], 1, 0)
            part[r, w] = part[r, w] + new if add else new
            return carry

        lax.fori_loop(0, d // tile, step, 0)

    @scoped
    def down_rows(l, g_ref, core):
        r = rows(core * td, td)

        def step(i, carry):
            w = cols(i * tile, tile)
            part[r, w] = mm(g_ref[r, :], wd[l, :, w], 1, 0)
            return carry

        lax.fori_loop(0, d // tile, step, 0)

    @scoped
    def m_half(l, kb, start, size, add):
        r, k = rows(start, size), pl.ds(pl.multiple_of(kb * fb, fb), fb)

        def step(i, carry):
            w = rows(i * tile, tile)
            new = mm(a_t[r, k], wg[l, w, k], 1, 1) + mm(b_t[r, k], wu[l, w, k], 1, 1)
            o = cols(i * tile, tile)
            part[r, o] = part[r, o] + new if add else new
            return carry

        lax.fori_loop(0, d // tile, step, 0)

    def bwd_tile(l, o_ref, i, a_ref, b_ref):
        w = cols(i * tile, tile)
        q_f = mm(o_ref[...], wd[l, rows(i * tile, tile)], 1, 1).astype(BF16).astype(F32)
        a_f, b_f = a_ref[:, w].astype(F32), b_ref[:, w].astype(F32)
        s = jax.nn.sigmoid(a_f)
        g_t[:, w] = (a_f * s * b_f).astype(BF16)
        a_t[:, w] = (q_f * b_f * s * (1.0 + a_f * (1.0 - s))).astype(BF16)
        b_t[:, w] = (q_f * a_f * s).astype(BF16)

    @scoped
    def bwd_hidden(l, o_ref, a_ref, b_ref):
        for i in range(hh // tile):
            bwd_tile(l, o_ref, i, a_ref, b_ref)

    @scoped
    def weight_grads(n_ref, col, o_ref, between):
        t = min(256, fb)

        def half_rows(core):
            for i in range(rb // t):
                n_rows = n_ref[:, cols(col + core * rb + i * t, t)]
                w = rows(core * rb + i * t, t)
                acc_g[w, :] += mm(n_rows, a_t[...], 0, 0)
                acc_u[w, :] += mm(n_rows, b_t[...], 0, 0)

        half_rows(co)
        if between is not None:
            between()
        half_rows(c)
        for i in range(fb // t):
            acc_d[pl.ds(i * t, t), :] += mm(g_t[:, cols(x * fb + i * t, t)], o_ref[...], 0, 0)

    @scoped
    def zero_acc():
        for ref in (acc_g, acc_u, acc_d):
            def step(i, carry, ref=ref):
                ref[rows(i * 16, 16), :] = jnp.zeros((16, ref.shape[1]), F32)
                return carry

            lax.fori_loop(0, ref.shape[0] // 16, step, 0)

    def rinv(h_f):
        return lax.rsqrt(jnp.mean(h_f * h_f, axis=-1, keepdims=True) + 1e-6)

    def core_land(key):
        return core_hbm if key == "d2" else acc_d

    def core_push(key):
        for k in range(4):
            push((key, "c", k), lambda k=k: (part.at[rows(co * td + order[k] * ch, ch)], core_land(key).at[rows(order[k] * ch, ch)], to_c))

    def z_ids(key):
        base = sid((key, "A", 0))
        for h in range(2):
            for i, s in enumerate("ABCD"):
                assert sid((key, s, h)) == base + 4 * h + i
        return base

    for sum_key in ("d0", "d1", "d2"):
        z_ids(sum_key)

    def mine(zi, h):
        return part.at[rows(c * td + zi * ch + h * hc, hc)]

    def slot(key, i, h):
        return from_z.at[i, pl.ds(h * hc, hc)]

    def core_back(k):
        return local(("cl", k), core_hbm.at[rows(order[k] * ch, ch)], part.at[rows(co * td + order[k] * ch, ch)])

    def core_back_start(key):
        for k in range(4):
            got((key, "c", k), core_land(key).at[rows(order[k] * ch, ch)])
            send_done((key, "c", k))
            core_back(k).start()

    @scoped
    def core_sum_send(key):
        z_ids(key)
        for k in range(4):
            if key == "d2":
                core_back(k).wait()
            else:
                got((key, "c", k), core_land(key).at[rows(order[k] * ch, ch)])

            def step(i, carry):
                r = order[k] * ch + i * 16
                mine_r = rows(c * td + r, 16)
                part[mine_r, :] = part[mine_r, :] + (part[rows(co * td + r, 16), :] if key == "d2" else acc_d[rows(r, 16), :])
                return carry

            lax.fori_loop(0, ch // 16, step, 0)
            if k == 0:
                for h in range(2):
                    push((key, "A", h), lambda h=h: (mine(order[0], h), slot(key, 0, h), at_z(pair)))
            elif k < 3:
                @pl.when(outer == 1)
                def _():
                    for h in range(2):
                        copy_of((key, "BC"[k - 1], h), (key, "BC"[k - 1], h), mine(order[k], h), slot(key, k, h), at_z(pair)).start()


    def z_relay(key, n, h):
        @pl.when(inner == 1)
        def _():
            got((key, "AB"[n], h), slot(key, n, h))
            zi = (far_outer, far_inner)[n]
            work = slot(key, n, h)

            def step(i, carry):
                r = rows(i * 8, 8)
                work[r, :] = work[r, :] + part[rows(c * td + zi * ch + h * hc + i * 8, 8), :]
                return carry

            lax.fori_loop(0, hc // 8, step, 0)
            if n == 0:
                copy_of((key, "B", h), (key, "B", h), work, slot(key, 1, h), at_z(far_outer)).start()
            else:
                copy_of((key, "C", h), (key, "D", h), work, slot(key, 3, h), at_z(far_inner)).start()

    def z_got(key):
        base = z_ids(key)
        for h in range(2):
            for i in range(2):
                with jax.named_scope("got_" + key):
                    got(base + 4 * h + 2 * inner + i, slot(key, 2 * inner + i, h))

    def z_sum(key, i):
        r = rows(i * 16, 16)
        return part[rows(c * td + z * ch + i * 16, 16), :] + from_z[2 * inner, r, :] + from_z[2 * inner + 1, r, :]

    def relay_sends_done(key):
        @pl.when(inner == 1)
        def _():
            for s in "BC":
                for h in range(2):
                    copy_of((key, s, h), 0, mine(0, h), slot(key, 0, h), at_z(pair)).wait_send()

    def sum_sends_done(key):
        for part_key in [(key, "c", k) for k in range(4)] + [(key, "A", h) for h in range(2)]:
            send_done(part_key)

        @pl.when(outer == 1)
        def _():
            for s in "BC":
                for h in range(2):
                    copy_of((key, s, h), 0, mine(0, h), slot(key, 0, h), at_z(pair)).wait_send()

    def quarter(ref, core, zi):
        return ref.at[rows(core * td + zi * ch, ch)]

    def zg_id(key, zi):
        base = sid((key, "z", 0))
        for i in range(4):
            assert sid((key, "z", i)) == base + i
        return base + zi

    relayed = ("n1z",)

    def takes(key):
        return (pair, far_inner, far_outer) if key in relayed else others

    def z_push(key, make, zi):
        for k, dev in enumerate((toward,) if key in relayed else others):
            push((key, "zs", k), lambda dev=dev: (*make(zi), at_z(dev)), zg_id(key, zi), group=("X", key[:2]))
        if key in relayed:
            z_forward(key, 3, make(zi)[1], zg_id(key, zi), pair)
            passed[(key, "fw", 3)] = lambda: make(z)[1]

    def z_forward(key, i, ref, rkey, dev):
        @pl.when(inner == 1)
        def _():
            copy_of((key, "fw", i), rkey, ref, ref, at_z(dev)).start()

    def z_pass(key, make, i):
        zi = takes(key)[i]
        with jax.named_scope("got_%s_%d" % (key, i)):
            got(zg_id(key, zi), make(zi)[1])
        if key in relayed:
            z_forward(key, i, make(zi)[1], zg_id(key, zi), (far_inner, pair, pair)[i])
            passed[(key, "fw", i)] = lambda: make(zi)[1]

    def passed_done(which):
        @pl.when(inner == 1)
        def _():
            for key in [k1 for k1 in passed if k1[0] == which]:
                ref = passed.pop(key)
                copy_of(key, 0, ref(), ref(), to_c).wait_send()

    def z_gather(key, ref):
        z_push(key, lambda zi: (quarter(ref, c, zi), quarter(ref, c, zi)), z)
        push((key, "s", 0), lambda: (quarter(ref, c, z), quarter(ref, c, z), to_c), (key, "s"), group=("X", key[:2]))

    def z_take(key, ref, i):
        z_pass(key, lambda zi: (quarter(ref, c, zi), quarter(ref, c, zi)), i)
        push((key, "s", 1 + i), lambda: (quarter(ref, c, takes(key)[i]), quarter(ref, c, takes(key)[i]), to_c), (key, "s"), group=("X", key[:2]))

    def z_gathered_partner(key, ref):
        got((key, "s"), ref.at[rows(co * td, td)])

    def stage(buf, block, slot_ref, key):
        for core in range(2):
            local((key, core), buf.at[block, core], slot_ref.at[pl.ds(core * td, td)]).start()

    def staged(buf, block, slot_ref, key):
        for core in range(2):
            local((key, core), buf.at[block, core], slot_ref.at[pl.ds(core * td, td)]).wait()

    def save_ab(block):
        return (local("sa", a_t, a_save.at[block]), local("sb", b_t, b_save.at[block]))

    @scoped
    def f0_other(j, slot):
        fwd(0, nb.at[slot], None)
        for s in save_ab(block_of(j)):
            s.start()

    def saves_done(block):
        for s in save_ab(block):
            s.wait()

    def a_kept(k):
        return wg.at[1, rows(k * t2, t2)]

    def b_kept(k):
        return wd.at[1, rows((k // 2) * t2, t2), cols((k % 2) * hh, hh)]

    def load_ab(block, k):
        return (local(("la", k), a_save.at[block], a_kept(k)), local(("lb", k), b_save.at[block], b_kept(k)))

    def grad_piece(i, xb, core):
        return (acc_g, acc_u)[i].at[rows(core * rb, rb), cols(xb * fb, fb)]

    def grad_land(l, i, xb, core):
        if l == 1:
            return (dwg1, dwu1)[i].at[:, cols((2 * xb + core) * fb, fb)]
        return part.at[:, cols(i * hh + xb * fb, fb)]

    def grads_push(l):
        for i in range(2):
            for xb in range(2):
                push(("q", l, i, xb), lambda i=i, xb=xb: (grad_piece(i, xb, co), grad_land(l, i, xb, c), to_c), ("q", l))

    def grads_out():
        for i in range(2):
            for xb in range(2):
                local(("qo", i, xb), grad_piece(i, xb, c), grad_land(1, i, xb, c)).start()
        local("qd", acc_d, dwd1).start()

    @scoped
    def grads_out_done(l):
        for i in range(2):
            for xb in range(2):
                if l == 1:
                    local(("qo", i, xb), grad_piece(i, xb, c), grad_land(1, i, xb, c)).wait()
                send_done(("q", l, i, xb))
        got(("q", l), acc_d)
        if l == 1:
            local("qd", acc_d, dwd1).wait()

    barrier = pltpu.get_barrier_semaphore()
    for dev in (to_c, to_x, {"fsdp": 2 * xo + co}, to_y, at_z((z + 1) % 4), at_z((z + 2) % 4), at_z((z + 3) % 4)):
        pl.semaphore_signal(barrier, inc=1, device_id=dev, device_id_type=MESH)
    x_load = local("x", x_in, nb.at[1, pl.ds(0, td)])
    x_load.start()
    with jax.named_scope("barrier"):
        pl.semaphore_wait(barrier, 7)

    dy_src = lambda: dy_in
    n0_src = lambda: n0_buf.at[q, c]
    n1_src = lambda: n_own.at[rows(c * td, td)]
    o0_src = lambda: o_own.at[rows(c * td, td)]
    cut_n, cut_o = ch, half

    push_w(0, 0)
    push_wc(0)
    x_load.wait()

    def n0_step(i, carry):
        h_f = n_own[rows(i * 16, 16), :].astype(F32)
        r_inv = rinv(h_f)
        nb[0, rows(c * td + i * 16, 16), :] = (h_f * r_inv * gain[0:1, :]).astype(BF16)
        r_own[rows(c * td + i * 16, 16), :] = jnp.broadcast_to(r_inv, (16, 128))
        return carry

    lax.fori_loop(0, td // 16, n0_step, 0)
    n0_mine = lambda: nb.at[0, rows(c * td, td)]
    push("n0p", lambda: (n0_mine(), n0_mine(), to_c))
    r_mine = lambda: r_own.at[rows(c * td, td)]
    push("rp", lambda: (r_mine(), r_mine(), to_c))
    keep = local("n0k", n0_mine(), n0_buf.at[q, c])
    keep.start()
    keep.wait()
    ag_quarter("n0", n0_buf, n0_src, "y")
    ag_quarter("n0", n0_buf, n0_src, "x")
    ag_quarter("o1", o1_buf, dy_src, "y")
    push_w(0, 1)
    push_w(1, 0)
    push_w(1, 1)
    ag_x("o1", o1_buf, dy_src, 0)
    push("xp", lambda: (x_in, x_part, to_c))
    push("dyp", lambda: (dy_in, o1_buf.at[q, c], to_c))
    push_wc(1)
    local("xc", x_in.at[rows(z * ch, ch)], x_ch).start()
    local("dy_own", dy_in, ob.at[0, rows(c * td, td)]).start()

    @scoped
    def h1_calc():
        def h1_step(i, carry):
            r = rows(i * 16, 16)
            h1 = (x_ch[r, :].astype(F32) + z_sum("d0", i)).astype(BF16)
            h1_ch[r, :] = h1
            h_f = h1.astype(F32)
            n_own[rows(c * td + z * ch + i * 16, 16), :] = (h_f * rinv(h_f) * gain[1:2, :]).astype(BF16)
            return carry

        lax.fori_loop(0, ch // 16, h1_step, 0)

    def h1_done():
        z_got("d0")
        relay_sends_done("d0")
        h1_calc()
        z_gather("n1z", n_own)

    relay_gu(0, 0, 0)
    ag_spread("n0", n0_buf, "y")
    ag_spread("o1", o1_buf, "y")
    relay_gu(0, 0, 1)
    ag_spread("n0", n0_buf, "x")
    relay_gu(0, 1, 0)
    relay_gu(0, 1, 1)
    got("n0p", nb.at[0, rows(co * td, td)])
    got("rp", r_own.at[rows(co * td, td)])
    keep2 = local("n0k2", nb.at[0, rows(co * td, td)], n0_buf.at[q, co])
    keep2.start()
    have_gu(0, (0,))
    with jax.named_scope("fwd_tile0"):
        fwd_tile(0, nb.at[0], g_t, 0)
    relay_d(0, 0)
    relay_d(0, 1)
    have_gu(0, (1,))
    with jax.named_scope("fwd_tile1"):
        for i in range(1, hh // tile):
            fwd_tile(0, nb.at[0], g_t, i)
    for s in save_ab(q):
        s.start()
    have_d_own(0)
    relay_d(0, 2)
    down_half(0, g_t, x, 0, t2, False)
    relay_d(0, 3)
    ag_spread_got("n0", n0_buf, "y")
    have_d(0)
    down_half(0, g_t, xo, co * td, td, True)
    core_push("d0")
    down_half(0, g_t, xo, c * td, td, True)
    core_sum_send("d0")
    keep2.wait()
    send_done("n0p")
    saves_done(q)
    partner_has("n0", n0_buf, 0)
    stage(n0_buf, block_of(0), nb.at[0], "sn")
    relay_gu(1, 0, 0)
    staged(n0_buf, block_of(0), nb.at[0], "sn")
    f0_other(0, 0)
    z_relay("d0", 0, 0)
    relay_gu(1, 0, 1)
    z_relay("d0", 0, 1)
    ag_spread_got("n0", n0_buf, "x")
    ag_spread_got("o1", o1_buf, "y")
    partner_has("n0", n0_buf, 1)
    stage(n0_buf, block_of(1), nb.at[0], "sn")
    z_relay("d0", 1, 0)
    relay_gu(1, 1, 0)
    z_relay("d0", 1, 1)
    local("xc", x_in.at[rows(z * ch, ch)], x_ch).wait()

    @pl.when(outer == 1)
    def _():
        h1_done()

    relay_gu(1, 1, 1)

    @pl.when(inner == 1)
    def _():
        h1_done()

    local("dyc", dy_in.at[rows(z * ch, ch)], x_ch).start()
    group_done(("W", 0))
    flush(("xp", "dyp", "rp"))
    relay_d(1, 0)
    z_take("n1z", n_own, 0)
    z_take("n1z", n_own, 1)
    relay_d(1, 1)
    z_take("n1z", n_own, 2)
    relay_d(1, 2)
    saves_done(block_of(0))
    for h in range(2):
        ag_x("n1", n1_buf, n1_src, h)
    ag_x("o1", o1_buf, dy_src, 1)
    for h in range(2):
        ag_y("n1", n1_buf, n1_src, h)
    got("dyp", o1_buf.at[q, co])
    dy_other = local("dy_other", o1_buf.at[q, co], ob.at[0, rows(co * td, td)])
    dy_other.start()
    z_gathered_partner("n1z", n_own)

    have_gu(1, (0, 1))
    fwd(1, n_own, g_t)
    local("dy_own", dy_in, ob.at[0, rows(c * td, td)]).wait()
    dy_other.wait()
    have_d_own(1)
    bwd_tile(1, ob.at[0], x, a_t, b_t)
    sum_sends_done("d0")
    m_half(1, x, 0, t2, False)
    have_d(1)
    bwd_tile(1, ob.at[0], xo, a_t, b_t)
    g_keep = local("gk", g_t, g_save)
    g_keep.start()
    m_half(1, xo, co * td, td, True)
    core_push("d1")
    m_half(1, xo, c * td, td, True)
    core_sum_send("d1")
    zero_acc()
    g_keep.wait()
    local("dyc", dy_in.at[rows(z * ch, ch)], x_ch).wait()

    @scoped
    def e_calc():
        def e_step(i, dg1):
            r = rows(i * 16, 16)
            m = z_sum("d1", i)
            h_f = h1_ch[r, :].astype(F32)
            r_inv = rinv(h_f)
            xh = h_f * r_inv
            v = m * gain[1:2, :]
            e = x_ch[r, :].astype(F32) + r_inv * (v - xh * jnp.mean(v * xh, axis=-1, keepdims=True))
            o_own[rows(c * td + z * ch + i * 16, 16), :] = e.astype(BF16)
            return dg1 + jnp.sum(m * xh, axis=0, keepdims=True)

        dg[1:2, :] = lax.fori_loop(0, ch // 16, e_step, jnp.zeros((1, d), F32))

    def at_step(k, n):
        return pl.when(k == n)

    def stage_n(buf, block, slot):
        stage(buf, block, nb.at[slot], ("n", slot))

    def staged_n(buf, block, slot):
        staged(buf, block, nb.at[slot], ("n", slot))

    def stage_o(buf, block, slot):
        stage(buf, block, ob.at[slot], ("o", slot))

    def staged_o(buf, block, slot):
        staged(buf, block, ob.at[slot], ("o", slot))

    xl = lambda: [local("xl0", x_in, nb.at[0, rows(c * td, td)]), local("xl1", x_part, nb.at[0, rows(co * td, td)])]

    def n_half(slot):
        return wu.at[1, rows(slot * t2, t2)]

    def n_half_copies(block, slot):
        return [local(("nh", slot, core), n0_buf.at[block, core, :, cols(2 * x * rb, 2 * rb)], wu.at[1, rows(slot * t2 + core * td, td)]) for core in range(2)]

    def load_n_half(block, slot):
        for s in n_half_copies(block, slot):
            s.start()

    own_g = nb.at[1, :, pl.ds(0, hh)]

    def e_done():
        z_got("d1")
        relay_sends_done("d1")
        e_calc()
        z_gather("o0z", o_own)
        for dev in others:
            pl.semaphore_signal(credit, inc=1, device_id=at_z(dev), device_id_type=MESH)

    def l1_step(k, carry):
        slot = 1 - (k + 3) // 4

        @pl.when(k > 0)
        def _():
            @at_step(k, 1)
            def _():
                partner_has("o1", o1_buf, 0)
                stage_o(o1_buf, block_of(0), 0)

            staged_n(n1_buf, block_of(k - 1), 0)
            with jax.named_scope("fwd_a"):
                fwd_tile(1, nb.at[0], None, 0)

            @at_step(k, 2)
            def _():
                ag_got_x("o1", o1_buf, 1, cut_o)

            @at_step(k, 3)
            def _():
                ag_got_dx("o1", o1_buf, cut_o)
                for h in range(2):
                    ag_got_dy("o1", o1_buf, h, cut_o)

            with jax.named_scope("fwd_b"):
                for i in range(1, hh // tile):
                    fwd_tile(1, nb.at[0], None, i)

            @pl.when(k * inner == 2)
            def _():
                e_done()

            @pl.when(k > 1)
            def _():
                partner_has("o1", o1_buf, k - 1)
                stage_o(o1_buf, block_of(k - 1), 0)

            @at_step(k, 3)
            def _():
                for i in range(3):
                    z_take("o0z", o_own, i)
                for h in range(2):
                    ag_x("o0", o0_buf, o0_src, h)
                    ag_y("o0", o0_buf, o0_src, h)

            @at_step(k, 1)
            def _():
                z_relay("d1", 1, 0)
                ag_got_x("n1", n1_buf, 1, half)

            staged_o(o1_buf, block_of(k - 1), 0)
            bwd_hidden(1, ob.at[0], a_t, b_t)

            @at_step(k, 1)
            def _():
                z_relay("d1", 1, 1)

                @pl.when(outer == 1)
                def _():
                    e_done()

                partner_has("n1", n1_buf, 1)

            @at_step(k, 2)
            def _():
                local("gl", g_save, own_g).wait()
                sum_sends_done("d1")
                down_rows(1, own_g, co)
                core_push("d2")
                ag_got_dx("n1", n1_buf, half)
                ag_got_dy("n1", n1_buf, 1, half)
                down_rows(1, own_g, c)
                core_back_start("d2")

            @at_step(k, 1)
            def _():
                group_done(("X", "n1"))
                passed_done("n1z")
                local("gl", g_save, own_g).start()

            @at_step(k, 3)
            def _():
                z_relay("d2", 0, 0)
                group_done(("W", 1))
                for i in range(3):
                    for s in load_ab(block_of(i - 1) if i else q, i):
                        s.start()
                    load_n_half(block_of(i - 1) if i else q, i)

        weight_grads(nb.at[slot], 2 * x * rb, ob.at[0], None)

        @at_step(k, 1)
        def _():
            stage_n(n1_buf, block_of(1), 0)

        @at_step(k, 2)
        def _():
            partner_has("n1", n1_buf, 2)
            stage_n(n1_buf, block_of(2), 0)
            pl.semaphore_wait(credit, 3)
            core_sum_send("d2")

        @at_step(k, 0)
        def _():
            staged(n0_buf, block_of(1), nb.at[0], "sn")
            f0_other(1, 0)
            ag_got_x("o1", o1_buf, 0, cut_o)
            ag_got_x("n1", n1_buf, 0, half)
            z_relay("d1", 0, 0)
            ag_got_y("n1", n1_buf, 0)
            ag_dx("o1", o1_buf, cut_o)
            ag_dx("n0", n0_buf, cut_n)
            ag_dy("n0", n0_buf, cut_n)
            z_relay("d1", 0, 1)
            ag_got_y("n1", n1_buf, 1)
            partner_has("n1", n1_buf, 0)
            stage_n(n1_buf, block_of(0), 0)
            saves_done(block_of(1))

        return carry

    lax.fori_loop(0, 4, l1_step, 0)
    got("xp", x_part)
    for s in xl():
        s.start()
    for s in load_ab(q, 0):
        s.wait()
    z_gathered_partner("o0z", o_own)
    z_relay("d2", 0, 1)
    grads_push(1)
    grads_out()

    def y_rows(zi):
        return y_out.at[rows(zi * ch, ch)]

    zg_id("y", 0)

    @scoped
    def dgain0():
        def dg_step(i, carry):
            w = cols(i * tile, tile)
            m = mm(a_t[...], wg[0, rows(i * tile, tile)], 1, 1) + mm(b_t[...], wu[0, rows(i * tile, tile)], 1, 1)
            xh = nb[0, :, w].astype(F32) * r_own[:, 0:1]
            dg[0:1, w] = jnp.sum(m * xh, axis=0, keepdims=True)
            return carry

        lax.fori_loop(0, d // tile, dg_step, 0)

    def y_done():
        z_got("d2")

        def y_step(i, carry):
            r = rows(i * 16, 16)
            x_ch[r, :] = (h1_ch[r, :].astype(F32) + z_sum("d2", i)).astype(BF16)
            return carry

        lax.fori_loop(0, ch // 16, y_step, 0)
        local("yk", x_ch, y_rows(z)).start()
        z_push("y", lambda zi: (x_ch, y_rows(zi)), z)

    def l0_step(k, carry):
        oslot = (k + 1) % 2

        @at_step(k, 2)
        def _():
            ag_got_dx("o0", o0_buf, half)
            ag_got_dy("o0", o0_buf, 1, half)

        @pl.when(k > 0)
        def _():
            staged_o_any(k)

        bwd_hidden(0, ob.at[oslot], a_kept(k), b_kept(k))

        @at_step(k, 0)
        def _():
            for s in xl():
                s.wait()
            ag_got_dx("n0", n0_buf, cut_n)
            ag_got_dy_whole("n0", n0_buf, cut_n)
            z_relay("d2", 1, 0)
            dgain0()
            dg_z[z] = dg[...]
            for i in range(3):
                push(("gs", i), lambda i=i: (dg_z.at[z], dg_z.at[z], at_z(others[i])), "gz")
            z_relay("d2", 1, 1)
            partner_has("n0", n0_buf, 2)
            stage_n(n0_buf, block_of(2), 0)
            load_n_half(block_of(2), 3)
            ag_got_y("o0", o0_buf, 0)
            grads_out_done(1)
            zero_acc()
            for i in range(4):
                for s in n_half_copies(block_of(i - 1) if i else q, i):
                    s.wait()
            for i in range(1, 3):
                for s in load_ab(block_of(i - 1), i):
                    s.wait()

        @at_step(k, 1)
        def _():
            @pl.when(inner == 1)
            def _():
                y_done()

            for h in range(2):
                send_done(("d2", "A", h))
                for s in "BC":
                    copy_of(("d2", s, h), 0, mine(0, h), slot("d2", 0, h), at_z(pair)).wait_send()
            partner_has("o0", o0_buf, 1)
            group_done(("X", "o0"))
            stage_o(o0_buf, block_of(1), 1)
            got("gz", dg_z.at[pl.ds(0, 3)])
            for i in range(3):
                send_done(("gs", i))
            dg[...] = dg_z[0] + dg_z[1] + dg_z[2] + dg_z[3]
            push("gc", lambda: (dg, dg_core, to_c))

        @at_step(k, 2)
        def _():
            got("gc", dg_core)
            copy_of("gc", 0, dg, dg_core, to_c).wait_send()
            dg[...] = dg[...] + dg_core[...]
            push("gx", lambda: (dg, dg_x, to_x))
            partner_has("o0", o0_buf, 2)
            stage_o(o0_buf, block_of(2), 0)

        @at_step(k, 3)
        def _():
            got("gx", dg_x)
            copy_of("gx", 0, dg, dg_x, to_x).wait_send()
            dg[...] = dg[...] + dg_x[...]
            push("gy", lambda: (dg, dg_y, to_y))

        def between():
            @at_step(k, 3)
            def _():
                grads_push(0)

        weight_grads(n_half(k), 0, ob.at[oslot], between)

        @at_step(k, 0)
        def _():
            staged_n(n0_buf, block_of(2), 0)
            with jax.named_scope("f0_a"):
                fwd_tile(0, nb.at[0], None, 0, a_kept(3), b_kept(3))
            ag_got_x("o0", o0_buf, 0, half)
            ag_got_y("o0", o0_buf, 1)
            ag_got_x("o0", o0_buf, 1, half)
            with jax.named_scope("f0_b"):
                for i in range(1, hh // tile):
                    fwd_tile(0, nb.at[0], None, i, a_kept(3), b_kept(3))

            @pl.when(outer == 1)
            def _():
                y_done()

            for a in ("n0", "o1", "n1"):
                group_done(("S", a))
            partner_has("o0", o0_buf, 0)
            stage_o(o0_buf, block_of(0), 0)

        return carry

    def staged_o_any(k):
        for n, slot in ((1, 0), (2, 1), (3, 0)):
            @at_step(k, n)
            def _(n=n, slot=slot):
                staged_o(o0_buf, block_of(n - 1), slot)

    lax.fori_loop(0, 4, l0_step, 0)
    for key in ("gc", "gx", "gy"):
        sent.pop(key)
    got("gy", dg_y)
    copy_of("gy", 0, dg, dg_y, to_y).wait_send()
    dgain_out[...] = dg[...] + dg_y[...]
    for i in range(3):
        with jax.named_scope("got_y"):
            z_pass("y", lambda zi: (x_ch, y_rows(zi)), i)
    local("yk", x_ch, y_rows(z)).wait()
    grads_out_done(0)
    for key in list(sent):
        send_done(key)
    for group in list(groups):
        group_done(group)
    assert not passed


def finish(acc_g, acc_u, acc_d, other, g1, u1, d1, y_in, g_out, u_out, d_out, y_out, buf, ybuf, sem_in, sem_out):
    rb, hh = other.shape[0], acc_g.shape[1]
    fb = hh // 2
    f = lax.axis_index("fsdp")
    c = f % 2
    ins = [pltpu.make_async_copy(src, buf.at[i], sem_in.at[i]) for i, src in enumerate((g1, u1, d1))]
    ins.append(pltpu.make_async_copy(y_in, ybuf, sem_in.at[3]))
    for copy in ins:
        copy.start()
    outs = []

    def out(src, dst):
        copy = pltpu.make_async_copy(src, dst, sem_out.at[len(outs)])
        copy.start()
        outs.append(copy)

    for i, (acc, dst) in enumerate(((acc_g, g_out), (acc_u, u_out))):
        for xb in range(2):
            own = pl.ds(pl.multiple_of((2 * xb + c) * fb, 128), fb)
            out(acc.at[pl.ds(pl.multiple_of(c * rb, rb), rb), pl.ds(xb * fb, fb)], dst.at[0, :, own])
            theirs = pl.ds(pl.multiple_of((2 * xb + 1 - c) * fb, 128), fb)
            out(other.at[:, pl.ds(i * hh + xb * fb, fb)], dst.at[0, :, theirs])
    out(acc_d, d_out.at[0])
    for i, dst in enumerate((g_out, u_out, d_out)):
        ins[i].wait()
        out(buf.at[i], dst.at[1])
    ins[3].wait()
    out(ybuf, y_out)
    for copy in outs:
        copy.wait()


def make_call(td, d, rb, hs):
    fb = hs // 4
    hh, t2, ch = 2 * fb, 2 * td, td // 4
    shape = jax.ShapeDtypeStruct
    hbm = pl.BlockSpec(memory_space=pl.ANY)
    vmem = pl.BlockSpec(memory_space=pltpu.VMEM)
    block = shape((4, 2, td, d), BF16)
    outs = [
        shape((td, d), BF16), shape((rb, hs), F32), shape((rb, hs), F32), shape((fb, d), F32), shape((2, d), F32),
        pltpu.VMEM((2 * rb, hh), F32), pltpu.VMEM((2 * rb, hh), F32), pltpu.VMEM((fb, d), F32), pltpu.VMEM((t2, d), F32),
        block, block, block, block, shape((4, t2, hh), BF16), shape((4, t2, hh), BF16), shape((td, d), BF16), shape((t2, hh), BF16), shape((td, d), F32),
    ]
    scratch = [
        pltpu.VMEM((2, d, hh), BF16), pltpu.VMEM((2, d, hh), BF16), pltpu.VMEM((2, hh, d), BF16),
        pltpu.VMEM((2, t2, d), BF16), pltpu.VMEM((2, t2, d), BF16),
        pltpu.VMEM((t2, hh), BF16), pltpu.VMEM((t2, hh), BF16), pltpu.VMEM((t2, hh), BF16),
        pltpu.VMEM((4, ch, d), F32),
        pltpu.VMEM((ch, d), BF16), pltpu.VMEM((ch, d), BF16),
        pltpu.VMEM((t2, 128), F32),
        pltpu.VMEM((2, d), F32), pltpu.VMEM((2, d), F32), pltpu.VMEM((2, d), F32), pltpu.VMEM((2, d), F32), pltpu.VMEM((4, 2, d), F32),
        pltpu.SemaphoreType.DMA((NSEND,)), pltpu.SemaphoreType.DMA((NRECV,)), pltpu.SemaphoreType.DMA((NLOC,)), pltpu.SemaphoreType.REGULAR,
    ]
    step = pl.pallas_call(
        kernel,
        out_shape=outs,
        in_specs=[hbm] * 5 + [vmem],
        out_specs=[hbm] * 4 + [vmem] * 5 + [hbm] * 9,
        scratch_shapes=scratch,
        compiler_params=pltpu.CompilerParams(collective_id=0, has_side_effects=True, vmem_limit_bytes=VLIM),
    )
    end = pl.pallas_call(
        finish,
        out_shape=[shape((2, rb, hs), F32), shape((2, rb, hs), F32), shape((2, fb, d), F32), shape((td, d), BF16)],
        in_specs=[vmem] * 4 + [hbm] * 4,
        out_specs=[hbm] * 4,
        scratch_shapes=[pltpu.VMEM((3, rb, hs), F32), pltpu.VMEM((td, d), BF16), pltpu.SemaphoreType.DMA((4,)), pltpu.SemaphoreType.DMA((13,))],
        compiler_params=pltpu.CompilerParams(vmem_limit_bytes=VLIM2),
    )

    def call(*args):
        y, g1, u1, d1, dgain, acc_g, acc_u, acc_d, other = step(*args)[:9]
        kept = [pltpu.with_memory_space_constraint(v, pltpu.VMEM) for v in (acc_g, acc_u, acc_d, other)]
        stored = [pltpu.with_memory_space_constraint(v, pltpu.HBM) for v in (g1, u1, d1, y)]
        g, u, dd, y = end(*kept, *stored)
        return y, g, u, dd, dgain

    return call


def solution(mesh):
    tok_spec = P(("replica", "fsdp"), None)
    wide_spec = P(None, "fsdp", "tensor")
    down_spec = P(None, ("tensor", "fsdp"), None)
    gain_spec = P(None, None)

    def device_fn(x_loc, dy_loc, w_gate, w_up, w_down, norm_gain):
        call = make_call(x_loc.shape[0], x_loc.shape[1], w_gate.shape[1], w_gate.shape[2])
        return call(x_loc, dy_loc, w_gate, w_up, w_down, norm_gain)

    return jax.shard_map(device_fn, mesh=mesh, in_specs=(tok_spec, tok_spec, wide_spec, wide_spec, down_spec, gain_spec), out_specs=(tok_spec, wide_spec, wide_spec, down_spec, gain_spec), check_vma=False)
```

```python
import jax
import jax.numpy as jnp
import numpy as np
from jax import lax
from jax.experimental import pallas as pl
from jax.experimental.pallas import tpu as pltpu
from jax.sharding import PartitionSpec as P

F32 = jnp.float32
BF16 = jnp.bfloat16
MESH = pl.DeviceIdType.MESH
NSEND = 65
NRECV = 130
NLOC = 55
VLIM = 67043328 - 16 * 2**20 - 2**17
VLIM2 = 14 * 2**20


def mm(lhs, rhs, ldim, rdim):
    return lax.dot_general(lhs, rhs, (((ldim,), (rdim,)), ((), ())), preferred_element_type=F32)


def kernel(
    x_in, dy_in, wg_in, wu_in, wd_in, gain,
    y_out, dwg1, dwu1, dwd1, dgain_out, acc_g, acc_u, acc_d, part, n0_buf, n1_buf, o1_buf, o0_buf, a_save, b_save, x_part, g_save, core_hbm,
    wg, wu, wd, nb, ob, a_t, b_t, g_t, from_z,
    x_ch, h1_ch, r_own, dg, dg_core, dg_x, dg_y, dg_z, ssem, rsem, lsem, credit,
):
    td, d = x_in.shape
    rb = wg_in.shape[1]
    fb = wg_in.shape[2] // 4
    hh = 2 * fb
    t2, ch, half = 2 * td, td // 4, td // 2
    hc = ch // 2
    tile = min(512, fb)
    z = lax.axis_index("tensor")
    y = lax.axis_index("replica")
    f = lax.axis_index("fsdp")
    x, c = f // 2, f % 2
    xo, yo, co = 1 - x, 1 - y, 1 - c
    q, qx, qy, qd = 2 * y + x, 2 * y + xo, 2 * yo + x, 2 * yo + xo
    cs = (c + y) % 2
    cso = 1 - cs
    to_c, to_x, to_xs, to_y = {"fsdp": 2 * x + co}, {"fsdp": 2 * xo + c}, {"fsdp": 2 * xo + cs}, {"replica": yo}
    inner = ((z + 1) // 2) % 2
    outer = 1 - inner
    up = z // 2
    pair = z + 1 - 2 * (z % 2)
    far_outer, far_inner = 3 - 3 * up, 2 - up
    order = (outer * far_outer + inner * pair, outer * far_inner + inner * far_outer, outer * pair + inner * far_inner, z)

    n_own, o_own = nb.at[1], ob.at[1]

    def at_z(i):
        return {"tensor": i}

    def z_other(k):
        return (z + 4 + k * (1 - 2 * up)) % 4

    others = tuple(z_other(k) for k in (1, 2, 3))
    toward = outer * pair + inner * far_inner

    def rows(start, size):
        return pl.ds(start if isinstance(start, int) else pl.multiple_of(start, size if size % 16 == 0 else 8), size)

    def cols(start, size):
        return pl.ds(start if isinstance(start, int) else pl.multiple_of(start, 128), size)

    ids, sids, lids, sent, passed, groups = {}, {}, {}, {}, {}, {}

    def numbered(table, key, limit):
        i = table.setdefault(key, len(table))
        assert i < limit, i
        return i

    def sid(key):
        return numbered(ids, key, NRECV)

    def name_of(key):
        return key if isinstance(key, str) else "_".join(map(str, key))

    def copy_of(skey, rkey, src, dst, dev):
        send = 0 if skey is None else numbered(sids, skey, NSEND)
        recv = sid(rkey) if isinstance(rkey, (str, tuple)) else rkey
        return pltpu.make_async_remote_copy(src_ref=src, dst_ref=dst, send_sem=ssem.at[send], recv_sem=rsem.at[recv], device_id=dev, device_id_type=MESH)

    def push(key, make, rkey=None, group=None):
        src, dst, dev = make()
        copy_of(group or key, key if rkey is None else rkey, src, dst, dev).start()
        if group is None:
            sent[key] = make
        else:
            groups.setdefault(group, {})[key] = int(np.prod(src.shape))

    def group_done(group):
        n = sum(groups.pop(group).values()) // d
        assert n % 2 == 0 and n <= 2 * hh, n
        view = wd.at[:, pl.ds(0, n // 2)]
        copy_of(group, 0, view, view, to_c).wait_send()

    def got(key, dst):
        with jax.named_scope("got_" + (name_of(key) if isinstance(key, (str, tuple)) else "dyn")):
            copy_of(None, key, dst, dst, to_c).wait_recv()

    def send_done(key):
        copy_of(key, 0, *sent.pop(key)()).wait_send()

    def flush(keys):
        for key in keys:
            send_done(key)

    def local(key, src, dst):
        i = numbered(lids, key, NLOC)
        return pltpu.make_async_copy(src, dst, lsem.at[i])

    def scoped(fn):
        def run(*args):
            with jax.named_scope(fn.__name__):
                return fn(*args)

        return run

    gu = ((wg_in, wg), (wu_in, wu))
    pieces = (2, 2)

    def wview(m, l, row, xb, k=0, n=1):
        return gu[m][1].at[l, rows(row * rb + k * (rb // n), rb // n), cols(xb * fb, fb)]

    def wsrc(m, l, xb, core, k=0, n=1):
        return gu[m][0].at[l, pl.ds(k * (rb // n), rb // n), cols((2 * xb + core) * fb, fb)]

    def push_w(l, m):
        n = pieces[l]
        for xb in range(2):
            for k in range(n):
                push(("wx", l, m, xb, k), lambda xb=xb, k=k: (wsrc(m, l, xb, cs, k, n), wview(m, l, f, xb, k, n), to_xs), group=("W", l))
        for k in range(4 * m):
            r0 = y * (fb // 2) + k * (fb // 8)
            push(("wdx", l, k), lambda r0=r0: (wd_in.at[l, rows(r0, fb // 8)], wd.at[l, rows(x * fb + r0, fb // 8)], to_x), group=("W", l))
        if (l, m) == (1, 1):
            r1 = yo * (fb // 2) + 3 * (fb // 8)
            push("wdx_last", lambda: (wd_in.at[l, rows(r1, fb // 8)], wd.at[l, rows(x * fb + r1, fb // 8)], to_x), group=("W", l))

    def push_wc(l):
        for m in range(2):
            for xb in range(2):
                push(("wc", l, m, xb), lambda m=m, xb=xb: (wsrc(m, l, xb, co), wview(m, l, f, xb), to_c), ("wc", l, xb * (1 - l)), group=("W", l))
                local(("w", l, m, xb), wsrc(m, l, xb, c), wview(m, l, f, xb)).start()
        local(("wd", l), wd_in.at[l], wd.at[l, rows(x * fb, fb)]).start()

    def relay_gu(l, m, xb):
        n = pieces[l]
        for k in range(n):
            ref = lambda k=k: wview(m, l, 2 * xo + cs, xb, k, n)
            got(("wx", l, m, xb, k), ref())
            push(("wy", l, m, xb, k), lambda k=k: (ref(k), ref(k), to_y), ("wy", l, xb * (1 - l)), group=("W", l))

    def relay_d(l, k):
        ref = lambda: wd.at[l, rows(xo * fb + y * (fb // 2) + k * (fb // 8), fb // 8)]
        got(("wdx", l, k), ref())
        push(("wdy", l, k), lambda: (ref(), ref(), to_y), ("wdy", l), group=("W", l))

    def have_gu(l, xbs):
        for m in range(2):
            for xb in xbs:
                local(("w", l, m, xb), wsrc(m, l, xb, c), wview(m, l, f, xb)).wait()
        whole = wd.at[0, pl.ds(0, 2 * len(xbs) * rb // 4)]
        got(("wc", l, xbs[-1] * (1 - l)), whole)
        got(("wy", l, xbs[-1] * (1 - l)), whole)

    def have_d_own(l):
        local(("wd", l), wd_in.at[l], wd.at[l, rows(x * fb, fb)]).wait()

    def have_d(l):
        got(("wdy", l), wd.at[l, pl.ds(0, (4 - l) * (fb // 8))])
        if l == 1:
            got(("wdx", 1, 3), wd.at[1, rows(xo * fb + y * (fb // 2) + 3 * (fb // 8), fb // 8)])
            got("wdx_last", wd.at[1, rows(xo * fb + yo * (fb // 2) + 3 * (fb // 8), fb // 8)])

    def piece(buf, block, core, start, size):
        return buf.at[block, core, pl.ds(start, size)]

    def chunk(buf, block, core, zi):
        return buf.at[block, core, rows(zi * ch, ch)]

    def part_id(a, j):
        base = sid((a, "p", 0))
        for jj in range(3):
            assert sid((a, "p", jj)) == base + jj
        return base + j

    def share(a, j, tag, ref):
        push((a, "s", j, tag), lambda: (ref(), ref(), to_c), (a, "p", j), group=("S", a))

    def ag_x(a, buf, src, h):
        push((a, "x", h), lambda: (src().at[pl.ds(h * half, half)], piece(buf, q, c, h * half, half), to_x), group=("X", a))

    def ag_y(a, buf, src, h):
        push((a, "y", h), lambda: (src().at[pl.ds(h * half, half)], piece(buf, q, c, h * half, half), to_y), group=("X", a))

    def ag_quarter(a, buf, src, axis):
        push((a, axis + "c"), lambda: (src().at[rows(z * ch, ch)], chunk(buf, q, c, z), to_y if axis == "y" else to_x), group=("S", a))

    def ag_spread(a, buf, axis):
        block = qy if axis == "y" else qx
        got((a, axis + "c"), chunk(buf, block, c, z))
        for k in (1, 2, 3):
            push((a, axis, "zs", k), lambda k=k: (chunk(buf, block, c, z), chunk(buf, block, c, z), at_z(z_other(k))), (a, axis, "zb"), group=("S", a))

    def ag_spread_got(a, buf, axis):
        block = qy if axis == "y" else qx
        got((a, axis, "zb"), buf.at[block, c, pl.ds(0, 3 * ch)])
        share(a, 0 if axis == "y" else 1, 0, lambda: buf.at[block, c])

    def ag_dx(a, buf, cut):
        push((a, "dx"), lambda: (piece(buf, qy, c, 0, cut), piece(buf, qy, c, 0, cut), to_x), group=("S", a))

    def ag_got_y(a, buf, h):
        got((a, "y", h), piece(buf, qy, c, h * half, half))
        share(a, 0, h, lambda: piece(buf, qy, c, h * half, half))
        if h == 0:
            ag_dx(a, buf, half)

    def ag_dy(a, buf, cut):
        push((a, "dy", 0), lambda: (piece(buf, qx, c, cut, td - cut), piece(buf, qx, c, cut, td - cut), to_y), group=("S", a))

    def ag_got_dy_whole(a, buf, cut):
        got((a, "dy", 0), piece(buf, qd, c, cut, td - cut))
        share(a, 2, 0, lambda: piece(buf, qd, c, cut, td - cut))

    def diag_piece(h, cut):
        start = max(cut, h * half)
        return start, (h + 1) * half - start

    def ag_got_x(a, buf, h, cut):
        got((a, "x", h), piece(buf, qx, c, h * half, half))
        start, size = diag_piece(h, cut)
        if size:
            push((a, "dy", h), lambda: (piece(buf, qx, c, start, size), piece(buf, qx, c, start, size), to_y), group=("S", a))
        share(a, 1, h, lambda: piece(buf, qx, c, h * half, half))

    def ag_got_dx(a, buf, cut):
        got((a, "dx"), piece(buf, qd, c, 0, cut))
        share(a, 2, "x", lambda: piece(buf, qd, c, 0, cut))

    def ag_got_dy(a, buf, h, cut):
        start, size = diag_piece(h, cut)
        if size:
            got((a, "dy", h), piece(buf, qd, c, start, size))
            share(a, 2, h, lambda: piece(buf, qd, c, start, size))

    def block_of(j):
        return 2 * ((y + (j + 1) % 2) % 2) + (x + (j + 1) // 2) % 2

    def partner_has(a, buf, j):
        with jax.named_scope("got_p_" + a):
            got(part_id(a, j), buf.at[block_of(j), co])

    for a in ("n0", "o1", "n1", "o0"):
        for j in range(3):
            sid((a, "p", j))

    def fwd_tile(l, n_ref, g_ref, i, a_ref=None, b_ref=None):
        w = cols(i * tile, tile)
        a = mm(n_ref[...], wg[l, :, w], 1, 0).astype(BF16)
        b = mm(n_ref[...], wu[l, :, w], 1, 0).astype(BF16)
        (a_t if a_ref is None else a_ref)[:, w] = a
        (b_t if b_ref is None else b_ref)[:, w] = b
        if g_ref is not None:
            a_f = a.astype(F32)
            g_ref[:, w] = (a_f * jax.nn.sigmoid(a_f) * b.astype(F32)).astype(BF16)

    @scoped
    def fwd(l, n_ref, g_ref, a_ref=None, b_ref=None):
        def step(i, carry):
            fwd_tile(l, n_ref, g_ref, i, a_ref, b_ref)
            return carry

        lax.fori_loop(0, hh // tile, step, 0)

    @scoped
    def down_half(l, g_ref, kb, start, size, add):
        r, k = rows(start, size), pl.ds(pl.multiple_of(kb * fb, fb), fb)

        def step(i, carry):
            w = cols(i * tile, tile)
            new = mm(g_ref[r, k], wd[l, k, w], 1, 0)
            part[r, w] = part[r, w] + new if add else new
            return carry

        lax.fori_loop(0, d // tile, step, 0)

    @scoped
    def down_rows(l, g_ref, core):
        r = rows(core * td, td)

        def step(i, carry):
            w = cols(i * tile, tile)
            part[r, w] = mm(g_ref[r, :], wd[l, :, w], 1, 0)
            return carry

        lax.fori_loop(0, d // tile, step, 0)

    @scoped
    def m_half(l, kb, start, size, add):
        r, k = rows(start, size), pl.ds(pl.multiple_of(kb * fb, fb), fb)

        def step(i, carry):
            w = rows(i * tile, tile)
            new = mm(a_t[r, k], wg[l, w, k], 1, 1) + mm(b_t[r, k], wu[l, w, k], 1, 1)
            o = cols(i * tile, tile)
            part[r, o] = part[r, o] + new if add else new
            return carry

        lax.fori_loop(0, d // tile, step, 0)

    def bwd_tile(l, o_ref, i, a_ref, b_ref):
        w = cols(i * tile, tile)
        q_f = mm(o_ref[...], wd[l, rows(i * tile, tile)], 1, 1).astype(BF16).astype(F32)
        a_f, b_f = a_ref[:, w].astype(F32), b_ref[:, w].astype(F32)
        s = jax.nn.sigmoid(a_f)
        g_t[:, w] = (a_f * s * b_f).astype(BF16)
        a_t[:, w] = (q_f * b_f * s * (1.0 + a_f * (1.0 - s))).astype(BF16)
        b_t[:, w] = (q_f * a_f * s).astype(BF16)

    @scoped
    def bwd_hidden(l, o_ref, a_ref, b_ref):
        for i in range(hh // tile):
            bwd_tile(l, o_ref, i, a_ref, b_ref)

    @scoped
    def weight_grads(n_ref, col, o_ref, theirs):
        t = min(256, fb)

        def half_rows(core):
            for i in range(rb // t):
                n_rows = n_ref[:, cols(col + core * rb + i * t, t)]
                w = rows(core * rb + i * t, t)
                acc_g[w, :] += mm(n_rows, a_t[...], 0, 0)
                acc_u[w, :] += mm(n_rows, b_t[...], 0, 0)

        if theirs is None:
            half_rows(co)
        else:
            @pl.when(theirs)
            def _():
                half_rows(co)

        half_rows(c)
        for i in range(fb // t):
            acc_d[pl.ds(i * t, t), :] += mm(g_t[:, cols(x * fb + i * t, t)], o_ref[...], 0, 0)

    @scoped
    def zero_acc():
        for ref in (acc_g, acc_u, acc_d):
            def step(i, carry, ref=ref):
                ref[rows(i * 16, 16), :] = jnp.zeros((16, ref.shape[1]), F32)
                return carry

            lax.fori_loop(0, ref.shape[0] // 16, step, 0)

    def rinv(h_f):
        return lax.rsqrt(jnp.mean(h_f * h_f, axis=-1, keepdims=True) + 1e-6)

    def core_land(key):
        return core_hbm if key == "d2" else acc_d

    def core_push(key):
        for k in range(4):
            push((key, "c", k), lambda k=k: (part.at[rows(co * td + order[k] * ch, ch)], core_land(key).at[rows(order[k] * ch, ch)], to_c))

    def z_ids(key):
        base = sid((key, "A", 0))
        for h in range(2):
            for i, s in enumerate("ABCD"):
                assert sid((key, s, h)) == base + 4 * h + i
        return base

    for sum_key in ("d0", "d1", "d2"):
        z_ids(sum_key)

    def mine(zi, h):
        return part.at[rows(c * td + zi * ch + h * hc, hc)]

    def slot(key, i, h):
        return from_z.at[i, pl.ds(h * hc, hc)]

    def core_back(k):
        return local(("cl", k), core_hbm.at[rows(order[k] * ch, ch)], part.at[rows(co * td + order[k] * ch, ch)])

    def core_back_start(key):
        for k in range(4):
            got((key, "c", k), core_land(key).at[rows(order[k] * ch, ch)])
            send_done((key, "c", k))
            core_back(k).start()

    @scoped
    def core_sum_send(key):
        z_ids(key)
        for k in range(4):
            if key == "d2":
                core_back(k).wait()
            else:
                got((key, "c", k), core_land(key).at[rows(order[k] * ch, ch)])

            def step(i, carry):
                r = order[k] * ch + i * 16
                mine_r = rows(c * td + r, 16)
                part[mine_r, :] = part[mine_r, :] + (part[rows(co * td + r, 16), :] if key == "d2" else acc_d[rows(r, 16), :])
                return carry

            lax.fori_loop(0, ch // 16, step, 0)
            if k == 0:
                for h in range(2):
                    push((key, "A", h), lambda h=h: (mine(order[0], h), slot(key, 0, h), at_z(pair)))
            elif k < 3:
                @pl.when(outer == 1)
                def _():
                    for h in range(2):
                        copy_of((key, "BC"[k - 1], h), (key, "BC"[k - 1], h), mine(order[k], h), slot(key, k, h), at_z(pair)).start()


    def z_relay(key, n, h):
        @pl.when(inner == 1)
        def _():
            got((key, "AB"[n], h), slot(key, n, h))
            zi = (far_outer, far_inner)[n]
            work = slot(key, n, h)

            def step(i, carry):
                r = rows(i * 8, 8)
                work[r, :] = work[r, :] + part[rows(c * td + zi * ch + h * hc + i * 8, 8), :]
                return carry

            lax.fori_loop(0, hc // 8, step, 0)
            if n == 0:
                copy_of((key, "B", h), (key, "B", h), work, slot(key, 1, h), at_z(far_outer)).start()
            else:
                copy_of((key, "C", h), (key, "D", h), work, slot(key, 3, h), at_z(far_inner)).start()

    def z_got(key):
        base = z_ids(key)
        for h in range(2):
            for i in range(2):
                with jax.named_scope("got_" + key):
                    got(base + 4 * h + 2 * inner + i, slot(key, 2 * inner + i, h))

    def z_sum(key, i):
        r = rows(i * 16, 16)
        return part[rows(c * td + z * ch + i * 16, 16), :] + from_z[2 * inner, r, :] + from_z[2 * inner + 1, r, :]

    def relay_sends_done(key):
        @pl.when(inner == 1)
        def _():
            for s in "BC":
                for h in range(2):
                    copy_of((key, s, h), 0, mine(0, h), slot(key, 0, h), at_z(pair)).wait_send()

    def sum_sends_done(key):
        for part_key in [(key, "c", k) for k in range(4)] + [(key, "A", h) for h in range(2)]:
            send_done(part_key)

        @pl.when(outer == 1)
        def _():
            for s in "BC":
                for h in range(2):
                    copy_of((key, s, h), 0, mine(0, h), slot(key, 0, h), at_z(pair)).wait_send()

    def quarter(ref, core, zi):
        return ref.at[rows(core * td + zi * ch, ch)]

    def zg_id(key, zi):
        base = sid((key, "z", 0))
        for i in range(4):
            assert sid((key, "z", i)) == base + i
        return base + zi

    relayed = ("n1z",)

    def takes(key):
        return (pair, far_inner, far_outer) if key in relayed else others

    def z_push(key, make, zi):
        for k, dev in enumerate((toward,) if key in relayed else others):
            push((key, "zs", k), lambda dev=dev: (*make(zi), at_z(dev)), zg_id(key, zi), group=("X", key[:2]))
        if key in relayed:
            z_forward(key, 3, make(zi)[1], zg_id(key, zi), pair)
            passed[(key, "fw", 3)] = lambda: make(z)[1]

    def z_forward(key, i, ref, rkey, dev):
        @pl.when(inner == 1)
        def _():
            copy_of((key, "fw", i), rkey, ref, ref, at_z(dev)).start()

    def z_pass(key, make, i):
        zi = takes(key)[i]
        with jax.named_scope("got_%s_%d" % (key, i)):
            got(zg_id(key, zi), make(zi)[1])
        if key in relayed:
            z_forward(key, i, make(zi)[1], zg_id(key, zi), (far_inner, pair, pair)[i])
            passed[(key, "fw", i)] = lambda: make(zi)[1]

    def passed_done(which):
        @pl.when(inner == 1)
        def _():
            for key in [k1 for k1 in passed if k1[0] == which]:
                ref = passed.pop(key)
                copy_of(key, 0, ref(), ref(), to_c).wait_send()

    def z_gather(key, ref):
        z_push(key, lambda zi: (quarter(ref, c, zi), quarter(ref, c, zi)), z)
        push((key, "s", 0), lambda: (quarter(ref, c, z), quarter(ref, c, z), to_c), (key, "s"), group=("X", key[:2]))

    def z_take(key, ref, i):
        z_pass(key, lambda zi: (quarter(ref, c, zi), quarter(ref, c, zi)), i)
        push((key, "s", 1 + i), lambda: (quarter(ref, c, takes(key)[i]), quarter(ref, c, takes(key)[i]), to_c), (key, "s"), group=("X", key[:2]))

    def z_gathered_partner(key, ref):
        got((key, "s"), ref.at[rows(co * td, td)])

    def stage(buf, block, slot_ref, key):
        for core in range(2):
            local((key, core), buf.at[block, core], slot_ref.at[pl.ds(core * td, td)]).start()

    def staged(buf, block, slot_ref, key):
        for core in range(2):
            local((key, core), buf.at[block, core], slot_ref.at[pl.ds(core * td, td)]).wait()

    def save_ab(block):
        return (local("sa", a_t, a_save.at[block]), local("sb", b_t, b_save.at[block]))

    @scoped
    def f0_other(j, slot):
        fwd(0, nb.at[slot], None)
        for s in save_ab(block_of(j)):
            s.start()

    def saves_done(block):
        for s in save_ab(block):
            s.wait()

    def a_kept(k):
        return wg.at[1, rows(k * t2, t2)]

    def b_kept(k):
        return wd.at[1, rows((k // 2) * t2, t2), cols((k % 2) * hh, hh)]

    def load_ab(block, k):
        return (local(("la", k), a_save.at[block], a_kept(k)), local(("lb", k), b_save.at[block], b_kept(k)))

    def grad_piece(i, xb, core):
        return (acc_g, acc_u)[i].at[rows(core * rb, rb), cols(xb * fb, fb)]

    def grad_land(l, i, xb, core):
        if l == 1:
            return (dwg1, dwu1)[i].at[:, cols((2 * xb + core) * fb, fb)]
        return part.at[:, cols(i * hh + xb * fb, fb)]

    def grads_push(l):
        for i in range(2):
            for xb in range(2):
                push(("q", l, i, xb), lambda i=i, xb=xb: (grad_piece(i, xb, co), grad_land(l, i, xb, c), to_c), ("q", l))

    def grads_out():
        for i in range(2):
            for xb in range(2):
                local(("qo", i, xb), grad_piece(i, xb, c), grad_land(1, i, xb, c)).start()
        local("qd", acc_d, dwd1).start()

    @scoped
    def grads_out_done(l):
        for i in range(2):
            for xb in range(2):
                if l == 1:
                    local(("qo", i, xb), grad_piece(i, xb, c), grad_land(1, i, xb, c)).wait()
                send_done(("q", l, i, xb))
        got(("q", l), acc_d)
        if l == 1:
            local("qd", acc_d, dwd1).wait()
        else:
            got("dab", nb.at[0])
            for i in range(2):
                w = pl.ds(i * hh, hh)
                part[:, w] += mm(n_half(3)[:, rows(c * rb, rb)], their_d(i)[...], 0, 0)
            for i in range(2):
                send_done(("dab", i))

    barrier = pltpu.get_barrier_semaphore()
    for dev in (to_c, to_x, {"fsdp": 2 * xo + co}, to_y, at_z((z + 1) % 4), at_z((z + 2) % 4), at_z((z + 3) % 4)):
        pl.semaphore_signal(barrier, inc=1, device_id=dev, device_id_type=MESH)
    x_load = local("x", x_in, nb.at[1, pl.ds(0, td)])
    x_load.start()
    with jax.named_scope("barrier"):
        pl.semaphore_wait(barrier, 7)

    dy_src = lambda: dy_in
    n0_src = lambda: n0_buf.at[q, c]
    n1_src = lambda: n_own.at[rows(c * td, td)]
    o0_src = lambda: o_own.at[rows(c * td, td)]
    cut_n, cut_o = ch, half

    push_w(0, 0)
    push_wc(0)
    x_load.wait()

    def n0_step(i, carry):
        h_f = n_own[rows(i * 16, 16), :].astype(F32)
        r_inv = rinv(h_f)
        nb[0, rows(c * td + i * 16, 16), :] = (h_f * r_inv * gain[0:1, :]).astype(BF16)
        r_own[rows(c * td + i * 16, 16), :] = jnp.broadcast_to(r_inv, (16, 128))
        return carry

    lax.fori_loop(0, td // 16, n0_step, 0)
    n0_mine = lambda: nb.at[0, rows(c * td, td)]
    push("n0p", lambda: (n0_mine(), n0_mine(), to_c))
    r_mine = lambda: r_own.at[rows(c * td, td)]
    push("rp", lambda: (r_mine(), r_mine(), to_c))
    keep = local("n0k", n0_mine(), n0_buf.at[q, c])
    keep.start()
    keep.wait()
    ag_quarter("n0", n0_buf, n0_src, "y")
    ag_quarter("n0", n0_buf, n0_src, "x")
    ag_quarter("o1", o1_buf, dy_src, "y")
    push_w(0, 1)
    push_w(1, 0)
    push_w(1, 1)
    ag_x("o1", o1_buf, dy_src, 1)
    push("xp", lambda: (x_in, x_part, to_c))
    push("dyp", lambda: (dy_in, o1_buf.at[q, c], to_c))
    push_wc(1)
    local("xc", x_in.at[rows(z * ch, ch)], x_ch).start()
    local("dy_own", dy_in, ob.at[0, rows(c * td, td)]).start()

    @scoped
    def h1_calc():
        def h1_step(i, carry):
            r = rows(i * 16, 16)
            h1 = (x_ch[r, :].astype(F32) + z_sum("d0", i)).astype(BF16)
            h1_ch[r, :] = h1
            h_f = h1.astype(F32)
            n_own[rows(c * td + z * ch + i * 16, 16), :] = (h_f * rinv(h_f) * gain[1:2, :]).astype(BF16)
            return carry

        lax.fori_loop(0, ch // 16, h1_step, 0)

    def h1_done():
        z_got("d0")
        relay_sends_done("d0")
        h1_calc()
        z_gather("n1z", n_own)

    relay_gu(0, 0, 0)
    ag_spread("n0", n0_buf, "y")
    ag_spread("o1", o1_buf, "y")
    relay_gu(0, 0, 1)
    ag_spread("n0", n0_buf, "x")
    relay_gu(0, 1, 0)
    relay_gu(0, 1, 1)
    got("n0p", nb.at[0, rows(co * td, td)])
    got("rp", r_own.at[rows(co * td, td)])
    keep2 = local("n0k2", nb.at[0, rows(co * td, td)], n0_buf.at[q, co])
    keep2.start()
    have_gu(0, (0,))
    with jax.named_scope("fwd_tile0"):
        fwd_tile(0, nb.at[0], g_t, 0)
    relay_d(0, 0)
    relay_d(0, 1)
    have_gu(0, (1,))
    with jax.named_scope("fwd_tile1"):
        for i in range(1, hh // tile):
            fwd_tile(0, nb.at[0], g_t, i)
    for s in save_ab(q):
        s.start()
    have_d_own(0)
    relay_d(0, 2)
    down_half(0, g_t, x, 0, t2, False)
    relay_d(0, 3)
    ag_spread_got("n0", n0_buf, "y")
    have_d(0)
    down_half(0, g_t, xo, co * td, td, True)
    core_push("d0")
    down_half(0, g_t, xo, c * td, td, True)
    core_sum_send("d0")
    keep2.wait()
    send_done("n0p")
    saves_done(q)
    partner_has("n0", n0_buf, 0)
    stage(n0_buf, block_of(0), nb.at[0], "sn")
    relay_gu(1, 0, 0)
    staged(n0_buf, block_of(0), nb.at[0], "sn")
    f0_other(0, 0)
    z_relay("d0", 0, 0)
    relay_gu(1, 0, 1)
    z_relay("d0", 0, 1)
    ag_spread_got("n0", n0_buf, "x")
    ag_spread_got("o1", o1_buf, "y")
    partner_has("n0", n0_buf, 1)
    stage(n0_buf, block_of(1), nb.at[0], "sn")
    z_relay("d0", 1, 0)
    relay_gu(1, 1, 0)
    z_relay("d0", 1, 1)
    local("xc", x_in.at[rows(z * ch, ch)], x_ch).wait()

    @pl.when(outer == 1)
    def _():
        h1_done()

    relay_gu(1, 1, 1)

    @pl.when(inner == 1)
    def _():
        h1_done()

    local("dyc", dy_in.at[rows(z * ch, ch)], x_ch).start()
    group_done(("W", 0))
    flush(("xp", "dyp", "rp"))
    relay_d(1, 0)
    z_take("n1z", n_own, 0)
    z_take("n1z", n_own, 1)
    relay_d(1, 1)
    z_take("n1z", n_own, 2)
    relay_d(1, 2)
    saves_done(block_of(0))
    for h in (1, 0):
        ag_x("n1", n1_buf, n1_src, h)
    ag_x("o1", o1_buf, dy_src, 0)
    for h in range(2):
        ag_y("n1", n1_buf, n1_src, h)
    got("dyp", o1_buf.at[q, co])
    dy_other = local("dy_other", o1_buf.at[q, co], ob.at[0, rows(co * td, td)])
    dy_other.start()
    z_gathered_partner("n1z", n_own)

    have_gu(1, (0, 1))
    fwd(1, n_own, g_t)
    local("dy_own", dy_in, ob.at[0, rows(c * td, td)]).wait()
    dy_other.wait()
    have_d_own(1)
    bwd_tile(1, ob.at[0], x, a_t, b_t)
    sum_sends_done("d0")
    m_half(1, x, 0, t2, False)
    have_d(1)
    bwd_tile(1, ob.at[0], xo, a_t, b_t)
    g_keep = local("gk", g_t, g_save)
    g_keep.start()
    m_half(1, xo, co * td, td, True)
    core_push("d1")
    m_half(1, xo, c * td, td, True)
    core_sum_send("d1")
    zero_acc()
    g_keep.wait()
    local("dyc", dy_in.at[rows(z * ch, ch)], x_ch).wait()

    @scoped
    def e_calc():
        def e_step(i, dg1):
            r = rows(i * 16, 16)
            m = z_sum("d1", i)
            h_f = h1_ch[r, :].astype(F32)
            r_inv = rinv(h_f)
            xh = h_f * r_inv
            v = m * gain[1:2, :]
            e = x_ch[r, :].astype(F32) + r_inv * (v - xh * jnp.mean(v * xh, axis=-1, keepdims=True))
            o_own[rows(c * td + z * ch + i * 16, 16), :] = e.astype(BF16)
            return dg1 + jnp.sum(m * xh, axis=0, keepdims=True)

        dg[1:2, :] = lax.fori_loop(0, ch // 16, e_step, jnp.zeros((1, d), F32))

    def at_step(k, n):
        return pl.when(k == n)

    def stage_n(buf, block, slot):
        stage(buf, block, nb.at[slot], ("n", slot))

    def staged_n(buf, block, slot):
        staged(buf, block, nb.at[slot], ("n", slot))

    def stage_o(buf, block, slot):
        stage(buf, block, ob.at[slot], ("o", slot))

    def staged_o(buf, block, slot):
        staged(buf, block, ob.at[slot], ("o", slot))

    xl = lambda: [local("xl0", x_in, nb.at[0, rows(c * td, td)]), local("xl1", x_part, nb.at[0, rows(co * td, td)])]

    def n_half(slot):
        return wu.at[1, rows(slot * t2, t2)]

    def n_half_copies(block, slot):
        return [local(("nh", slot, core), n0_buf.at[block, core, :, cols(2 * x * rb, 2 * rb)], wu.at[1, rows(slot * t2 + core * td, td)]) for core in range(2)]

    def load_n_half(block, slot):
        for s in n_half_copies(block, slot):
            s.start()

    own_g = nb.at[1, :, pl.ds(0, hh)]

    def e_done():
        z_got("d1")
        relay_sends_done("d1")
        e_calc()
        z_gather("o0z", o_own)
        for dev in others:
            pl.semaphore_signal(credit, inc=1, device_id=at_z(dev), device_id_type=MESH)

    def l1_step(k, carry):
        slot = 1 - (k + 3) // 4

        @pl.when(k > 0)
        def _():
            @at_step(k, 1)
            def _():
                partner_has("o1", o1_buf, 0)
                stage_o(o1_buf, block_of(0), 0)

            staged_n(n1_buf, block_of(k - 1), 0)
            with jax.named_scope("fwd_a"):
                fwd_tile(1, nb.at[0], None, 0)

            @at_step(k, 2)
            def _():
                ag_got_x("o1", o1_buf, 0, cut_o)

            @at_step(k, 3)
            def _():
                ag_got_dx("o1", o1_buf, cut_o)
                for h in range(2):
                    ag_got_dy("o1", o1_buf, h, cut_o)

            with jax.named_scope("fwd_b"):
                for i in range(1, hh // tile):
                    fwd_tile(1, nb.at[0], None, i)

            @pl.when(k * inner == 2)
            def _():
                e_done()

            @pl.when(k > 1)
            def _():
                partner_has("o1", o1_buf, k - 1)
                stage_o(o1_buf, block_of(k - 1), 0)

            @at_step(k, 3)
            def _():
                for i in range(3):
                    z_take("o0z", o_own, i)
                for h in range(2):
                    ag_x("o0", o0_buf, o0_src, 1 - h)
                    ag_y("o0", o0_buf, o0_src, h)

            @at_step(k, 1)
            def _():
                z_relay("d1", 1, 0)
                ag_got_x("n1", n1_buf, 0, half)

            staged_o(o1_buf, block_of(k - 1), 0)
            bwd_hidden(1, ob.at[0], a_t, b_t)

            @at_step(k, 1)
            def _():
                z_relay("d1", 1, 1)

                @pl.when(outer == 1)
                def _():
                    e_done()

                partner_has("n1", n1_buf, 1)

            @at_step(k, 2)
            def _():
                local("gl", g_save, own_g).wait()
                sum_sends_done("d1")
                down_rows(1, own_g, co)
                core_push("d2")
                ag_got_dx("n1", n1_buf, half)
                ag_got_dy("n1", n1_buf, 1, half)
                down_rows(1, own_g, c)
                core_back_start("d2")

            @at_step(k, 1)
            def _():
                group_done(("X", "n1"))
                passed_done("n1z")
                local("gl", g_save, own_g).start()

            @at_step(k, 3)
            def _():
                z_relay("d2", 0, 0)
                group_done(("W", 1))
                for i in range(3):
                    for s in load_ab(block_of(i - 1) if i else q, i):
                        s.start()
                    load_n_half(block_of(i - 1) if i else q, i)

        weight_grads(nb.at[slot], 2 * x * rb, ob.at[0], None)

        @at_step(k, 1)
        def _():
            stage_n(n1_buf, block_of(1), 0)

        @at_step(k, 2)
        def _():
            partner_has("n1", n1_buf, 2)
            stage_n(n1_buf, block_of(2), 0)
            pl.semaphore_wait(credit, 3)
            core_sum_send("d2")

        @at_step(k, 0)
        def _():
            staged(n0_buf, block_of(1), nb.at[0], "sn")
            f0_other(1, 0)
            ag_got_x("o1", o1_buf, 1, cut_o)
            ag_got_x("n1", n1_buf, 1, half)
            z_relay("d1", 0, 0)
            ag_got_y("n1", n1_buf, 0)
            ag_dx("o1", o1_buf, cut_o)
            ag_dx("n0", n0_buf, cut_n)
            ag_dy("n0", n0_buf, cut_n)
            z_relay("d1", 0, 1)
            ag_got_y("n1", n1_buf, 1)
            partner_has("n1", n1_buf, 0)
            stage_n(n1_buf, block_of(0), 0)
            saves_done(block_of(1))

        return carry

    lax.fori_loop(0, 4, l1_step, 0)
    got("xp", x_part)
    for s in xl():
        s.start()
    for s in load_ab(q, 0):
        s.wait()
    z_gathered_partner("o0z", o_own)
    z_relay("d2", 0, 1)
    grads_push(1)
    grads_out()

    def y_rows(zi):
        return y_out.at[rows(zi * ch, ch)]

    zg_id("y", 0)

    @scoped
    def dgain0():
        def dg_step(i, carry):
            w = cols(i * tile, tile)
            m = mm(a_t[...], wg[0, rows(i * tile, tile)], 1, 1) + mm(b_t[...], wu[0, rows(i * tile, tile)], 1, 1)
            xh = nb[0, :, w].astype(F32) * r_own[:, 0:1]
            dg[0:1, w] = jnp.sum(m * xh, axis=0, keepdims=True)
            return carry

        lax.fori_loop(0, d // tile, dg_step, 0)

    def y_done():
        z_got("d2")

        def y_step(i, carry):
            r = rows(i * 16, 16)
            x_ch[r, :] = (h1_ch[r, :].astype(F32) + z_sum("d2", i)).astype(BF16)
            return carry

        lax.fori_loop(0, ch // 16, y_step, 0)
        local("yk", x_ch, y_rows(z)).start()
        for i, dev in enumerate((far_inner, pair)):
            push(("y", i), lambda dev=dev: (x_ch, y_rows(z), at_z(dev)), zg_id("y", z), group=("X", "y"))

        @pl.when(outer == 1)
        def _():
            copy_of(("y", 2), zg_id("y", z), x_ch, y_rows(z), at_z(far_outer)).start()

    def y_pass():
        got(zg_id("y", far_inner), y_rows(far_inner))
        copy_of(("y", 2), zg_id("y", far_inner), y_rows(far_inner), y_rows(far_inner), at_z(pair)).start()

    def their_d(i):
        return nb.at[0, :, pl.ds(i * hh, hh)]

    def l0_step(k, carry):
        oslot = (k + 1) % 2

        @at_step(k, 2)
        def _():
            ag_got_dx("o0", o0_buf, half)
            ag_got_dy("o0", o0_buf, 1, half)

        @pl.when(k > 0)
        def _():
            staged_o_any(k)

        bwd_hidden(0, ob.at[oslot], a_kept(k), b_kept(k))

        @at_step(k, 0)
        def _():
            for s in xl():
                s.wait()
            ag_got_dx("n0", n0_buf, cut_n)
            ag_got_dy_whole("n0", n0_buf, cut_n)
            z_relay("d2", 1, 0)
            dgain0()
            dg_z[z] = dg[...]
            for i in range(3):
                push(("gs", i), lambda i=i: (dg_z.at[z], dg_z.at[z], at_z(others[i])), "gz")
            z_relay("d2", 1, 1)
            partner_has("n0", n0_buf, 2)
            stage_n(n0_buf, block_of(2), 0)
            load_n_half(block_of(2), 3)
            ag_got_y("o0", o0_buf, 0)
            ag_got_x("o0", o0_buf, 1, half)
            grads_out_done(1)
            zero_acc()
            for i in range(4):
                for s in n_half_copies(block_of(i - 1) if i else q, i):
                    s.wait()
            for i in range(1, 3):
                for s in load_ab(block_of(i - 1), i):
                    s.wait()

        @at_step(k, 1)
        def _():
            @pl.when(inner == 1)
            def _():
                y_done()

            for h in range(2):
                send_done(("d2", "A", h))
                for s in "BC":
                    copy_of(("d2", s, h), 0, mine(0, h), slot("d2", 0, h), at_z(pair)).wait_send()
            partner_has("o0", o0_buf, 1)
            group_done(("X", "o0"))
            stage_o(o0_buf, block_of(1), 1)
            got("gz", dg_z.at[pl.ds(0, 3)])
            for i in range(3):
                send_done(("gs", i))
            dg[...] = dg_z[0] + dg_z[1] + dg_z[2] + dg_z[3]
            push("gc", lambda: (dg, dg_core, to_c))

        @at_step(k, 2)
        def _():
            got("gc", dg_core)
            copy_of("gc", 0, dg, dg_core, to_c).wait_send()
            dg[...] = dg[...] + dg_core[...]
            push("gx", lambda: (dg, dg_x, to_x))
            partner_has("o0", o0_buf, 2)
            stage_o(o0_buf, block_of(2), 0)

        @at_step(k, 3)
        def _():
            got("gx", dg_x)
            copy_of("gx", 0, dg, dg_x, to_x).wait_send()
            dg[...] = dg[...] + dg_x[...]
            push("gy", lambda: (dg, dg_y, to_y))

            @pl.when(inner == 1)
            def _():
                y_pass()

        @at_step(k, 3)
        def _():
            for i in range(2):
                push(("dab", i), lambda i=i: ((a_t, b_t)[i], their_d(i), to_c), "dab")

        weight_grads(n_half(k), 0, ob.at[oslot], k < 3)

        @at_step(k, 2)
        def _():
            grads_push(0)

        @at_step(k, 0)
        def _():
            staged_n(n0_buf, block_of(2), 0)
            with jax.named_scope("f0_a"):
                fwd_tile(0, nb.at[0], None, 0, a_kept(3), b_kept(3))
            ag_got_y("o0", o0_buf, 1)
            ag_got_x("o0", o0_buf, 0, half)
            with jax.named_scope("f0_b"):
                for i in range(1, hh // tile):
                    fwd_tile(0, nb.at[0], None, i, a_kept(3), b_kept(3))

            partner_has("o0", o0_buf, 0)
            stage_o(o0_buf, block_of(0), 0)

            @pl.when(outer == 1)
            def _():
                y_done()

            for a in ("n0", "o1", "n1"):
                group_done(("S", a))

        return carry

    def staged_o_any(k):
        for n, slot in ((1, 0), (2, 1), (3, 0)):
            @at_step(k, n)
            def _(n=n, slot=slot):
                staged_o(o0_buf, block_of(n - 1), slot)

    lax.fori_loop(0, 4, l0_step, 0)
    for key in ("gc", "gx", "gy"):
        sent.pop(key)
    got("gy", dg_y)
    copy_of("gy", 0, dg, dg_y, to_y).wait_send()
    dgain_out[...] = dg[...] + dg_y[...]
    grads_out_done(0)
    with jax.named_scope("got_y"):
        got(zg_id("y", pair), y_rows(pair))
        got(zg_id("y", far_outer), y_rows(far_outer))

        @pl.when(outer == 1)
        def _():
            got(zg_id("y", far_inner), y_rows(far_inner))

        copy_of(("y", 2), 0, x_ch, x_ch, to_c).wait_send()
    local("yk", x_ch, y_rows(z)).wait()
    for key in list(sent):
        send_done(key)
    for group in list(groups):
        group_done(group)
    assert not passed


def finish(acc_g, acc_u, acc_d, other, gain_in, g1, u1, d1, y_in, g_out, u_out, d_out, y_out, gain_out, buf, ybuf, sem_in, sem_out):
    rb, hh = other.shape[0], acc_g.shape[1]
    fb = hh // 2
    f = lax.axis_index("fsdp")
    c = f % 2
    ins = [pltpu.make_async_copy(src, buf.at[i], sem_in.at[i]) for i, src in enumerate((g1, u1, d1))]
    ins.append(pltpu.make_async_copy(y_in, ybuf, sem_in.at[3]))
    for copy in ins:
        copy.start()
    outs = []

    def out(src, dst):
        copy = pltpu.make_async_copy(src, dst, sem_out.at[len(outs)])
        copy.start()
        outs.append(copy)

    for i, (acc, dst) in enumerate(((acc_g, g_out), (acc_u, u_out))):
        for xb in range(2):
            own = pl.ds(pl.multiple_of((2 * xb + c) * fb, 128), fb)
            out(acc.at[pl.ds(pl.multiple_of(c * rb, rb), rb), pl.ds(xb * fb, fb)], dst.at[0, :, own])
            theirs = pl.ds(pl.multiple_of((2 * xb + 1 - c) * fb, 128), fb)
            out(other.at[:, pl.ds(i * hh + xb * fb, fb)], dst.at[0, :, theirs])
    out(acc_d, d_out.at[0])
    out(gain_in, gain_out)
    for i, dst in enumerate((g_out, u_out, d_out)):
        ins[i].wait()
        out(buf.at[i], dst.at[1])
    ins[3].wait()
    out(ybuf, y_out)
    for copy in outs:
        copy.wait()


def make_call(td, d, rb, hs):
    fb = hs // 4
    hh, t2, ch = 2 * fb, 2 * td, td // 4
    shape = jax.ShapeDtypeStruct
    hbm = pl.BlockSpec(memory_space=pl.ANY)
    vmem = pl.BlockSpec(memory_space=pltpu.VMEM)
    block = shape((4, 2, td, d), BF16)
    outs = [
        shape((td, d), BF16), shape((rb, hs), F32), shape((rb, hs), F32), shape((fb, d), F32), pltpu.VMEM((2, d), F32),
        pltpu.VMEM((2 * rb, hh), F32), pltpu.VMEM((2 * rb, hh), F32), pltpu.VMEM((fb, d), F32), pltpu.VMEM((t2, d), F32),
        block, block, block, block, shape((4, t2, hh), BF16), shape((4, t2, hh), BF16), shape((td, d), BF16), shape((t2, hh), BF16), shape((td, d), F32),
    ]
    scratch = [
        pltpu.VMEM((2, d, hh), BF16), pltpu.VMEM((2, d, hh), BF16), pltpu.VMEM((2, hh, d), BF16),
        pltpu.VMEM((2, t2, d), BF16), pltpu.VMEM((2, t2, d), BF16),
        pltpu.VMEM((t2, hh), BF16), pltpu.VMEM((t2, hh), BF16), pltpu.VMEM((t2, hh), BF16),
        pltpu.VMEM((4, ch, d), F32),
        pltpu.VMEM((ch, d), BF16), pltpu.VMEM((ch, d), BF16),
        pltpu.VMEM((t2, 128), F32),
        pltpu.VMEM((2, d), F32), pltpu.VMEM((2, d), F32), pltpu.VMEM((2, d), F32), pltpu.VMEM((2, d), F32), pltpu.VMEM((4, 2, d), F32),
        pltpu.SemaphoreType.DMA((NSEND,)), pltpu.SemaphoreType.DMA((NRECV,)), pltpu.SemaphoreType.DMA((NLOC,)), pltpu.SemaphoreType.REGULAR,
    ]
    step = pl.pallas_call(
        kernel,
        out_shape=outs,
        in_specs=[hbm] * 5 + [vmem],
        out_specs=[hbm] * 4 + [vmem] * 5 + [hbm] * 9,
        scratch_shapes=scratch,
        compiler_params=pltpu.CompilerParams(collective_id=0, has_side_effects=True, vmem_limit_bytes=VLIM),
    )
    end = pl.pallas_call(
        finish,
        out_shape=[shape((2, rb, hs), F32), shape((2, rb, hs), F32), shape((2, fb, d), F32), shape((td, d), BF16), shape((2, d), F32)],
        in_specs=[vmem] * 5 + [hbm] * 4,
        out_specs=[hbm] * 5,
        scratch_shapes=[pltpu.VMEM((3, rb, hs), F32), pltpu.VMEM((td, d), BF16), pltpu.SemaphoreType.DMA((4,)), pltpu.SemaphoreType.DMA((14,))],
        compiler_params=pltpu.CompilerParams(vmem_limit_bytes=VLIM2),
    )

    def call(*args):
        y, g1, u1, d1, dgain, acc_g, acc_u, acc_d, other = step(*args)[:9]
        kept = [pltpu.with_memory_space_constraint(v, pltpu.VMEM) for v in (acc_g, acc_u, acc_d, other, dgain)]
        stored = [pltpu.with_memory_space_constraint(v, pltpu.HBM) for v in (g1, u1, d1, y)]
        g, u, dd, y, dgain = end(*kept, *stored)
        return y, g, u, dd, dgain

    return call


def solution(mesh):
    tok_spec = P(("replica", "fsdp"), None)
    wide_spec = P(None, "fsdp", "tensor")
    down_spec = P(None, ("tensor", "fsdp"), None)
    gain_spec = P(None, None)

    def device_fn(x_loc, dy_loc, w_gate, w_up, w_down, norm_gain):
        call = make_call(x_loc.shape[0], x_loc.shape[1], w_gate.shape[1], w_gate.shape[2])
        return call(x_loc, dy_loc, w_gate, w_up, w_down, norm_gain)

    return jax.shard_map(device_fn, mesh=mesh, in_specs=(tok_spec, tok_spec, wide_spec, wide_spec, down_spec, gain_spec), out_specs=(tok_spec, wide_spec, wide_spec, down_spec, gain_spec), check_vma=False)
```

```python
import jax
import jax.numpy as jnp
import numpy as np
from jax import lax
from jax.experimental import pallas as pl
from jax.experimental.pallas import tpu as pltpu
from jax.sharding import PartitionSpec as P

F32 = jnp.float32
BF16 = jnp.bfloat16
MESH = pl.DeviceIdType.MESH
NSEND = 65
NRECV = 130
NLOC = 55
VLIM = 67043328 - 16 * 2**20 - 2**17
VLIM2 = 14 * 2**20


def mm(lhs, rhs, ldim, rdim):
    return lax.dot_general(lhs, rhs, (((ldim,), (rdim,)), ((), ())), preferred_element_type=F32)


def kernel(
    x_in, dy_in, wg_in, wu_in, wd_in, gain,
    y_out, dwg1, dwu1, dwd1, dgain_out, acc_g, acc_u, acc_d, part, n0_buf, n1_buf, o1_buf, o0_buf, a_save, b_save, x_part, g_save, core_hbm,
    wg, wu, wd, nb, ob, a_t, b_t, g_t, from_z,
    x_ch, h1_ch, r_own, dg, dg_core, dg_x, dg_y, dg_z, ssem, rsem, lsem, credit,
):
    td, d = x_in.shape
    rb = wg_in.shape[1]
    fb = wg_in.shape[2] // 4
    hh = 2 * fb
    t2, ch, half = 2 * td, td // 4, td // 2
    hc = ch // 2
    tile = min(512, fb)
    z = lax.axis_index("tensor")
    y = lax.axis_index("replica")
    f = lax.axis_index("fsdp")
    x, c = f // 2, f % 2
    xo, yo, co = 1 - x, 1 - y, 1 - c
    q, qx, qy, qd = 2 * y + x, 2 * y + xo, 2 * yo + x, 2 * yo + xo
    cs = (c + y) % 2
    cso = 1 - cs
    to_c, to_x, to_xs, to_y = {"fsdp": 2 * x + co}, {"fsdp": 2 * xo + c}, {"fsdp": 2 * xo + cs}, {"replica": yo}
    inner = ((z + 1) // 2) % 2
    outer = 1 - inner
    up = z // 2
    pair = z + 1 - 2 * (z % 2)
    far_outer, far_inner = 3 - 3 * up, 2 - up
    order = (outer * far_outer + inner * pair, outer * far_inner + inner * far_outer, outer * pair + inner * far_inner, z)

    n_own, o_own = nb.at[1], ob.at[1]

    def at_z(i):
        return {"tensor": i}

    def z_other(k):
        return (z + 4 + k * (1 - 2 * up)) % 4

    others = tuple(z_other(k) for k in (1, 2, 3))
    toward = outer * pair + inner * far_inner

    def rows(start, size):
        return pl.ds(start if isinstance(start, int) else pl.multiple_of(start, size if size % 16 == 0 else 8), size)

    def cols(start, size):
        return pl.ds(start if isinstance(start, int) else pl.multiple_of(start, 128), size)

    ids, sids, lids, sent, passed, groups = {}, {}, {}, {}, {}, {}

    def numbered(table, key, limit):
        i = table.setdefault(key, len(table))
        assert i < limit, i
        return i

    def sid(key):
        return numbered(ids, key, NRECV)

    def name_of(key):
        return key if isinstance(key, str) else "_".join(map(str, key))

    def copy_of(skey, rkey, src, dst, dev):
        send = 0 if skey is None else numbered(sids, skey, NSEND)
        recv = sid(rkey) if isinstance(rkey, (str, tuple)) else rkey
        return pltpu.make_async_remote_copy(src_ref=src, dst_ref=dst, send_sem=ssem.at[send], recv_sem=rsem.at[recv], device_id=dev, device_id_type=MESH)

    def push(key, make, rkey=None, group=None):
        src, dst, dev = make()
        copy_of(group or key, key if rkey is None else rkey, src, dst, dev).start()
        if group is None:
            sent[key] = make
        else:
            groups.setdefault(group, {})[key] = int(np.prod(src.shape))

    def group_done(group):
        n = sum(groups.pop(group).values()) // d
        assert n % 2 == 0 and n <= 2 * hh, n
        view = wd.at[:, pl.ds(0, n // 2)]
        copy_of(group, 0, view, view, to_c).wait_send()

    def got(key, dst):
        with jax.named_scope("got_" + (name_of(key) if isinstance(key, (str, tuple)) else "dyn")):
            copy_of(None, key, dst, dst, to_c).wait_recv()

    def send_done(key):
        copy_of(key, 0, *sent.pop(key)()).wait_send()

    def flush(keys):
        for key in keys:
            send_done(key)

    def local(key, src, dst):
        i = numbered(lids, key, NLOC)
        return pltpu.make_async_copy(src, dst, lsem.at[i])

    def scoped(fn):
        def run(*args):
            with jax.named_scope(fn.__name__):
                return fn(*args)

        return run

    gu = ((wg_in, wg), (wu_in, wu))
    pieces = (2, 2)

    def wview(m, l, row, xb, k=0, n=1):
        return gu[m][1].at[l, rows(row * rb + k * (rb // n), rb // n), cols(xb * fb, fb)]

    def wsrc(m, l, xb, core, k=0, n=1):
        return gu[m][0].at[l, pl.ds(k * (rb // n), rb // n), cols((2 * xb + core) * fb, fb)]

    def push_w(l, m):
        n = pieces[l]
        for xb in range(2):
            for k in range(n):
                push(("wx", l, m, xb, k), lambda xb=xb, k=k: (wsrc(m, l, xb, cs, k, n), wview(m, l, f, xb, k, n), to_xs), group=("W", l))
        for k in range(4 * m):
            r0 = y * (fb // 2) + k * (fb // 8)
            push(("wdx", l, k), lambda r0=r0: (wd_in.at[l, rows(r0, fb // 8)], wd.at[l, rows(x * fb + r0, fb // 8)], to_x), group=("W", l))
        if (l, m) == (1, 1):
            r1 = yo * (fb // 2) + 3 * (fb // 8)
            push("wdx_last", lambda: (wd_in.at[l, rows(r1, fb // 8)], wd.at[l, rows(x * fb + r1, fb // 8)], to_x), group=("W", l))

    def push_wc(l):
        for m in range(2):
            for xb in range(2):
                push(("wc", l, m, xb), lambda m=m, xb=xb: (wsrc(m, l, xb, co), wview(m, l, f, xb), to_c), ("wc", l, xb * (1 - l)), group=("W", l))
                local(("w", l, m, xb), wsrc(m, l, xb, c), wview(m, l, f, xb)).start()
        local(("wd", l), wd_in.at[l], wd.at[l, rows(x * fb, fb)]).start()

    def relay_gu(l, m, xb):
        n = pieces[l]
        for k in range(n):
            ref = lambda k=k: wview(m, l, 2 * xo + cs, xb, k, n)
            got(("wx", l, m, xb, k), ref())
            push(("wy", l, m, xb, k), lambda k=k: (ref(k), ref(k), to_y), ("wy", l, xb * (1 - l)), group=("W", l))

    def relay_d(l, k):
        ref = lambda: wd.at[l, rows(xo * fb + y * (fb // 2) + k * (fb // 8), fb // 8)]
        got(("wdx", l, k), ref())
        push(("wdy", l, k), lambda: (ref(), ref(), to_y), ("wdy", l), group=("W", l))

    def have_gu(l, xbs):
        for m in range(2):
            for xb in xbs:
                local(("w", l, m, xb), wsrc(m, l, xb, c), wview(m, l, f, xb)).wait()
        whole = wd.at[0, pl.ds(0, 2 * len(xbs) * rb // 4)]
        got(("wc", l, xbs[-1] * (1 - l)), whole)
        got(("wy", l, xbs[-1] * (1 - l)), whole)

    def have_d_own(l):
        local(("wd", l), wd_in.at[l], wd.at[l, rows(x * fb, fb)]).wait()

    def have_d(l):
        got(("wdy", l), wd.at[l, pl.ds(0, (4 - l) * (fb // 8))])
        if l == 1:
            got(("wdx", 1, 3), wd.at[1, rows(xo * fb + y * (fb // 2) + 3 * (fb // 8), fb // 8)])
            got("wdx_last", wd.at[1, rows(xo * fb + yo * (fb // 2) + 3 * (fb // 8), fb // 8)])

    def piece(buf, block, core, start, size):
        return buf.at[block, core, pl.ds(start, size)]

    def chunk(buf, block, core, zi):
        return buf.at[block, core, rows(zi * ch, ch)]

    def part_id(a, j):
        base = sid((a, "p", 0))
        for jj in range(3):
            assert sid((a, "p", jj)) == base + jj
        return base + j

    def share(a, j, tag, ref):
        push((a, "s", j, tag), lambda: (ref(), ref(), to_c), (a, "p", j), group=("S", a))

    def ag_x(a, buf, src, h):
        push((a, "x", h), lambda: (src().at[pl.ds(h * half, half)], piece(buf, q, c, h * half, half), to_x), group=("X", a))

    def ag_y(a, buf, src, h):
        push((a, "y", h), lambda: (src().at[pl.ds(h * half, half)], piece(buf, q, c, h * half, half), to_y), group=("X", a))

    def ag_quarter(a, buf, src, axis):
        push((a, axis + "c"), lambda: (src().at[rows(z * ch, ch)], chunk(buf, q, c, z), to_y if axis == "y" else to_x), group=("S", a))

    def ag_spread(a, buf, axis):
        block = qy if axis == "y" else qx
        got((a, axis + "c"), chunk(buf, block, c, z))
        for k in (1, 2, 3):
            push((a, axis, "zs", k), lambda k=k: (chunk(buf, block, c, z), chunk(buf, block, c, z), at_z(z_other(k))), (a, axis, "zb"), group=("S", a))

    def ag_spread_got(a, buf, axis):
        block = qy if axis == "y" else qx
        got((a, axis, "zb"), buf.at[block, c, pl.ds(0, 3 * ch)])
        share(a, 0 if axis == "y" else 1, 0, lambda: buf.at[block, c])

    def ag_dx(a, buf, cut):
        push((a, "dx"), lambda: (piece(buf, qy, c, 0, cut), piece(buf, qy, c, 0, cut), to_x), group=("S", a))

    def ag_got_y(a, buf, h):
        got((a, "y", h), piece(buf, qy, c, h * half, half))
        share(a, 0, h, lambda: piece(buf, qy, c, h * half, half))
        if h == 0:
            ag_dx(a, buf, half)

    def ag_dy(a, buf, cut):
        push((a, "dy", 0), lambda: (piece(buf, qx, c, cut, td - cut), piece(buf, qx, c, cut, td - cut), to_y), group=("S", a))

    def ag_got_dy_whole(a, buf, cut):
        got((a, "dy", 0), piece(buf, qd, c, cut, td - cut))
        share(a, 2, 0, lambda: piece(buf, qd, c, cut, td - cut))

    def diag_piece(h, cut):
        start = max(cut, h * half)
        return start, (h + 1) * half - start

    def ag_got_x(a, buf, h, cut):
        got((a, "x", h), piece(buf, qx, c, h * half, half))
        start, size = diag_piece(h, cut)
        if size:
            push((a, "dy", h), lambda: (piece(buf, qx, c, start, size), piece(buf, qx, c, start, size), to_y), group=("S", a))
        share(a, 1, h, lambda: piece(buf, qx, c, h * half, half))

    def ag_got_dx(a, buf, cut):
        got((a, "dx"), piece(buf, qd, c, 0, cut))
        share(a, 2, "x", lambda: piece(buf, qd, c, 0, cut))

    def ag_got_dy(a, buf, h, cut):
        start, size = diag_piece(h, cut)
        if size:
            got((a, "dy", h), piece(buf, qd, c, start, size))
            share(a, 2, h, lambda: piece(buf, qd, c, start, size))

    def block_of(j):
        return 2 * ((y + (j + 1) % 2) % 2) + (x + (j + 1) // 2) % 2

    def partner_has(a, buf, j):
        with jax.named_scope("got_p_" + a):
            got(part_id(a, j), buf.at[block_of(j), co])

    for a in ("n0", "o1", "n1", "o0"):
        for j in range(3):
            sid((a, "p", j))

    def fwd_tile(l, n_ref, g_ref, i, a_ref=None, b_ref=None):
        w = cols(i * tile, tile)
        a = mm(n_ref[...], wg[l, :, w], 1, 0).astype(BF16)
        b = mm(n_ref[...], wu[l, :, w], 1, 0).astype(BF16)
        (a_t if a_ref is None else a_ref)[:, w] = a
        (b_t if b_ref is None else b_ref)[:, w] = b
        if g_ref is not None:
            a_f = a.astype(F32)
            g_ref[:, w] = (a_f * jax.nn.sigmoid(a_f) * b.astype(F32)).astype(BF16)

    @scoped
    def fwd(l, n_ref, g_ref, a_ref=None, b_ref=None):
        def step(i, carry):
            fwd_tile(l, n_ref, g_ref, i, a_ref, b_ref)
            return carry

        lax.fori_loop(0, hh // tile, step, 0)

    @scoped
    def down_half(l, g_ref, kb, start, size, add):
        r, k = rows(start, size), pl.ds(pl.multiple_of(kb * fb, fb), fb)

        def step(i, carry):
            w = cols(i * tile, tile)
            new = mm(g_ref[r, k], wd[l, k, w], 1, 0)
            part[r, w] = part[r, w] + new if add else new
            return carry

        lax.fori_loop(0, d // tile, step, 0)

    @scoped
    def down_rows(l, g_ref, core):
        r = rows(core * td, td)

        def step(i, carry):
            w = cols(i * tile, tile)
            part[r, w] = mm(g_ref[r, :], wd[l, :, w], 1, 0)
            return carry

        lax.fori_loop(0, d // tile, step, 0)

    @scoped
    def m_half(l, kb, start, size, add):
        r, k = rows(start, size), pl.ds(pl.multiple_of(kb * fb, fb), fb)

        def step(i, carry):
            w = rows(i * tile, tile)
            new = mm(a_t[r, k], wg[l, w, k], 1, 1) + mm(b_t[r, k], wu[l, w, k], 1, 1)
            o = cols(i * tile, tile)
            part[r, o] = part[r, o] + new if add else new
            return carry

        lax.fori_loop(0, d // tile, step, 0)

    def bwd_tile(l, o_ref, i, a_ref, b_ref):
        w = cols(i * tile, tile)
        q_f = mm(o_ref[...], wd[l, rows(i * tile, tile)], 1, 1).astype(BF16).astype(F32)
        a_f, b_f = a_ref[:, w].astype(F32), b_ref[:, w].astype(F32)
        s = jax.nn.sigmoid(a_f)
        g_t[:, w] = (a_f * s * b_f).astype(BF16)
        a_t[:, w] = (q_f * b_f * s * (1.0 + a_f * (1.0 - s))).astype(BF16)
        b_t[:, w] = (q_f * a_f * s).astype(BF16)

    @scoped
    def bwd_hidden(l, o_ref, a_ref, b_ref):
        for i in range(hh // tile):
            bwd_tile(l, o_ref, i, a_ref, b_ref)

    @scoped
    def weight_grads(n_ref, col, o_ref, theirs):
        t = min(256, fb)

        def half_rows(core):
            for i in range(rb // t):
                n_rows = n_ref[:, cols(col + core * rb + i * t, t)]
                w = rows(core * rb + i * t, t)
                acc_g[w, :] += mm(n_rows, a_t[...], 0, 0)
                acc_u[w, :] += mm(n_rows, b_t[...], 0, 0)

        if theirs is None:
            half_rows(co)
        else:
            @pl.when(theirs)
            def _():
                half_rows(co)

        half_rows(c)
        for i in range(fb // t):
            acc_d[pl.ds(i * t, t), :] += mm(g_t[:, cols(x * fb + i * t, t)], o_ref[...], 0, 0)

    @scoped
    def zero_acc():
        for ref in (acc_g, acc_u, acc_d):
            def step(i, carry, ref=ref):
                ref[rows(i * 16, 16), :] = jnp.zeros((16, ref.shape[1]), F32)
                return carry

            lax.fori_loop(0, ref.shape[0] // 16, step, 0)

    def rinv(h_f):
        return lax.rsqrt(jnp.mean(h_f * h_f, axis=-1, keepdims=True) + 1e-6)

    def core_land(key):
        return core_hbm if key == "d2" else acc_d

    def core_push(key):
        for k in range(4):
            push((key, "c", k), lambda k=k: (part.at[rows(co * td + order[k] * ch, ch)], core_land(key).at[rows(order[k] * ch, ch)], to_c))

    def z_ids(key):
        base = sid((key, "A", 0))
        for h in range(2):
            for i, s in enumerate("ABCD"):
                assert sid((key, s, h)) == base + 4 * h + i
        return base

    for sum_key in ("d0", "d1", "d2"):
        z_ids(sum_key)

    def mine(zi, h):
        return part.at[rows(c * td + zi * ch + h * hc, hc)]

    def slot(key, i, h):
        return from_z.at[i, pl.ds(h * hc, hc)]

    def core_back(k):
        return local(("cl", k), core_hbm.at[rows(order[k] * ch, ch)], part.at[rows(co * td + order[k] * ch, ch)])

    def core_back_start(key):
        for k in range(4):
            got((key, "c", k), core_land(key).at[rows(order[k] * ch, ch)])
            send_done((key, "c", k))
            core_back(k).start()

    @scoped
    def core_sum_send(key):
        z_ids(key)
        for k in range(4):
            if key == "d2":
                core_back(k).wait()
            else:
                got((key, "c", k), core_land(key).at[rows(order[k] * ch, ch)])

            def step(i, carry):
                r = order[k] * ch + i * 16
                mine_r = rows(c * td + r, 16)
                part[mine_r, :] = part[mine_r, :] + (part[rows(co * td + r, 16), :] if key == "d2" else acc_d[rows(r, 16), :])
                return carry

            lax.fori_loop(0, ch // 16, step, 0)
            if k == 0:
                for h in range(2):
                    push((key, "A", h), lambda h=h: (mine(order[0], h), slot(key, 0, h), at_z(pair)))
            elif k < 3:
                @pl.when(outer == 1)
                def _():
                    for h in range(2):
                        copy_of((key, "BC"[k - 1], h), (key, "BC"[k - 1], h), mine(order[k], h), slot(key, k, h), at_z(pair)).start()


    def z_relay(key, n, h):
        @pl.when(inner == 1)
        def _():
            got((key, "AB"[n], h), slot(key, n, h))
            zi = (far_outer, far_inner)[n]
            work = slot(key, n, h)

            def step(i, carry):
                r = rows(i * 8, 8)
                work[r, :] = work[r, :] + part[rows(c * td + zi * ch + h * hc + i * 8, 8), :]
                return carry

            lax.fori_loop(0, hc // 8, step, 0)
            if n == 0:
                copy_of((key, "B", h), (key, "B", h), work, slot(key, 1, h), at_z(far_outer)).start()
            else:
                copy_of((key, "C", h), (key, "D", h), work, slot(key, 3, h), at_z(far_inner)).start()

    def z_got(key):
        base = z_ids(key)
        for h in range(2):
            for i in range(2):
                with jax.named_scope("got_" + key):
                    got(base + 4 * h + 2 * inner + i, slot(key, 2 * inner + i, h))

    def z_sum(key, i):
        r = rows(i * 16, 16)
        return part[rows(c * td + z * ch + i * 16, 16), :] + from_z[2 * inner, r, :] + from_z[2 * inner + 1, r, :]

    def relay_sends_done(key):
        @pl.when(inner == 1)
        def _():
            for s in "BC":
                for h in range(2):
                    copy_of((key, s, h), 0, mine(0, h), slot(key, 0, h), at_z(pair)).wait_send()

    def sum_sends_done(key):
        for part_key in [(key, "c", k) for k in range(4)] + [(key, "A", h) for h in range(2)]:
            send_done(part_key)

        @pl.when(outer == 1)
        def _():
            for s in "BC":
                for h in range(2):
                    copy_of((key, s, h), 0, mine(0, h), slot(key, 0, h), at_z(pair)).wait_send()

    def quarter(ref, core, zi):
        return ref.at[rows(core * td + zi * ch, ch)]

    def zg_id(key, zi):
        base = sid((key, "z", 0))
        for i in range(4):
            assert sid((key, "z", i)) == base + i
        return base + zi

    relayed = ("n1z",)

    def takes(key):
        return (pair, far_inner, far_outer) if key in relayed else others

    def z_push(key, make, zi):
        for k, dev in enumerate((toward,) if key in relayed else others):
            push((key, "zs", k), lambda dev=dev: (*make(zi), at_z(dev)), zg_id(key, zi), group=("X", key[:2]))
        if key in relayed:
            z_forward(key, 3, make(zi)[1], zg_id(key, zi), pair)
            passed[(key, "fw", 3)] = lambda: make(z)[1]

    def z_forward(key, i, ref, rkey, dev):
        @pl.when(inner == 1)
        def _():
            copy_of((key, "fw", i), rkey, ref, ref, at_z(dev)).start()

    def z_pass(key, make, i):
        zi = takes(key)[i]
        with jax.named_scope("got_%s_%d" % (key, i)):
            got(zg_id(key, zi), make(zi)[1])
        if key in relayed:
            z_forward(key, i, make(zi)[1], zg_id(key, zi), (far_inner, pair, pair)[i])
            passed[(key, "fw", i)] = lambda: make(zi)[1]

    def passed_done(which):
        @pl.when(inner == 1)
        def _():
            for key in [k1 for k1 in passed if k1[0] == which]:
                ref = passed.pop(key)
                copy_of(key, 0, ref(), ref(), to_c).wait_send()

    def z_gather(key, ref):
        z_push(key, lambda zi: (quarter(ref, c, zi), quarter(ref, c, zi)), z)
        push((key, "s", 0), lambda: (quarter(ref, c, z), quarter(ref, c, z), to_c), (key, "s"), group=("X", key[:2]))

    def z_take(key, ref, i):
        z_pass(key, lambda zi: (quarter(ref, c, zi), quarter(ref, c, zi)), i)
        push((key, "s", 1 + i), lambda: (quarter(ref, c, takes(key)[i]), quarter(ref, c, takes(key)[i]), to_c), (key, "s"), group=("X", key[:2]))

    def z_gathered_partner(key, ref):
        got((key, "s"), ref.at[rows(co * td, td)])

    def stage(buf, block, slot_ref, key):
        for core in range(2):
            local((key, core), buf.at[block, core], slot_ref.at[pl.ds(core * td, td)]).start()

    def staged(buf, block, slot_ref, key):
        for core in range(2):
            local((key, core), buf.at[block, core], slot_ref.at[pl.ds(core * td, td)]).wait()

    def save_ab(block):
        return (local("sa", a_t, a_save.at[block]), local("sb", b_t, b_save.at[block]))

    @scoped
    def f0_other(j, slot):
        fwd(0, nb.at[slot], None)
        for s in save_ab(block_of(j)):
            s.start()

    def saves_done(block):
        for s in save_ab(block):
            s.wait()

    def a_kept(k):
        return wg.at[1, rows(k * t2, t2)]

    def b_kept(k):
        return wd.at[1, rows((k // 2) * t2, t2), cols((k % 2) * hh, hh)]

    def load_ab(block, k):
        return (local(("la", k), a_save.at[block], a_kept(k)), local(("lb", k), b_save.at[block], b_kept(k)))

    def grad_piece(i, xb, core):
        return (acc_g, acc_u)[i].at[rows(core * rb, rb), cols(xb * fb, fb)]

    def grad_land(l, i, xb, core):
        if l == 1:
            return (dwg1, dwu1)[i].at[:, cols((2 * xb + core) * fb, fb)]
        return part.at[:, cols(i * hh + xb * fb, fb)]

    def grads_push(l):
        for i in range(2):
            for xb in range(2):
                push(("q", l, i, xb), lambda i=i, xb=xb: (grad_piece(i, xb, co), grad_land(l, i, xb, c), to_c), ("q", l))

    def grads_out():
        for i in range(2):
            for xb in range(2):
                local(("qo", i, xb), grad_piece(i, xb, c), grad_land(1, i, xb, c)).start()
        local("qd", acc_d, dwd1).start()

    @scoped
    def grads_out_done(l):
        for i in range(2):
            for xb in range(2):
                if l == 1:
                    local(("qo", i, xb), grad_piece(i, xb, c), grad_land(1, i, xb, c)).wait()
                send_done(("q", l, i, xb))
        got(("q", l), acc_d)
        if l == 1:
            local("qd", acc_d, dwd1).wait()
        else:
            got("dab", nb.at[0])
            for i in range(2):
                w = pl.ds(i * hh, hh)
                part[:, w] += mm(n_half(3)[:, rows(c * rb, rb)], their_d(i)[...], 0, 0)
            for i in range(2):
                send_done(("dab", i))

    barrier = pltpu.get_barrier_semaphore()
    for dev in (to_c, to_x, {"fsdp": 2 * xo + co}, to_y, at_z((z + 1) % 4), at_z((z + 2) % 4), at_z((z + 3) % 4)):
        pl.semaphore_signal(barrier, inc=1, device_id=dev, device_id_type=MESH)
    x_load = local("x", x_in, nb.at[1, pl.ds(0, td)])
    x_load.start()
    with jax.named_scope("barrier"):
        pl.semaphore_wait(barrier, 7)

    dy_src = lambda: dy_in
    n0_src = lambda: n0_buf.at[q, c]
    n1_src = lambda: n_own.at[rows(c * td, td)]
    o0_src = lambda: o_own.at[rows(c * td, td)]
    cut_n, cut_o = ch, half

    push_w(0, 0)
    push_wc(0)
    x_load.wait()

    def n0_step(i, carry):
        h_f = n_own[rows(i * 16, 16), :].astype(F32)
        r_inv = rinv(h_f)
        nb[0, rows(c * td + i * 16, 16), :] = (h_f * r_inv * gain[0:1, :]).astype(BF16)
        r_own[rows(c * td + i * 16, 16), :] = jnp.broadcast_to(r_inv, (16, 128))
        return carry

    lax.fori_loop(0, td // 16, n0_step, 0)
    n0_mine = lambda: nb.at[0, rows(c * td, td)]
    push("n0p", lambda: (n0_mine(), n0_mine(), to_c))
    r_mine = lambda: r_own.at[rows(c * td, td)]
    push("rp", lambda: (r_mine(), r_mine(), to_c))
    keep = local("n0k", n0_mine(), n0_buf.at[q, c])
    keep.start()
    keep.wait()
    ag_quarter("n0", n0_buf, n0_src, "y")
    ag_quarter("n0", n0_buf, n0_src, "x")
    ag_quarter("o1", o1_buf, dy_src, "y")
    push_w(0, 1)
    push_w(1, 0)
    push_w(1, 1)
    ag_x("o1", o1_buf, dy_src, 1)
    push("xp", lambda: (x_in, x_part, to_c))
    push("dyp", lambda: (dy_in, o1_buf.at[q, c], to_c))
    push_wc(1)
    local("xc", x_in.at[rows(z * ch, ch)], x_ch).start()
    local("dy_own", dy_in, ob.at[0, rows(c * td, td)]).start()

    @scoped
    def h1_calc():
        def h1_step(i, carry):
            r = rows(i * 16, 16)
            h1 = (x_ch[r, :].astype(F32) + z_sum("d0", i)).astype(BF16)
            h1_ch[r, :] = h1
            h_f = h1.astype(F32)
            n_own[rows(c * td + z * ch + i * 16, 16), :] = (h_f * rinv(h_f) * gain[1:2, :]).astype(BF16)
            return carry

        lax.fori_loop(0, ch // 16, h1_step, 0)

    def h1_done():
        z_got("d0")
        relay_sends_done("d0")
        h1_calc()
        z_gather("n1z", n_own)

    relay_gu(0, 0, 0)
    ag_spread("n0", n0_buf, "y")
    ag_spread("o1", o1_buf, "y")
    relay_gu(0, 0, 1)
    ag_spread("n0", n0_buf, "x")
    relay_gu(0, 1, 0)
    relay_gu(0, 1, 1)
    got("n0p", nb.at[0, rows(co * td, td)])
    got("rp", r_own.at[rows(co * td, td)])
    keep2 = local("n0k2", nb.at[0, rows(co * td, td)], n0_buf.at[q, co])
    keep2.start()
    have_gu(0, (0,))
    with jax.named_scope("fwd_tile0"):
        fwd_tile(0, nb.at[0], g_t, 0)
    relay_d(0, 0)
    relay_d(0, 1)
    have_gu(0, (1,))
    with jax.named_scope("fwd_tile1"):
        for i in range(1, hh // tile):
            fwd_tile(0, nb.at[0], g_t, i)
    for s in save_ab(q):
        s.start()
    have_d_own(0)
    relay_d(0, 2)
    down_half(0, g_t, x, 0, t2, False)
    relay_d(0, 3)
    ag_spread_got("n0", n0_buf, "y")
    have_d(0)
    down_half(0, g_t, xo, co * td, td, True)
    core_push("d0")
    down_half(0, g_t, xo, c * td, td, True)
    core_sum_send("d0")
    keep2.wait()
    send_done("n0p")
    saves_done(q)
    partner_has("n0", n0_buf, 0)
    stage(n0_buf, block_of(0), nb.at[0], "sn")
    relay_gu(1, 0, 0)
    staged(n0_buf, block_of(0), nb.at[0], "sn")
    f0_other(0, 0)
    z_relay("d0", 0, 0)
    relay_gu(1, 0, 1)
    z_relay("d0", 0, 1)
    ag_spread_got("n0", n0_buf, "x")
    ag_spread_got("o1", o1_buf, "y")
    partner_has("n0", n0_buf, 1)
    stage(n0_buf, block_of(1), nb.at[0], "sn")
    z_relay("d0", 1, 0)
    relay_gu(1, 1, 0)
    z_relay("d0", 1, 1)
    local("xc", x_in.at[rows(z * ch, ch)], x_ch).wait()

    @pl.when(outer == 1)
    def _():
        h1_done()

    relay_gu(1, 1, 1)

    @pl.when(inner == 1)
    def _():
        h1_done()

    local("dyc", dy_in.at[rows(z * ch, ch)], x_ch).start()
    group_done(("W", 0))
    flush(("xp", "dyp", "rp"))
    relay_d(1, 0)
    z_take("n1z", n_own, 0)
    z_take("n1z", n_own, 1)
    relay_d(1, 1)
    z_take("n1z", n_own, 2)
    relay_d(1, 2)
    saves_done(block_of(0))
    for h in (1, 0):
        ag_x("n1", n1_buf, n1_src, h)
    ag_x("o1", o1_buf, dy_src, 0)
    for h in range(2):
        ag_y("n1", n1_buf, n1_src, h)
    got("dyp", o1_buf.at[q, co])
    dy_other = local("dy_other", o1_buf.at[q, co], ob.at[0, rows(co * td, td)])
    dy_other.start()
    z_gathered_partner("n1z", n_own)

    have_gu(1, (0, 1))
    fwd(1, n_own, g_t)
    local("dy_own", dy_in, ob.at[0, rows(c * td, td)]).wait()
    dy_other.wait()
    have_d_own(1)
    bwd_tile(1, ob.at[0], x, a_t, b_t)
    sum_sends_done("d0")
    m_half(1, x, 0, t2, False)
    have_d(1)
    bwd_tile(1, ob.at[0], xo, a_t, b_t)
    g_keep = local("gk", g_t, g_save)
    g_keep.start()
    m_half(1, xo, co * td, td, True)
    core_push("d1")
    m_half(1, xo, c * td, td, True)
    core_sum_send("d1")
    zero_acc()
    g_keep.wait()
    local("dyc", dy_in.at[rows(z * ch, ch)], x_ch).wait()

    @scoped
    def e_calc():
        def e_step(i, dg1):
            r = rows(i * 16, 16)
            m = z_sum("d1", i)
            h_f = h1_ch[r, :].astype(F32)
            r_inv = rinv(h_f)
            xh = h_f * r_inv
            v = m * gain[1:2, :]
            e = x_ch[r, :].astype(F32) + r_inv * (v - xh * jnp.mean(v * xh, axis=-1, keepdims=True))
            o_own[rows(c * td + z * ch + i * 16, 16), :] = e.astype(BF16)
            return dg1 + jnp.sum(m * xh, axis=0, keepdims=True)

        dg[1:2, :] = lax.fori_loop(0, ch // 16, e_step, jnp.zeros((1, d), F32))

    def at_step(k, n):
        return pl.when(k == n)

    def stage_n(buf, block, slot):
        stage(buf, block, nb.at[slot], ("n", slot))

    def staged_n(buf, block, slot):
        staged(buf, block, nb.at[slot], ("n", slot))

    def stage_o(buf, block, slot):
        stage(buf, block, ob.at[slot], ("o", slot))

    def staged_o(buf, block, slot):
        staged(buf, block, ob.at[slot], ("o", slot))

    xl = lambda: [local("xl0", x_in, nb.at[0, rows(c * td, td)]), local("xl1", x_part, nb.at[0, rows(co * td, td)])]

    def n_half(slot):
        return wu.at[1, rows(slot * t2, t2)]

    def n_half_copies(block, slot):
        return [local(("nh", slot, core), n0_buf.at[block, core, :, cols(2 * x * rb, 2 * rb)], wu.at[1, rows(slot * t2 + core * td, td)]) for core in range(2)]

    def load_n_half(block, slot):
        for s in n_half_copies(block, slot):
            s.start()

    own_g = nb.at[1, :, pl.ds(0, hh)]

    def e_done():
        z_got("d1")
        relay_sends_done("d1")
        e_calc()
        z_gather("o0z", o_own)
        for dev in others:
            pl.semaphore_signal(credit, inc=1, device_id=at_z(dev), device_id_type=MESH)

    def l1_step(k, carry):
        slot = 1 - (k + 3) // 4

        @pl.when(k > 0)
        def _():
            @at_step(k, 1)
            def _():
                partner_has("o1", o1_buf, 0)
                stage_o(o1_buf, block_of(0), 0)

            staged_n(n1_buf, block_of(k - 1), 0)
            with jax.named_scope("fwd_a"):
                fwd_tile(1, nb.at[0], None, 0)

            @at_step(k, 2)
            def _():
                ag_got_x("o1", o1_buf, 0, cut_o)

            @at_step(k, 3)
            def _():
                ag_got_dx("o1", o1_buf, cut_o)
                for h in range(2):
                    ag_got_dy("o1", o1_buf, h, cut_o)

            with jax.named_scope("fwd_b"):
                for i in range(1, hh // tile):
                    fwd_tile(1, nb.at[0], None, i)

            @pl.when(k * inner == 2)
            def _():
                e_done()

            @pl.when(k > 1)
            def _():
                partner_has("o1", o1_buf, k - 1)
                stage_o(o1_buf, block_of(k - 1), 0)

            @at_step(k, 3)
            def _():
                for i in range(3):
                    z_take("o0z", o_own, i)
                for h in range(2):
                    ag_x("o0", o0_buf, o0_src, 1 - h)
                    ag_y("o0", o0_buf, o0_src, h)

            @at_step(k, 1)
            def _():
                z_relay("d1", 1, 0)
                ag_got_x("n1", n1_buf, 0, half)

            staged_o(o1_buf, block_of(k - 1), 0)
            bwd_hidden(1, ob.at[0], a_t, b_t)

            @at_step(k, 1)
            def _():
                z_relay("d1", 1, 1)

                @pl.when(outer == 1)
                def _():
                    e_done()

                partner_has("n1", n1_buf, 1)

            @at_step(k, 2)
            def _():
                local("gl", g_save, own_g).wait()
                sum_sends_done("d1")
                down_rows(1, own_g, co)
                core_push("d2")
                ag_got_dx("n1", n1_buf, half)
                ag_got_dy("n1", n1_buf, 1, half)
                down_rows(1, own_g, c)
                core_back_start("d2")

            @at_step(k, 1)
            def _():
                group_done(("X", "n1"))
                passed_done("n1z")
                local("gl", g_save, own_g).start()

            @at_step(k, 3)
            def _():
                z_relay("d2", 0, 0)
                group_done(("W", 1))
                for i in range(3):
                    for s in load_ab(block_of(i - 1) if i else q, i):
                        s.start()
                    load_n_half(block_of(i - 1) if i else q, i)

        weight_grads(nb.at[slot], 2 * x * rb, ob.at[0], None)

        @at_step(k, 1)
        def _():
            stage_n(n1_buf, block_of(1), 0)

        @at_step(k, 2)
        def _():
            partner_has("n1", n1_buf, 2)
            stage_n(n1_buf, block_of(2), 0)
            pl.semaphore_wait(credit, 3)
            core_sum_send("d2")

        @at_step(k, 0)
        def _():
            staged(n0_buf, block_of(1), nb.at[0], "sn")
            f0_other(1, 0)
            ag_got_x("o1", o1_buf, 1, cut_o)
            ag_got_x("n1", n1_buf, 1, half)
            z_relay("d1", 0, 0)
            ag_got_y("n1", n1_buf, 0)
            ag_dx("o1", o1_buf, cut_o)
            ag_dx("n0", n0_buf, cut_n)
            ag_dy("n0", n0_buf, cut_n)
            z_relay("d1", 0, 1)
            ag_got_y("n1", n1_buf, 1)
            partner_has("n1", n1_buf, 0)
            stage_n(n1_buf, block_of(0), 0)
            saves_done(block_of(1))

        return carry

    lax.fori_loop(0, 4, l1_step, 0)
    got("xp", x_part)
    for s in xl():
        s.start()
    for s in load_ab(q, 0):
        s.wait()
    z_gathered_partner("o0z", o_own)
    z_relay("d2", 0, 1)
    grads_push(1)
    grads_out()

    def y_rows(zi):
        return y_out.at[rows(zi * ch, ch)]

    zg_id("y", 0)

    @scoped
    def dgain0():
        def dg_step(i, carry):
            w = cols(i * tile, tile)
            m = mm(a_t[...], wg[0, rows(i * tile, tile)], 1, 1) + mm(b_t[...], wu[0, rows(i * tile, tile)], 1, 1)
            xh = nb[0, :, w].astype(F32) * r_own[:, 0:1]
            dg[0:1, w] = jnp.sum(m * xh, axis=0, keepdims=True)
            return carry

        lax.fori_loop(0, d // tile, dg_step, 0)

    def y_done():
        z_got("d2")

        def y_step(i, carry):
            r = rows(i * 16, 16)
            x_ch[r, :] = (h1_ch[r, :].astype(F32) + z_sum("d2", i)).astype(BF16)
            return carry

        lax.fori_loop(0, ch // 16, y_step, 0)
        local("yk", x_ch, y_rows(z)).start()
        for i, dev in enumerate((far_inner, pair)):
            push(("y", i), lambda dev=dev: (x_ch, y_rows(z), at_z(dev)), zg_id("y", z), group=("X", "y"))

        @pl.when(outer == 1)
        def _():
            copy_of(("y", 2), zg_id("y", z), x_ch, y_rows(z), at_z(far_outer)).start()

    def y_pass():
        got(zg_id("y", far_inner), y_rows(far_inner))
        copy_of(("y", 2), zg_id("y", far_inner), y_rows(far_inner), y_rows(far_inner), at_z(pair)).start()

    def their_d(i):
        return nb.at[0, :, pl.ds(i * hh, hh)]

    def l0_step(k, carry):
        oslot = (k + 1) % 2

        @at_step(k, 2)
        def _():
            ag_got_dx("o0", o0_buf, half)
            ag_got_dy("o0", o0_buf, 1, half)

        @pl.when(k > 0)
        def _():
            staged_o_any(k)

        @pl.when(k * inner == 3)
        def _():
            y_pass()

        bwd_hidden(0, ob.at[oslot], a_kept(k), b_kept(k))

        @at_step(k, 0)
        def _():
            for s in xl():
                s.wait()
            ag_got_dx("n0", n0_buf, cut_n)
            ag_got_dy_whole("n0", n0_buf, cut_n)
            z_relay("d2", 1, 0)
            dgain0()
            dg_z[z] = dg[...]
            for i in range(3):
                push(("gs", i), lambda i=i: (dg_z.at[z], dg_z.at[z], at_z(others[i])), "gz")
            z_relay("d2", 1, 1)
            partner_has("n0", n0_buf, 2)
            stage_n(n0_buf, block_of(2), 0)
            load_n_half(block_of(2), 3)
            ag_got_y("o0", o0_buf, 0)
            ag_got_x("o0", o0_buf, 1, half)
            grads_out_done(1)
            zero_acc()
            for i in range(4):
                for s in n_half_copies(block_of(i - 1) if i else q, i):
                    s.wait()
            for i in range(1, 3):
                for s in load_ab(block_of(i - 1), i):
                    s.wait()

        @at_step(k, 1)
        def _():
            @pl.when(inner == 1)
            def _():
                y_done()

            for h in range(2):
                send_done(("d2", "A", h))
                for s in "BC":
                    copy_of(("d2", s, h), 0, mine(0, h), slot("d2", 0, h), at_z(pair)).wait_send()
            partner_has("o0", o0_buf, 1)
            group_done(("X", "o0"))
            stage_o(o0_buf, block_of(1), 1)
            got("gz", dg_z.at[pl.ds(0, 3)])
            for i in range(3):
                send_done(("gs", i))
            dg[...] = dg_z[0] + dg_z[1] + dg_z[2] + dg_z[3]
            push("gc", lambda: (dg, dg_core, to_c))

        @at_step(k, 2)
        def _():
            got("gc", dg_core)
            copy_of("gc", 0, dg, dg_core, to_c).wait_send()
            dg[...] = dg[...] + dg_core[...]
            push("gx", lambda: (dg, dg_x, to_x))
            partner_has("o0", o0_buf, 2)
            stage_o(o0_buf, block_of(2), 0)

        @at_step(k, 3)
        def _():
            got("gx", dg_x)
            copy_of("gx", 0, dg, dg_x, to_x).wait_send()
            dg[...] = dg[...] + dg_x[...]
            push("gy", lambda: (dg, dg_y, to_y))

        @at_step(k, 3)
        def _():
            for i in range(2):
                push(("dab", i), lambda i=i: ((a_t, b_t)[i], their_d(i), to_c), "dab")

        weight_grads(n_half(k), 0, ob.at[oslot], k < 3)

        @at_step(k, 2)
        def _():
            grads_push(0)

        @at_step(k, 0)
        def _():
            staged_n(n0_buf, block_of(2), 0)
            with jax.named_scope("f0_a"):
                fwd_tile(0, nb.at[0], None, 0, a_kept(3), b_kept(3))
            ag_got_y("o0", o0_buf, 1)
            ag_got_x("o0", o0_buf, 0, half)
            with jax.named_scope("f0_b"):
                for i in range(1, hh // tile):
                    fwd_tile(0, nb.at[0], None, i, a_kept(3), b_kept(3))

            partner_has("o0", o0_buf, 0)
            stage_o(o0_buf, block_of(0), 0)

            @pl.when(outer == 1)
            def _():
                y_done()

            for a in ("n0", "o1", "n1"):
                group_done(("S", a))

        return carry

    def staged_o_any(k):
        for n, slot in ((1, 0), (2, 1), (3, 0)):
            @at_step(k, n)
            def _(n=n, slot=slot):
                staged_o(o0_buf, block_of(n - 1), slot)

    lax.fori_loop(0, 4, l0_step, 0)
    for key in ("gc", "gx", "gy"):
        sent.pop(key)
    got("gy", dg_y)
    copy_of("gy", 0, dg, dg_y, to_y).wait_send()
    dgain_out[...] = dg[...] + dg_y[...]
    grads_out_done(0)
    with jax.named_scope("got_y"):
        got(zg_id("y", pair), y_rows(pair))
        got(zg_id("y", far_outer), y_rows(far_outer))

        @pl.when(outer == 1)
        def _():
            got(zg_id("y", far_inner), y_rows(far_inner))

        copy_of(("y", 2), 0, x_ch, x_ch, to_c).wait_send()
    local("yk", x_ch, y_rows(z)).wait()
    for key in list(sent):
        send_done(key)
    for group in list(groups):
        group_done(group)
    assert not passed


def finish(acc_g, acc_u, acc_d, other, gain_in, g1, u1, d1, y_in, g_out, u_out, d_out, y_out, gain_out, buf, ybuf, sem_in, sem_out):
    rb, hh = other.shape[0], acc_g.shape[1]
    fb = hh // 2
    f = lax.axis_index("fsdp")
    c = f % 2
    ins = [pltpu.make_async_copy(src, buf.at[i], sem_in.at[i]) for i, src in enumerate((g1, u1, d1))]
    ins.append(pltpu.make_async_copy(y_in, ybuf, sem_in.at[3]))
    for copy in ins:
        copy.start()
    outs = []

    def out(src, dst):
        copy = pltpu.make_async_copy(src, dst, sem_out.at[len(outs)])
        copy.start()
        outs.append(copy)

    for i, (acc, dst) in enumerate(((acc_g, g_out), (acc_u, u_out))):
        for xb in range(2):
            own = pl.ds(pl.multiple_of((2 * xb + c) * fb, 128), fb)
            out(acc.at[pl.ds(pl.multiple_of(c * rb, rb), rb), pl.ds(xb * fb, fb)], dst.at[0, :, own])
            theirs = pl.ds(pl.multiple_of((2 * xb + 1 - c) * fb, 128), fb)
            out(other.at[:, pl.ds(i * hh + xb * fb, fb)], dst.at[0, :, theirs])
    out(acc_d, d_out.at[0])
    out(gain_in, gain_out)
    for i, dst in enumerate((g_out, u_out, d_out)):
        ins[i].wait()
        out(buf.at[i], dst.at[1])
    ins[3].wait()
    out(ybuf, y_out)
    for copy in outs:
        copy.wait()


def make_call(td, d, rb, hs):
    fb = hs // 4
    hh, t2, ch = 2 * fb, 2 * td, td // 4
    shape = jax.ShapeDtypeStruct
    hbm = pl.BlockSpec(memory_space=pl.ANY)
    vmem = pl.BlockSpec(memory_space=pltpu.VMEM)
    block = shape((4, 2, td, d), BF16)
    outs = [
        shape((td, d), BF16), shape((rb, hs), F32), shape((rb, hs), F32), shape((fb, d), F32), pltpu.VMEM((2, d), F32),
        pltpu.VMEM((2 * rb, hh), F32), pltpu.VMEM((2 * rb, hh), F32), pltpu.VMEM((fb, d), F32), pltpu.VMEM((t2, d), F32),
        block, block, block, block, shape((4, t2, hh), BF16), shape((4, t2, hh), BF16), shape((td, d), BF16), shape((t2, hh), BF16), shape((td, d), F32),
    ]
    scratch = [
        pltpu.VMEM((2, d, hh), BF16), pltpu.VMEM((2, d, hh), BF16), pltpu.VMEM((2, hh, d), BF16),
        pltpu.VMEM((2, t2, d), BF16), pltpu.VMEM((2, t2, d), BF16),
        pltpu.VMEM((t2, hh), BF16), pltpu.VMEM((t2, hh), BF16), pltpu.VMEM((t2, hh), BF16),
        pltpu.VMEM((4, ch, d), F32),
        pltpu.VMEM((ch, d), BF16), pltpu.VMEM((ch, d), BF16),
        pltpu.VMEM((t2, 128), F32),
        pltpu.VMEM((2, d), F32), pltpu.VMEM((2, d), F32), pltpu.VMEM((2, d), F32), pltpu.VMEM((2, d), F32), pltpu.VMEM((4, 2, d), F32),
        pltpu.SemaphoreType.DMA((NSEND,)), pltpu.SemaphoreType.DMA((NRECV,)), pltpu.SemaphoreType.DMA((NLOC,)), pltpu.SemaphoreType.REGULAR,
    ]
    step = pl.pallas_call(
        kernel,
        out_shape=outs,
        in_specs=[hbm] * 5 + [vmem],
        out_specs=[hbm] * 4 + [vmem] * 5 + [hbm] * 9,
        scratch_shapes=scratch,
        compiler_params=pltpu.CompilerParams(collective_id=0, has_side_effects=True, vmem_limit_bytes=VLIM),
    )
    end = pl.pallas_call(
        finish,
        out_shape=[shape((2, rb, hs), F32), shape((2, rb, hs), F32), shape((2, fb, d), F32), shape((td, d), BF16), shape((2, d), F32)],
        in_specs=[vmem] * 5 + [hbm] * 4,
        out_specs=[hbm] * 5,
        scratch_shapes=[pltpu.VMEM((3, rb, hs), F32), pltpu.VMEM((td, d), BF16), pltpu.SemaphoreType.DMA((4,)), pltpu.SemaphoreType.DMA((14,))],
        compiler_params=pltpu.CompilerParams(vmem_limit_bytes=VLIM2),
    )

    def call(*args):
        y, g1, u1, d1, dgain, acc_g, acc_u, acc_d, other = step(*args)[:9]
        kept = [pltpu.with_memory_space_constraint(v, pltpu.VMEM) for v in (acc_g, acc_u, acc_d, other, dgain)]
        stored = [pltpu.with_memory_space_constraint(v, pltpu.HBM) for v in (g1, u1, d1, y)]
        g, u, dd, y, dgain = end(*kept, *stored)
        return y, g, u, dd, dgain

    return call


def solution(mesh):
    tok_spec = P(("replica", "fsdp"), None)
    wide_spec = P(None, "fsdp", "tensor")
    down_spec = P(None, ("tensor", "fsdp"), None)
    gain_spec = P(None, None)

    def device_fn(x_loc, dy_loc, w_gate, w_up, w_down, norm_gain):
        call = make_call(x_loc.shape[0], x_loc.shape[1], w_gate.shape[1], w_gate.shape[2])
        return call(x_loc, dy_loc, w_gate, w_up, w_down, norm_gain)

    return jax.shard_map(device_fn, mesh=mesh, in_specs=(tok_spec, tok_spec, wide_spec, wide_spec, down_spec, gain_spec), out_specs=(tok_spec, wide_spec, wide_spec, down_spec, gain_spec), check_vma=False)
```
